512 devices in a mesh: runs: 2 (over y), gx: 16 (over z), gy: 8 (over x), gz: 2 (over core).
Axes of the slice: x: 8, y: 2, z: 16, core: 2. Of those that a mesh axis runs over, the one named last changes fastest.
The devices are a block of a 8x8x16 slice.
Arguments:
- positions: float32 [3, 8, 65536], P(None, None, ('runs', 'gx', 'gy', 'gz')), parts along dimension 2, as said below
- velocities: float32 [3, 8, 65536], P(None, None, ('runs', 'gx', 'gy', 'gz')), parts along dimension 2, may hold values from -5 to 5
- send_list: int32 [91136], P(('runs', 'gx', 'gy', 'gz')), parts along dimension 0, may hold values from 0 to 127, as said below
- pair_list: int32 [2, 917504], P(None, ('runs', 'gx', 'gy', 'gz')), parts along dimension 1, may hold values from 0 to 306, as said below
- constraint_flags: int32 [7, 65536], P(None, ('runs', 'gx', 'gy', 'gz')), parts along dimension 1, may hold values 0 or 1
Outputs:
- final_positions: float32 [3, 8, 65536], P(None, None, ('runs', 'gx', 'gy', 'gz')), parts along dimension 2
- final_velocities: float32 [3, 8, 65536], P(None, None, ('runs', 'gx', 'gy', 'gz')), parts along dimension 2
- energies: float32 [6, 2], P('runs'), parts along dimension 0
The draws below stay inside these ranges and needn't reach their ends.
There are 2 independent parts, one for each index of `runs`. The reference program is written for one: setup_inputs(seed, part) draws one part's arguments, and reference() takes and returns one part's arrays. A program takes and returns all parts, laid end to end along the dimension named above; each array names one. Nothing has to cross between parts.
Inputs may be any that keep to these rules, and one draw needn't show every extreme that they name: `send_list`: each domain's 178 entries are its own clusters (0 to 127, counted within the domain), in seven zone blocks of the sizes and order given in the reference program; a cluster may appear in several blocks. `pair_list`: each domain's 1792 slots name clusters of its extended set: 0 to 127 its own, then its received zone blocks in order; padding slots hold 306 in both rows; every cluster appears in a slot with itself; no unordered pair appears twice. `positions`: eight beads of a cluster lie in its cell of side 1, the cells of a domain filling a box of 1 by 8 by 16; neighbouring beads of a cluster are between 0.25 and 0.6 apart.
All inputs are finite; a program needn't handle non-finite values. No bound on the sum of `constraint_flags` on one device may be relied on, other than what follows from the above.
Results may differ from the reference program's by a relative error of at most 0.0003.
Values sent between devices are 32-bit elements; how exact they have to be, the bound alone decides.
A program may use at most 64 MiB of HBM per device.

```python
import jax
import jax.numpy as jnp
import numpy as np
from jax import lax

CX = 1
CY = 8
CZ = 16
ITERS = 3
NORDER = 4
NITER = 1
CL = 128
HC = 178
NP = 1792
DOMAINS = 256
NCL = 32768
BEADS = 262144
N_GX = 16
N_GY = 8
N_GZ = 2


zone_list = ((1, 0, 0), (0, 1, 0), (0, 0, 1), (1, 1, 0), (1, 0, 1), (0, 1, 1), (1, 1, 1))


def cluster_layout(key):
    layout_key = jax.random.fold_in(key, 101)
    scores = jax.random.randint(layout_key, (DOMAINS, CL), 0, 16384) * CL + jnp.arange(CL, dtype=jnp.int32)[None]
    cell_of_slot = jnp.argsort(scores, axis=1).astype(jnp.int32)
    slot_of_cell = jnp.argsort(cell_of_slot, axis=1).astype(jnp.int32)
    return (cell_of_slot, slot_of_cell)


def zone_cells(direction):
    cell_list = []
    for coord_x in [0] if direction[0] else range(CX):
        for coord_y in [0] if direction[1] else range(CY):
            for coord_z in [0] if direction[2] else range(CZ):
                cell_list.append((coord_x, coord_y, coord_z))
    return cell_list


def send_cells():
    linear = []
    for direction in zone_list:
        for cell in zone_cells(direction):
            linear.append((cell[0] * CY + cell[1]) * CZ + cell[2])
    return np.array(linear, np.int32)


def candidate_pairs():
    home_table = np.full((CX + 1, CY + 1, CZ + 1), -1, np.int32)
    halo_table = np.full((CX + 1, CY + 1, CZ + 1), -1, np.int32)
    for coord_x in range(CX):
        for coord_y in range(CY):
            for coord_z in range(CZ):
                home_table[coord_x, coord_y, coord_z] = (coord_x * CY + coord_y) * CZ + coord_z
    counter = CX * CY * CZ
    for direction in zone_list:
        for cell in zone_cells(direction):
            halo_table[cell[0] + direction[0] * CX, cell[1] + direction[1] * CY, cell[2] + direction[2] * CZ] = counter
            counter += 1
    dim_options = ((0, 0), (0, 1), (1, 0))
    patterns = []
    for first_dim in dim_options:
        for second_dim in dim_options:
            for third_dim in dim_options:
                pattern = (first_dim, second_dim, third_dim)
                leading = [entry for entry in pattern if entry != (0, 0)]
                if not leading or leading[0] == (0, 1):
                    patterns.append(pattern)
    first_home, first_halo, second_home, second_halo = ([], [], [], [])
    for coord_x in range(CX):
        for coord_y in range(CY):
            for coord_z in range(CZ):
                for pattern in patterns:
                    first_cell = (coord_x + pattern[0][0], coord_y + pattern[1][0], coord_z + pattern[2][0])
                    second_cell = (coord_x + pattern[0][1], coord_y + pattern[1][1], coord_z + pattern[2][1])
                    first_home.append(home_table[first_cell])
                    first_halo.append(halo_table[first_cell])
                    second_home.append(home_table[second_cell])
                    second_halo.append(halo_table[second_cell])
    return (np.array(first_home, np.int32), np.array(first_halo, np.int32), np.array(second_home, np.int32), np.array(second_halo, np.int32))


def draw_positions(key, part):
    cell_of_slot, slot_of_cell = cluster_layout(key)
    cell_x = cell_of_slot // (CY * CZ)
    cell_y = cell_of_slot // CZ % CY
    cell_z = cell_of_slot % CZ
    cell_coords = jnp.stack([cell_x, cell_y, cell_z]).astype(jnp.float32)
    beads = jnp.arange(8, dtype=jnp.float32)
    parity = (jnp.arange(8, dtype=jnp.int32) % 2).astype(jnp.float32)
    offsets = jnp.stack([0.115 + 0.11 * beads, 0.3 + 0.4 * parity, 0.115 + 0.11 * beads])
    spread = 0.03
    noise = jax.random.uniform(jax.random.fold_in(key, 202), (3, 8, DOMAINS, CL), jnp.float32, -spread, spread)
    result = cell_coords[:, None] + offsets[:, :, None, None] + noise
    return result.reshape(3, 8, DOMAINS * CL)


def draw_send_list(key, part):
    cell_of_slot, slot_of_cell = cluster_layout(key)
    return slot_of_cell[:, jnp.asarray(send_cells())].reshape(DOMAINS * HC).astype(jnp.int32)


def draw_pair_list(key, part):
    cell_of_slot, slot_of_cell = cluster_layout(key)
    first_home, first_halo, second_home, second_halo = candidate_pairs()
    padding = CL + HC

    def resolve(home_ids, halo_ids):
        from_home = slot_of_cell[:, jnp.asarray(np.maximum(home_ids, 0))]
        return jnp.where(jnp.asarray(home_ids >= 0)[None], from_home, jnp.asarray(halo_ids)[None])
    first_ids = resolve(first_home, first_halo)
    second_ids = resolve(second_home, second_halo)
    self_mask = jnp.asarray((first_home == second_home) & (first_halo == second_halo))[None]
    keep = (jax.random.randint(jax.random.fold_in(key, 303), (DOMAINS, NP), 0, 8) != 0) | self_mask
    first_ids = jnp.where(keep, first_ids, padding)
    second_ids = jnp.where(keep, second_ids, padding)
    order_scores = jax.random.randint(jax.random.fold_in(key, 404), (DOMAINS, NP), 0, 4096) * NP + jnp.arange(NP, dtype=jnp.int32)[None]
    shuffle = jnp.argsort(order_scores, axis=1)
    first_ids = jnp.take_along_axis(first_ids, shuffle, axis=1)
    second_ids = jnp.take_along_axis(second_ids, shuffle, axis=1)
    return jnp.stack([first_ids.reshape(-1), second_ids.reshape(-1)]).astype(jnp.int32)


def with_ends(values, key, smallest, high):
    place = [jax.random.randint(jax.random.fold_in(key, axis), (), 0, length) for axis, length in enumerate(values.shape)]
    longest = values.shape.index(max(values.shape))
    next_to = place[:longest] + [(place[longest] + 1) % values.shape[longest]] + place[longest + 1:]
    return values.at[tuple(place)].set(smallest).at[tuple(next_to)].set(high)


def level_of(stream_key, dims, cuts, least, top_value):
    def one(position, parts):
        heights = jax.random.uniform(jax.random.fold_in(jax.random.fold_in(stream_key, 6), position), (parts,), jnp.float32, least / len(cuts), top_value / len(cuts))
        return jnp.repeat(jnp.exp(heights), dims[position] // parts).reshape((-1,) + (1,) * (len(dims) - position - 1))

    factor_of = one(*cuts[0])
    for cut in cuts[1:]:
        factor_of = factor_of * one(*cut)
    return factor_of


def normal_values(stream_key, dims, scale, limit, shards=(), held_as=jnp.bfloat16):
    drawn = jax.random.normal(stream_key, dims, jnp.float32) * scale
    if len(shards) > 0:
        drawn = level_of(stream_key, dims, shards, -0.22, 0.18) * drawn
    return jnp.clip(drawn, min=-limit, max=limit).astype(held_as)


def setup_inputs(seed: int = 0, part: int = 0) -> dict:
    keys = jax.random.split(jax.random.key(seed), 6)
    own_keys = jax.random.split(jax.random.fold_in(keys[5], part), 6)
    positions = draw_positions(jax.random.fold_in(jax.random.fold_in(keys[5], part), 71), part)
    velocities = normal_values(own_keys[1], (3, 8, NCL), 1.0, 5.0, ((2, 256),), jnp.float32)
    send_list = draw_send_list(jax.random.fold_in(jax.random.fold_in(keys[5], part), 71), part)
    pair_list = draw_pair_list(jax.random.fold_in(jax.random.fold_in(keys[5], part), 71), part)
    constraint_flags = with_ends((jax.random.randint(own_keys[4], (7, NCL), 0, 4) < 3).astype(jnp.int32), jax.random.fold_in(own_keys[4], 1), 0, 1)
    return dict(positions=positions, velocities=velocities, send_list=send_list, pair_list=pair_list, constraint_flags=constraint_flags)


time_step = 0.02
strength = 2.0
root_half = 0.7071067811865476
zone_list = ((1, 0, 0), (0, 1, 0), (0, 0, 1), (1, 1, 0), (1, 0, 1), (0, 1, 1), (1, 1, 1))

def zone_sizes():
    return tuple(((CX if direction[0] == 0 else 1) * (CY if direction[1] == 0 else 1) * (CZ if direction[2] == 0 else 1) for direction in zone_list))

def zone_starts():
    block_sizes = zone_sizes()
    return tuple((sum(block_sizes[:number]) for number in range(7)))

def pair_kernel(extended, first_ids, second_ids):
    dummy_index = extended.shape[2] - 1
    first_coords = jnp.take(extended, first_ids, axis=2)
    second_coords = jnp.take(extended, second_ids, axis=2)
    separation = first_coords[:, :, None, :] - second_coords[:, None, :, :]
    scaled = lax.optimization_barrier(jnp.sum(separation * separation, axis=0))
    intersect = jnp.maximum(1.0 - scaled, 0.0)
    bead_row = lax.broadcasted_iota(jnp.int32, (8, 8, 1), 0)
    bead_column = lax.broadcasted_iota(jnp.int32, (8, 8, 1), 1)
    self_pair = (first_ids == second_ids)[None, None, :]
    usable = (first_ids < dummy_index)[None, None, :]
    weight = (jnp.where(self_pair, bead_row < bead_column, True) & usable).astype(jnp.float32)
    energy = strength * jnp.sum(weight * intersect * intersect * intersect)
    magnitude = 6.0 * strength * weight * intersect * intersect
    pushing = magnitude[None] * separation
    return (lax.optimization_barrier(jnp.sum(pushing, axis=2)), -lax.optimization_barrier(jnp.sum(pushing, axis=1)), energy)

def domain_forces(extended, pair_ids):
    first_blocks = pair_ids[0].reshape(28, -1)
    second_blocks = pair_ids[1].reshape(28, -1)

    def accumulate(state, blocks):
        forces, energy = state
        on_first, on_second, block_energy = pair_kernel(extended, blocks[0], blocks[1])
        forces = forces.at[:, :, blocks[0]].add(on_first)
        forces = forces.at[:, :, blocks[1]].add(on_second)
        return ((forces, energy + block_energy), None)
    initial = (jnp.zeros(extended.shape, jnp.float32), jnp.zeros((), jnp.float32))
    result = lax.scan(accumulate, initial, (first_blocks, second_blocks))
    return result[0]

def total_forces(coords, send_list, pair_list):
    grid_shape = (N_GX, N_GY, N_GZ)
    domain_count = N_GX * N_GY * N_GZ
    home_coords = coords.reshape((3, 8) + grid_shape + (CL,))
    send_grid = send_list.reshape(grid_shape + (HC,))
    block_sizes = zone_sizes()
    starts = zone_starts()
    pieces = []
    for number in range(7):
        direction = zone_list[number]
        backward = tuple((-component for component in direction))
        source = jnp.roll(home_coords, backward, axis=(2, 3, 4))
        chosen = jnp.roll(send_grid, backward, axis=(0, 1, 2))[..., starts[number]:starts[number] + block_sizes[number]]
        chosen = jnp.broadcast_to(chosen[None, None], (3, 8) + grid_shape + (block_sizes[number],))
        gathered = jnp.take_along_axis(source, chosen, axis=5)
        offset = jnp.array([direction[0] * CX, direction[1] * CY, direction[2] * CZ], jnp.float32)
        pieces.append(gathered + offset[:, None, None, None, None, None])
    dummy_cluster = jnp.zeros((3, 8) + grid_shape + (1,), jnp.float32)
    extended = jnp.concatenate([home_coords] + pieces + [dummy_cluster], axis=5)
    extended = jnp.moveaxis(extended.reshape(3, 8, domain_count, CL + HC + 1), 2, 0)
    domain_pairs = jnp.moveaxis(pair_list.reshape(2, domain_count, 14 * CL), 1, 0)
    forces, energies = lax.map(lambda pair_data: domain_forces(pair_data[0], pair_data[1]), (extended, domain_pairs))
    forces = jnp.moveaxis(forces, 0, 2)
    flat_home = forces[:, :, :, :CL].reshape(3, 8, domain_count * CL)
    halo_forces = forces[:, :, :, CL:CL + HC].reshape((3, 8) + grid_shape + (HC,))
    domain_base = (jnp.arange(domain_count, dtype=jnp.int32) * CL).reshape(grid_shape + (1,))
    for number in range(7):
        direction = zone_list[number]
        zone_forces = halo_forces[..., starts[number]:starts[number] + block_sizes[number]]
        zone_forces = jnp.roll(zone_forces, direction, axis=(2, 3, 4))
        targets = (send_grid[..., starts[number]:starts[number] + block_sizes[number]] + domain_base).reshape(-1)
        flat_home = flat_home.at[:, :, targets].add(zone_forces.reshape(3, 8, -1))
    return (flat_home, jnp.sum(energies))

def link_vectors(coords):
    return coords[:, :-1, :] - coords[:, 1:, :]

def link_lengths(coords):
    vectors = link_vectors(coords)
    return jnp.sqrt(lax.optimization_barrier(jnp.sum(vectors * vectors, axis=0)))

def expand(coupling, source):
    coupling_down = jnp.pad(coupling, ((1, 0), (0, 0)))
    coupling_up = jnp.pad(coupling, ((0, 1), (0, 0)))
    series = source
    result = source
    for expansion in range(NORDER):
        series = coupling_down * jnp.pad(series, ((1, 0), (0, 0)))[:-1] + coupling_up * jnp.pad(series, ((0, 1), (0, 0)))[1:]
        result = result + series
    return result

def apply_links(coords, directions, solution):
    shifts = directions * (root_half * solution)[None]
    return coords - jnp.pad(shifts, ((0, 0), (0, 1), (0, 0))) + jnp.pad(shifts, ((0, 0), (1, 0), (0, 0)))

def constrain(previous, updated, rest_length, link_flags):
    old_vectors = link_vectors(previous)
    directions = old_vectors / jnp.maximum(jnp.sqrt(lax.optimization_barrier(jnp.sum(old_vectors * old_vectors, axis=0))), 0.2)[None]
    coupling = 0.5 * lax.optimization_barrier(jnp.sum(directions[:, :-1] * directions[:, 1:], axis=0)) * link_flags[:-1] * link_flags[1:]
    projected = lax.optimization_barrier(jnp.sum(directions * link_vectors(updated), axis=0))
    solution = expand(coupling, link_flags * root_half * (projected - rest_length))
    updated = apply_links(updated, directions, solution)
    for correction in range(NITER):
        vectors = link_vectors(updated)
        squared = lax.optimization_barrier(jnp.sum(vectors * vectors, axis=0))
        target = jnp.sqrt(jnp.maximum(2.0 * rest_length * rest_length - squared, 0.25 * rest_length * rest_length))
        solution = expand(coupling, link_flags * root_half * (rest_length - target))
        updated = apply_links(updated, directions, solution)
    return updated

def reference(positions, velocities, send_list, pair_list, constraint_flags):
    link_flags = constraint_flags.astype(jnp.float32)
    rest_length = link_lengths(positions)
    forces, potential = total_forces(positions, send_list, pair_list)
    energy_rows = []
    for iteration in range(ITERS):
        half_speed = velocities + 0.5 * time_step * forces
        updated = constrain(positions, positions + time_step * half_speed, rest_length, link_flags)
        half_speed = (updated - positions) / time_step
        forces, potential = total_forces(updated, send_list, pair_list)
        velocities = half_speed + 0.5 * time_step * forces
        positions = updated
        kinetic = 0.5 * jnp.sum(velocities * velocities)
        energy_rows.append(jnp.stack([potential, kinetic]))
    energies = jnp.stack(energy_rows) / BEADS
    return (positions, velocities, energies)
```

```python
import functools

import jax
import jax.numpy as jnp
from jax import lax
from jax.experimental import pallas as pl
from jax.experimental.pallas import tpu as pltpu
from jax.sharding import PartitionSpec as P

CX, CY, CZ = 1, 8, 16
ITERS = 3
NORDER = 4
time_step = 0.02
root_half = 0.7071067811865476
MESH = pl.DeviceIdType.MESH
ZONES = ((1, 0, 0), (0, 1, 0), (0, 0, 1), (1, 1, 0), (1, 0, 1), (0, 1, 1), (1, 1, 1))
AXES = ("gx", "gy", "gz")
FIRST, SECOND = 24, 26
GROUPS = 14
SLOTS = 1792
F32 = jnp.float32


def roll(x, by, axis):
    size = x.shape[axis]
    by = by % size
    return x if by == 0 else pltpu.roll(x, by, axis)


def partners(sizes):
    found = set()
    for zone in ZONES:
        for sign in (1, -1):
            found.add(tuple((sign * z) % n for z, n in zip(zone, sizes)))
    for oy in range(sizes[1]):
        for oz in range(sizes[2]):
            found.add((0, oy, oz))
    for ox in range(sizes[0]):
        found.add((ox, 0, 0))
    found.discard((0, 0, 0))
    return sorted(found)


def lanes(rows=8):
    return lax.broadcasted_iota(jnp.int32, (rows, 128), 1)


def pack(parts):
    lane = lanes()
    one = jnp.where(
        lane < FIRST,
        parts[0],
        jnp.where(lane < 2 * FIRST, roll(parts[1], FIRST, 1), roll(parts[2], 2 * FIRST, 1)),
    )
    two = jnp.where(
        lane < FIRST + SECOND,
        parts[0],
        jnp.where(
            lane < FIRST + 2 * SECOND, roll(parts[1], SECOND, 1), roll(parts[2], 2 * SECOND, 1)
        ),
    )
    return one, two


def unpack(received):
    lane = lanes()
    within = lax.rem(lane, FIRST)
    one = jnp.where(within < 16, received[0], received[1])
    within = lax.rem(lane + (SECOND - FIRST % SECOND), SECOND)
    two = jnp.where(
        within < 16,
        received[2],
        jnp.where(
            within < 24, received[3], jnp.where(within < 25, received[4], received[5])
        ),
    )
    blocks = []
    for c in range(3):
        block = jnp.where(lane < FIRST, roll(one, -FIRST * c, 1), roll(two, -SECOND * c, 1))
        blocks.append(jnp.where(lane < FIRST + SECOND, block, 0.0))
    return blocks


def halves(value):
    high = value.astype(jnp.bfloat16).astype(F32)
    return jnp.concatenate([high, value - high], axis=0).astype(jnp.bfloat16)


def pick(table, index):
    return jnp.take_along_axis(table, index, axis=1, mode="promise_in_bounds")


def up(x):
    return roll(x, -1, 0)


def down(x):
    return roll(x, 1, 0)


def expand(coupling, coupling_down, source):
    series = source
    result = source
    for _ in range(NORDER):
        series = coupling_down * down(series) + coupling * up(series)
        result = result + series
    return result


def dot3(a, b):
    return a[0] * b[0] + a[1] * b[1] + a[2] * b[2]


def constrain(previous, updated, rest, flags, flags_pair):
    old = [x - up(x) for x in previous]
    length = jnp.maximum(jnp.sqrt(dot3(old, old)), 0.2)
    direction = [x / length for x in old]
    coupling = 0.5 * dot3(direction, [up(x) for x in direction]) * flags_pair
    coupling_down = down(coupling)
    links = [x - up(x) for x in updated]
    solution = expand(
        coupling, coupling_down, flags * root_half * (dot3(direction, links) - rest)
    )
    shifts = [x * (root_half * solution) for x in direction]
    updated = [x - s + down(s) for x, s in zip(updated, shifts)]
    links = [x - up(x) for x in updated]
    squared = dot3(links, links)
    target = jnp.sqrt(jnp.maximum(2.0 * rest * rest - squared, 0.25 * rest * rest))
    solution = expand(coupling, coupling_down, flags * root_half * (rest - target))
    shifts = [x * (root_half * solution) for x in direction]
    return [x - s + down(s) for x, s in zip(updated, shifts)]


def kernel(
    sizes,
    pos_ref,
    vel_ref,
    send_ref,
    pair_ref,
    flag_ref,
    out_pos,
    out_vel,
    out_en,
    cur,
    half_ref,
    rest_ref,
    ids,
    send_ids,
    flag8,
    table,
    back,
    near,
    pair_x,
    pair_f,
    coord_x,
    coord_m,
    force_x,
    force_m,
    got_x,
    got_m,
    ret_x,
    ret_m,
    row,
    plane,
    mid,
    line,
    c_send,
    c_recv,
    f_send,
    f_recv,
    p_send,
    p_recv,
    l_send,
    l_recv,
):
    me = tuple(lax.axis_index(a) for a in AXES)

    def at(offset):
        return {
            a: lax.rem(me[i] + (offset[i] % sizes[i]), sizes[i])
            for i, a in enumerate(AXES)
            if offset[i] % sizes[i]
        }

    barrier = pltpu.get_barrier_semaphore()
    others = partners(sizes)
    for offset in others:
        pl.semaphore_signal(barrier, inc=1, device_id=at(offset), device_id_type=MESH)

    lane = lanes()
    ids[...] = jnp.full(ids.shape, CL_PAD, jnp.int32)
    for g in range(GROUPS):
        for side in range(2):
            ids[pl.ds(16 * side + g, 1), :] = pair_ref[pl.ds(side, 1), pl.ds(128 * g, 128)]
    send_ids[...] = jnp.full(send_ids.shape, -1, jnp.int32)
    send_ids[pl.ds(0, 1), :] = send_ref[:, pl.ds(0, 128)]
    send_ids[pl.ds(1, 1), pl.ds(0, FIRST + SECOND)] = send_ref[:, pl.ds(128, FIRST + SECOND)]
    flag8[...] = jnp.zeros(flag8.shape, F32)
    flag8[pl.ds(0, 7), :] = flag_ref[...].astype(F32)
    columns = jnp.transpose(ids[...].astype(F32))
    send_columns = jnp.transpose(send_ids[...].astype(F32))
    wide = lax.broadcasted_iota(jnp.int32, (128, 384), 1).astype(F32)
    for side in range(2):
        value = 12.0 if side == 0 else -12.0
        for g in range(GROUPS):
            column = columns[:, 16 * side + g : 16 * side + g + 1]
            table[pl.ds(128 * (GROUPS * side + g), 128), :] = jnp.where(
                wide == column, value, 0.0
            ).astype(jnp.bfloat16)
    for b in range(2):
        back[pl.ds(128 * b, 128), :] = jnp.where(
            wide[:, :128] == send_columns[:, b : b + 1], 1.0, 0.0
        ).astype(jnp.bfloat16)

    rest_parts = []
    for c in range(3):
        start = pos_ref[c]
        cur[pl.ds(8 * c, 8), :] = start
        half_ref[pl.ds(8 * c, 8), :] = vel_ref[c]
        rest_parts.append(start - up(start))
    rest_ref[...] = jnp.sqrt(dot3(rest_parts, rest_parts))
    row[...] = jnp.zeros(row.shape, F32)

    pl.semaphore_wait(barrier, len(others))

    def coord_copies():
        copies = []
        for number, zone in enumerate(ZONES):
            source = coord_x if number == 0 else coord_m.at[0 if number < 3 else 1]
            target = got_x if number == 0 else got_m.at[number - 1]
            copies.append(
                pltpu.make_async_remote_copy(
                    src_ref=source,
                    dst_ref=target,
                    send_sem=c_send.at[number],
                    recv_sem=c_recv.at[number],
                    device_id=at(tuple(-z for z in zone)),
                    device_id_type=MESH,
                )
            )
        return copies

    def force_copies():
        copies = []
        for number, zone in enumerate(ZONES):
            source = force_x if number == 0 else force_m.at[0 if number < 3 else 1]
            target = ret_x if number == 0 else ret_m.at[number - 1]
            copies.append(
                pltpu.make_async_remote_copy(
                    src_ref=source,
                    dst_ref=target,
                    send_sem=f_send.at[number],
                    recv_sem=f_recv.at[number],
                    device_id=at(zone),
                    device_id_type=MESH,
                )
            )
        return copies

    def step(t, carry):
        send_x = jnp.broadcast_to(send_ids[pl.ds(0, 1), :], (8, 128))
        send_m = jnp.maximum(jnp.broadcast_to(send_ids[pl.ds(1, 1), :], (8, 128)), 0)
        home = [cur[pl.ds(8 * c, 8), :] for c in range(3)]
        chosen = [pick(x, send_m) for x in home]
        in_zone = [(lane >= a) & (lane < b) for a, b in ((0, 16), (16, 24), (24, 40), (40, 48), (48, 49), (49, 50))]
        for c, length in enumerate((CX, CY, CZ)):
            shifted = None
            for number in range(1, 7):
                if ZONES[number][c]:
                    mask = in_zone[number - 1]
                    shifted = mask if shifted is None else shifted | mask
            chosen[c] = chosen[c] + jnp.where(shifted, F32(length), 0.0)
        one, two = pack(chosen)
        coord_m[0] = one
        coord_m[1] = two
        for c in range(3):
            value = pick(home[c], send_x)
            coord_x[pl.ds(8 * c, 8), :] = value + F32(CX) if c == 0 else value
        copies = coord_copies()
        for copy in copies[::-1]:
            copy.start()

        index = [[ids[pl.ds(16 * side + 8 * h, 8), :] for h in range(2)] for side in range(2)]
        low = [[index[s][h] & 127 for h in range(2)] for s in range(2)]
        for r in range(24):
            source = jnp.broadcast_to(cur[pl.ds(r, 1), :], (8, 128))
            for s in range(2):
                for h in range(2):
                    pair_x[s, h, r] = pick(source, low[s][h])

        for copy in copies:
            copy.wait_recv()
        blocks = unpack([got_m[n] for n in range(6)])
        for c in range(3):
            near[pl.ds(8 * c, 8), :] = blocks[c]
        in_home = [[index[s][h] < 128 for h in range(2)] for s in range(2)]
        in_x = [[index[s][h] < 256 for h in range(2)] for s in range(2)]
        for r in range(24):
            source1 = jnp.broadcast_to(got_x[pl.ds(r, 1), :], (8, 128))
            source2 = jnp.broadcast_to(near[pl.ds(r, 1), :], (8, 128))
            for s in range(2):
                for h in range(2):
                    pair_x[s, h, r] = jnp.where(
                        in_home[s][h],
                        pair_x[s, h, r],
                        jnp.where(
                            in_x[s][h], pick(source1, low[s][h]), pick(source2, low[s][h])
                        ),
                    )

        energy = jnp.zeros((8, 128), F32)
        for h in range(2):
            usable = jnp.where(index[0][h] == CL_PAD, 0.0, 1.0)
            distinct = jnp.where(index[0][h] == index[1][h], 0.0, usable)
            second = [[None] * 3 for _ in range(8)]
            for k in range(8):
                xi = [pair_x[0, h, 8 * c + k] for c in range(3)]
                first = [None] * 3
                for l in range(8):
                    d = [xi[c] - pair_x[1, h, 8 * c + l] for c in range(3)]
                    u = jnp.maximum((usable if k < l else distinct) - dot3(d, d), 0.0)
                    uu = u * u
                    energy = energy + uu * u
                    for c in range(3):
                        push = uu * d[c]
                        first[c] = push if l == 0 else first[c] + push
                        second[l][c] = push if k == 0 else second[l][c] + push
                for c in range(3):
                    pair_f[pl.ds((8 * c + k) * 16 + 8 * h, 8), :] = first[c]
            for l in range(8):
                for c in range(3):
                    pair_f[pl.ds(384 + (8 * c + l) * 16 + 8 * h, 8), :] = second[l][c]

        left = jnp.concatenate(
            [
                halves(pair_f[pl.ds(384 * side + g, 24, stride=16), :])
                for side in range(2)
                for g in range(GROUPS)
            ],
            axis=1,
        )

        @pl.when(t > 0)
        def _():
            for copy in force_copies():
                copy.wait_send()

        halo = jnp.dot(left, table[:, pl.ds(128, 256)], preferred_element_type=F32)
        halo = halo[:24] + halo[24:]
        one, two = pack([halo[8 * c : 8 * c + 8, 128:] for c in range(3)])
        force_m[0] = one
        force_m[1] = two
        force_x[...] = halo[:, :128]
        returns = force_copies()
        for copy in returns[::-1]:
            copy.start()

        own = jnp.dot(left, table[:, pl.ds(0, 128)], preferred_element_type=F32)
        own = own[:24] + own[24:]
        total = jnp.sum(jnp.sum(energy, axis=0, keepdims=True), axis=1, keepdims=True)
        row[...] = jnp.where(lanes(1) == 2 * t - 2, 2.0 * total, row[...])
        for copy in copies:
            copy.wait_send()
        for copy in returns:
            copy.wait_recv()
        blocks = unpack([ret_m[n] for n in range(6)])
        came = jnp.concatenate([ret_x[...], jnp.concatenate(blocks, axis=0)], axis=1)
        came = jnp.dot(halves(came), back[...], preferred_element_type=F32)
        force = own + came[:24] + came[24:]
        force = [0.5 * time_step * force[8 * c : 8 * c + 8] for c in range(3)]

        again = jnp.where(t > 0, 1.0, 0.0).astype(F32)
        speed = [half_ref[pl.ds(8 * c, 8), :] + again * force[c] for c in range(3)]
        total = jnp.sum(jnp.sum(dot3(speed, speed), axis=0, keepdims=True), axis=1, keepdims=True)
        row[...] = jnp.where(lanes(1) == 2 * t - 1, 0.5 * total, row[...])

        @pl.when(t < ITERS)
        def _():
            flags = flag8[...]
            half = [speed[c] + force[c] for c in range(3)]
            before = [cur[pl.ds(8 * c, 8), :] for c in range(3)]
            moved = constrain(
                before,
                [x + time_step * v for x, v in zip(before, half)],
                rest_ref[...],
                flags,
                flags * up(flags),
            )
            for c in range(3):
                cur[pl.ds(8 * c, 8), :] = moved[c]
                half_ref[pl.ds(8 * c, 8), :] = (moved[c] - before[c]) / time_step

        @pl.when(t == ITERS)
        def _():
            for c in range(3):
                out_pos[c] = cur[pl.ds(8 * c, 8), :]
                out_vel[c] = speed[c]

        return carry

    lax.fori_loop(0, ITERS + 1, step, 0)
    for copy in force_copies():
        copy.wait_send()

    def gather(source, slots, offsets, own, send, recv):
        copies = []
        for number, offset in enumerate(offsets):
            copies.append(
                pltpu.make_async_remote_copy(
                    src_ref=source,
                    dst_ref=slots.at[own],
                    send_sem=send.at[number],
                    recv_sem=recv.at[number],
                    device_id=at(offset),
                    device_id_type=MESH,
                )
            )
        for copy in copies:
            copy.start()
        slots[own] = source[...]
        for copy in copies:
            copy.wait_recv()
        total = slots[0]
        for n in range(1, slots.shape[0]):
            total = total + slots[n]
        return total, copies

    offsets = [
        (0, y, z) for y in range(sizes[1]) for z in range(sizes[2]) if (y, z) != (0, 0)
    ]
    total, first_copies = gather(row, plane, offsets, me[1] * sizes[2] + me[2], p_send, p_recv)
    mid[...] = total
    offsets = [(x, 0, 0) for x in range(1, sizes[0])]
    total, second_copies = gather(mid, line, offsets, me[0], l_send, l_recv)
    total = total / F32(8 * 128 * sizes[0] * sizes[1] * sizes[2])
    for t in range(ITERS):
        out_en[pl.ds(t, 1), :] = total[:, 2 * t : 2 * t + 2]
    for copy in first_copies + second_copies:
        copy.wait_send()


CL_PAD = 306


def on_device(sizes, positions, velocities, send_list, pair_list, constraint_flags):
    dma = pltpu.SemaphoreType.DMA
    vmem = pltpu.VMEM
    plane = sizes[1] * sizes[2]
    return pl.pallas_call(
        functools.partial(kernel, sizes),
        out_shape=(
            jax.ShapeDtypeStruct((3, 8, 128), F32),
            jax.ShapeDtypeStruct((3, 8, 128), F32),
            jax.ShapeDtypeStruct((ITERS, 2), F32),
        ),
        in_specs=[pl.BlockSpec(memory_space=vmem)] * 5,
        out_specs=[pl.BlockSpec(memory_space=vmem)] * 3,
        scratch_shapes=[
            vmem((24, 128), F32),
            vmem((24, 128), F32),
            vmem((8, 128), F32),
            vmem((32, 128), jnp.int32),
            vmem((8, 128), jnp.int32),
            vmem((8, 128), F32),
            vmem((2 * SLOTS, 384), jnp.bfloat16),
            vmem((256, 128), jnp.bfloat16),
            vmem((24, 128), F32),
            vmem((2, 2, 24, 8, 128), F32),
            vmem((768, 128), F32),
            vmem((24, 128), F32),
            vmem((2, 8, 128), F32),
            vmem((24, 128), F32),
            vmem((2, 8, 128), F32),
            vmem((24, 128), F32),
            vmem((6, 8, 128), F32),
            vmem((24, 128), F32),
            vmem((6, 8, 128), F32),
            vmem((1, 128), F32),
            vmem((plane, 1, 128), F32),
            vmem((1, 128), F32),
            vmem((sizes[0], 1, 128), F32),
            dma((7,)),
            dma((7,)),
            dma((7,)),
            dma((7,)),
            dma((plane - 1,)),
            dma((plane - 1,)),
            dma((sizes[0] - 1,)),
            dma((sizes[0] - 1,)),
        ],
        compiler_params=pltpu.CompilerParams(collective_id=0, has_side_effects=True),
        name="membrane",
    )(positions, velocities, send_list.reshape(1, -1), pair_list, constraint_flags)


def solution(mesh):
    sizes = tuple(mesh.shape[a] for a in AXES)
    spec = ("runs", "gx", "gy", "gz")
    return jax.shard_map(
        functools.partial(on_device, sizes),
        mesh=mesh,
        in_specs=(
            P(None, None, spec),
            P(None, None, spec),
            P(spec),
            P(None, spec),
            P(None, spec),
        ),
        out_specs=(P(None, None, spec), P(None, None, spec), P("runs", None)),
        check_vma=False,
    )
```

```python
import functools

import jax
import jax.numpy as jnp
from jax import lax
from jax.experimental import pallas as pl
from jax.experimental.pallas import tpu as pltpu
from jax.sharding import PartitionSpec as P

CX, CY, CZ = 1, 8, 16
ITERS = 3
NORDER = 4
time_step = 0.02
root_half = 0.7071067811865476
MESH = pl.DeviceIdType.MESH
ZONES = ((1, 0, 0), (0, 1, 0), (0, 0, 1), (1, 1, 0), (1, 0, 1), (0, 1, 1), (1, 1, 1))
AXES = ("gx", "gy", "gz")
FIRST, SECOND = 24, 26
GROUPS = 14
SLOTS = 1792
F32 = jnp.float32


def roll(x, by, axis):
    size = x.shape[axis]
    by = by % size
    return x if by == 0 else pltpu.roll(x, by, axis)


def partners(sizes):
    found = set()
    for zone in ZONES:
        for sign in (1, -1):
            found.add(tuple((sign * z) % n for z, n in zip(zone, sizes)))
    found.discard((0, 0, 0))
    return sorted(found)


def lanes(rows=8):
    return lax.broadcasted_iota(jnp.int32, (rows, 128), 1)


def pack(parts):
    lane = lanes()
    one = jnp.where(
        lane < FIRST,
        parts[0],
        jnp.where(lane < 2 * FIRST, roll(parts[1], FIRST, 1), roll(parts[2], 2 * FIRST, 1)),
    )
    two = jnp.where(
        lane < FIRST + SECOND,
        parts[0],
        jnp.where(
            lane < FIRST + 2 * SECOND, roll(parts[1], SECOND, 1), roll(parts[2], 2 * SECOND, 1)
        ),
    )
    return one, two


def unpack(received):
    lane = lanes()
    within = lax.rem(lane, FIRST)
    one = jnp.where(within < 16, received[0], received[1])
    within = lax.rem(lane + (SECOND - FIRST % SECOND), SECOND)
    two = jnp.where(
        within < 16,
        received[2],
        jnp.where(
            within < 24, received[3], jnp.where(within < 25, received[4], received[5])
        ),
    )
    blocks = []
    for c in range(3):
        block = jnp.where(lane < FIRST, roll(one, -FIRST * c, 1), roll(two, -SECOND * c, 1))
        blocks.append(jnp.where(lane < FIRST + SECOND, block, 0.0))
    return blocks


def halves(value):
    high = value.astype(jnp.bfloat16).astype(F32)
    return jnp.concatenate([high, value - high], axis=0).astype(jnp.bfloat16)


def pick(table, index):
    return jnp.take_along_axis(table, index, axis=1, mode="promise_in_bounds")


def up(x):
    return roll(x, -1, 0)


def down(x):
    return roll(x, 1, 0)


def expand(coupling, coupling_down, source):
    series = source
    result = source
    for _ in range(NORDER):
        series = coupling_down * down(series) + coupling * up(series)
        result = result + series
    return result


def dot3(a, b):
    return a[0] * b[0] + a[1] * b[1] + a[2] * b[2]


def constrain(previous, updated, rest, flags, flags_pair):
    old = [x - up(x) for x in previous]
    length = jnp.maximum(jnp.sqrt(dot3(old, old)), 0.2)
    direction = [x / length for x in old]
    coupling = 0.5 * dot3(direction, [up(x) for x in direction]) * flags_pair
    coupling_down = down(coupling)
    links = [x - up(x) for x in updated]
    solution = expand(
        coupling, coupling_down, flags * root_half * (dot3(direction, links) - rest)
    )
    shifts = [x * (root_half * solution) for x in direction]
    updated = [x - s + down(s) for x, s in zip(updated, shifts)]
    links = [x - up(x) for x in updated]
    squared = dot3(links, links)
    target = jnp.sqrt(jnp.maximum(2.0 * rest * rest - squared, 0.25 * rest * rest))
    solution = expand(coupling, coupling_down, flags * root_half * (rest - target))
    shifts = [x * (root_half * solution) for x in direction]
    return [x - s + down(s) for x, s in zip(updated, shifts)]


def kernel(
    sizes,
    pos_ref,
    vel_ref,
    send_ref,
    pair_ref,
    flag_ref,
    out_pos,
    out_vel,
    out_en,
    cur,
    half_ref,
    rest_ref,
    ids,
    send_ids,
    flag8,
    table,
    back,
    near,
    pair_x,
    pair_f,
    coord_x,
    coord_m,
    force_x,
    force_m,
    got_x,
    got_m,
    ret_x,
    ret_m,
    row,
    plane,
    mid,
    line,
    c_send,
    c_recv,
    f_send,
    f_recv,
    p_send,
    p_recv,
    l_send,
    l_recv,
    token,
):
    me = tuple(lax.axis_index(a) for a in AXES)

    def at(offset):
        return {
            a: lax.rem(me[i] + (offset[i] % sizes[i]), sizes[i])
            for i, a in enumerate(AXES)
            if offset[i] % sizes[i]
        }

    barrier = pltpu.get_barrier_semaphore()
    others = partners(sizes)
    for offset in others:
        pl.semaphore_signal(barrier, inc=1, device_id=at(offset), device_id_type=MESH)

    lane = lanes()
    send_ids[...] = jnp.full(send_ids.shape, -1, jnp.int32)
    send_ids[pl.ds(0, 1), :] = send_ref[:, pl.ds(0, 128)]
    send_ids[pl.ds(1, 1), pl.ds(0, FIRST + SECOND)] = send_ref[:, pl.ds(128, FIRST + SECOND)]
    for c in range(3):
        cur[pl.ds(8 * c, 8), :] = pos_ref[c]
        half_ref[pl.ds(8 * c, 8), :] = vel_ref[c]
    row[...] = jnp.zeros(row.shape, F32)

    pl.semaphore_wait(barrier, len(others))

    def prepare():
        ids[...] = jnp.full(ids.shape, CL_PAD, jnp.int32)
        for g in range(GROUPS):
            for side in range(2):
                ids[pl.ds(16 * side + g, 1), :] = pair_ref[pl.ds(side, 1), pl.ds(128 * g, 128)]
        flag8[...] = jnp.zeros(flag8.shape, F32)
        flag8[pl.ds(0, 7), :] = flag_ref[...].astype(F32)
        columns = jnp.transpose(ids[...].astype(F32))
        send_columns = jnp.transpose(send_ids[...].astype(F32))
        wide = lax.broadcasted_iota(jnp.int32, (128, 384), 1).astype(F32)
        for side in range(2):
            value = 12.0 if side == 0 else -12.0
            for g in range(GROUPS):
                column = columns[:, 16 * side + g : 16 * side + g + 1]
                table[pl.ds(128 * (GROUPS * side + g), 128), :] = jnp.where(
                    wide == column, value, 0.0
                ).astype(jnp.bfloat16)
        for b in range(2):
            back[pl.ds(128 * b, 128), :] = jnp.where(
                wide[:, :128] == send_columns[:, b : b + 1], 1.0, 0.0
            ).astype(jnp.bfloat16)
        links = [pos_ref[c] - up(pos_ref[c]) for c in range(3)]
        rest_ref[...] = jnp.sqrt(dot3(links, links))

    ring = [tuple(sign if a == axis else 0 for a in range(3)) for axis in (0, 1) for sign in (1, -1)]

    def tell():
        for number, offset in enumerate(ring):
            pl.semaphore_signal(
                token.at[number], inc=1, device_id=at(offset), device_id_type=MESH
            )

    def hear():
        for number in range(len(ring)):
            pl.semaphore_wait(token.at[number], 1)

    def coord_copies():
        copies = []
        for number, zone in enumerate(ZONES):
            source = coord_x if number == 0 else coord_m.at[0 if number < 3 else 1]
            target = got_x if number == 0 else got_m.at[number - 1]
            copies.append(
                pltpu.make_async_remote_copy(
                    src_ref=source,
                    dst_ref=target,
                    send_sem=c_send.at[number],
                    recv_sem=c_recv.at[number],
                    device_id=at(tuple(-z for z in zone)),
                    device_id_type=MESH,
                )
            )
        return copies

    def force_copies():
        copies = []
        for number, zone in enumerate(ZONES):
            source = force_x if number == 0 else force_m.at[0 if number < 3 else 1]
            target = ret_x if number == 0 else ret_m.at[number - 1]
            copies.append(
                pltpu.make_async_remote_copy(
                    src_ref=source,
                    dst_ref=target,
                    send_sem=f_send.at[number],
                    recv_sem=f_recv.at[number],
                    device_id=at(zone),
                    device_id_type=MESH,
                )
            )
        return copies

    def step(t, carry):
        send_x = jnp.broadcast_to(send_ids[pl.ds(0, 1), :], (8, 128))
        send_m = jnp.maximum(jnp.broadcast_to(send_ids[pl.ds(1, 1), :], (8, 128)), 0)
        home = [cur[pl.ds(8 * c, 8), :] for c in range(3)]
        chosen = [pick(x, send_m) for x in home]
        in_zone = [(lane >= a) & (lane < b) for a, b in ((0, 16), (16, 24), (24, 40), (40, 48), (48, 49), (49, 50))]
        for c, length in enumerate((CX, CY, CZ)):
            shifted = None
            for number in range(1, 7):
                if ZONES[number][c]:
                    mask = in_zone[number - 1]
                    shifted = mask if shifted is None else shifted | mask
            chosen[c] = chosen[c] + jnp.where(shifted, F32(length), 0.0)
        one, two = pack(chosen)
        coord_m[0] = one
        coord_m[1] = two
        copies = coord_copies()
        for copy in copies[:0:-1]:
            copy.start()
        for c in range(3):
            value = pick(home[c], send_x)
            coord_x[pl.ds(8 * c, 8), :] = value + F32(CX) if c == 0 else value
        copies[0].start()

        pl.when(t == 0)(prepare)

        @pl.when(t > 0)
        def _():
            hear()

        tell()

        index = [[ids[pl.ds(16 * side + 8 * h, 8), :] for h in range(2)] for side in range(2)]
        low = [[index[s][h] & 127 for h in range(2)] for s in range(2)]
        for r in range(24):
            source = jnp.broadcast_to(cur[pl.ds(r, 1), :], (8, 128))
            for s in range(2):
                for h in range(2):
                    pair_x[s, h, r] = pick(source, low[s][h])

        in_home = [[index[s][h] < 128 for h in range(2)] for s in range(2)]
        in_x = [[index[s][h] < 256 for h in range(2)] for s in range(2)]
        copies[0].wait_recv()
        for r in range(24):
            source = jnp.broadcast_to(got_x[pl.ds(r, 1), :], (8, 128))
            for s in range(2):
                for h in range(2):
                    pair_x[s, h, r] = jnp.where(
                        in_home[s][h], pair_x[s, h, r], pick(source, low[s][h])
                    )

        for number in (2, 1, 5, 4, 3, 6):
            copies[number].wait_recv()
        blocks = unpack([got_m[n] for n in range(6)])
        for c in range(3):
            near[pl.ds(8 * c, 8), :] = blocks[c]
        for r in range(24):
            source = jnp.broadcast_to(near[pl.ds(r, 1), :], (8, 128))
            for s in range(2):
                for h in range(2):
                    pair_x[s, h, r] = jnp.where(
                        in_x[s][h], pair_x[s, h, r], pick(source, low[s][h])
                    )

        energy = jnp.zeros((8, 128), F32)
        for h in range(2):
            usable = jnp.where(index[0][h] == CL_PAD, 0.0, 1.0)
            distinct = jnp.where(index[0][h] == index[1][h], 0.0, usable)
            second = [[None] * 3 for _ in range(8)]
            for k in range(8):
                xi = [pair_x[0, h, 8 * c + k] for c in range(3)]
                first = [None] * 3
                for l in range(8):
                    d = [xi[c] - pair_x[1, h, 8 * c + l] for c in range(3)]
                    u = jnp.maximum((usable if k < l else distinct) - dot3(d, d), 0.0)
                    uu = u * u
                    energy = energy + uu * u
                    for c in range(3):
                        push = uu * d[c]
                        first[c] = push if l == 0 else first[c] + push
                        second[l][c] = push if k == 0 else second[l][c] + push
                for c in range(3):
                    pair_f[pl.ds((8 * c + k) * 16 + 8 * h, 8), :] = first[c]
            for l in range(8):
                for c in range(3):
                    pair_f[pl.ds(384 + (8 * c + l) * 16 + 8 * h, 8), :] = second[l][c]

        left = jnp.concatenate(
            [
                halves(pair_f[pl.ds(384 * side + g, 24, stride=16), :])
                for side in range(2)
                for g in range(GROUPS)
            ],
            axis=1,
        )

        @pl.when(t > 0)
        def _():
            for copy in force_copies():
                copy.wait_send()

        halo = jnp.dot(left, table[:, pl.ds(256, 128)], preferred_element_type=F32)
        halo = halo[:24] + halo[24:]
        one, two = pack([halo[8 * c : 8 * c + 8] for c in range(3)])
        force_m[0] = one
        force_m[1] = two
        returns = force_copies()
        for copy in returns[:0:-1]:
            copy.start()
        own = jnp.dot(left, table[:, pl.ds(0, 256)], preferred_element_type=F32)
        own = own[:24] + own[24:]
        force_x[...] = own[:, 128:]
        own = own[:, :128]
        returns[0].start()
        hear()

        @pl.when(t < ITERS)
        def _():
            tell()

        total = jnp.sum(jnp.sum(energy, axis=0, keepdims=True), axis=1, keepdims=True)
        row[...] = jnp.where(lanes(1) == 2 * t - 2, 2.0 * total, row[...])
        for copy in copies:
            copy.wait_send()
        for number in (2, 1, 0, 5, 4, 3, 6):
            returns[number].wait_recv()
        blocks = unpack([ret_m[n] for n in range(6)])
        came = jnp.concatenate([ret_x[...], jnp.concatenate(blocks, axis=0)], axis=1)
        came = jnp.dot(halves(came), back[...], preferred_element_type=F32)
        force = own + came[:24] + came[24:]
        force = [0.5 * time_step * force[8 * c : 8 * c + 8] for c in range(3)]

        again = jnp.where(t > 0, 1.0, 0.0).astype(F32)
        speed = [half_ref[pl.ds(8 * c, 8), :] + again * force[c] for c in range(3)]
        total = jnp.sum(jnp.sum(dot3(speed, speed), axis=0, keepdims=True), axis=1, keepdims=True)
        row[...] = jnp.where(lanes(1) == 2 * t - 1, 0.5 * total, row[...])

        @pl.when(t < ITERS)
        def _():
            flags = flag8[...]
            half = [speed[c] + force[c] for c in range(3)]
            before = [cur[pl.ds(8 * c, 8), :] for c in range(3)]
            moved = constrain(
                before,
                [x + time_step * v for x, v in zip(before, half)],
                rest_ref[...],
                flags,
                flags * up(flags),
            )
            for c in range(3):
                cur[pl.ds(8 * c, 8), :] = moved[c]
                half_ref[pl.ds(8 * c, 8), :] = (moved[c] - before[c]) / time_step

        @pl.when(t == ITERS)
        def _():
            for c in range(3):
                out_pos[c] = cur[pl.ds(8 * c, 8), :]
                out_vel[c] = speed[c]

        return carry

    lax.fori_loop(0, ITERS + 1, step, 0)
    for copy in force_copies():
        copy.wait_send()

    def gather(source, slots, offsets, own, send, recv):
        offsets = sorted(
            offsets, key=lambda o: -sum(min(o[a], sizes[a] - o[a]) for a in range(3))
        )
        copies = []
        for number, offset in enumerate(offsets):
            copies.append(
                pltpu.make_async_remote_copy(
                    src_ref=source,
                    dst_ref=slots.at[own],
                    send_sem=send.at[number],
                    recv_sem=recv.at[number],
                    device_id=at(offset),
                    device_id_type=MESH,
                )
            )
        for copy in copies:
            copy.start()
        slots[own] = source[...]
        for copy in copies:
            copy.wait_recv()
        total = slots[0]
        for n in range(1, slots.shape[0]):
            total = total + slots[n]
        return total, copies

    offsets = [
        (0, y, z) for y in range(sizes[1]) for z in range(sizes[2]) if (y, z) != (0, 0)
    ]
    total, first_copies = gather(row, plane, offsets, me[1] * sizes[2] + me[2], p_send, p_recv)
    mid[...] = total
    offsets = [(x, 0, 0) for x in range(1, sizes[0])]
    total, second_copies = gather(mid, line, offsets, me[0], l_send, l_recv)
    total = total / F32(8 * 128 * sizes[0] * sizes[1] * sizes[2])
    for t in range(ITERS):
        out_en[pl.ds(t, 1), :] = total[:, 2 * t : 2 * t + 2]
    for copy in first_copies + second_copies:
        copy.wait_send()


CL_PAD = 306


def on_device(sizes, positions, velocities, send_list, pair_list, constraint_flags):
    dma = pltpu.SemaphoreType.DMA
    vmem = pltpu.VMEM
    plane = sizes[1] * sizes[2]
    return pl.pallas_call(
        functools.partial(kernel, sizes),
        out_shape=(
            jax.ShapeDtypeStruct((3, 8, 128), F32),
            jax.ShapeDtypeStruct((3, 8, 128), F32),
            jax.ShapeDtypeStruct((ITERS, 2), F32),
        ),
        in_specs=[pl.BlockSpec(memory_space=vmem)] * 5,
        out_specs=[pl.BlockSpec(memory_space=vmem)] * 3,
        scratch_shapes=[
            vmem((24, 128), F32),
            vmem((24, 128), F32),
            vmem((8, 128), F32),
            vmem((32, 128), jnp.int32),
            vmem((8, 128), jnp.int32),
            vmem((8, 128), F32),
            vmem((2 * SLOTS, 384), jnp.bfloat16),
            vmem((256, 128), jnp.bfloat16),
            vmem((24, 128), F32),
            vmem((2, 2, 24, 8, 128), F32),
            vmem((768, 128), F32),
            vmem((24, 128), F32),
            vmem((2, 8, 128), F32),
            vmem((24, 128), F32),
            vmem((2, 8, 128), F32),
            vmem((24, 128), F32),
            vmem((6, 8, 128), F32),
            vmem((24, 128), F32),
            vmem((6, 8, 128), F32),
            vmem((1, 128), F32),
            vmem((plane, 1, 128), F32),
            vmem((1, 128), F32),
            vmem((sizes[0], 1, 128), F32),
            dma((7,)),
            dma((7,)),
            dma((7,)),
            dma((7,)),
            dma((plane - 1,)),
            dma((plane - 1,)),
            dma((sizes[0] - 1,)),
            dma((sizes[0] - 1,)),
            pltpu.SemaphoreType.REGULAR((4,)),
        ],
        compiler_params=pltpu.CompilerParams(collective_id=0, has_side_effects=True),
        name="membrane",
    )(positions, velocities, send_list.reshape(1, -1), pair_list, constraint_flags)


def solution(mesh):
    sizes = tuple(mesh.shape[a] for a in AXES)
    spec = ("runs", "gx", "gy", "gz")
    return jax.shard_map(
        functools.partial(on_device, sizes),
        mesh=mesh,
        in_specs=(
            P(None, None, spec),
            P(None, None, spec),
            P(spec),
            P(None, spec),
            P(None, spec),
        ),
        out_specs=(P(None, None, spec), P(None, None, spec), P("runs", None)),
        check_vma=False,
    )
```

```python
import functools

import jax
import jax.numpy as jnp
from jax import lax
from jax.experimental import pallas as pl
from jax.experimental.pallas import tpu as pltpu
from jax.sharding import PartitionSpec as P

CX, CY, CZ = 1, 8, 16
ITERS = 3
NORDER = 4
time_step = 0.02
root_half = 0.7071067811865476
MESH = pl.DeviceIdType.MESH
ZONES = ((1, 0, 0), (0, 1, 0), (0, 0, 1), (1, 1, 0), (1, 0, 1), (0, 1, 1), (1, 1, 1))
AXES = ("gx", "gy", "gz")
FIRST, SECOND = 24, 26
FAR, NEAR = (3, 6, 4, 5), (1, 2)
GROUPS = 14
SLOTS = 1792
F32 = jnp.float32


def roll(x, by, axis):
    size = x.shape[axis]
    by = by % size
    return x if by == 0 else pltpu.roll(x, by, axis)


def partners(sizes):
    found = set()
    for zone in ZONES:
        for sign in (1, -1):
            found.add(tuple((sign * z) % n for z, n in zip(zone, sizes)))
    found.discard((0, 0, 0))
    return sorted(found)


def lanes(rows=8):
    return lax.broadcasted_iota(jnp.int32, (rows, 128), 1)


def side_by_side(parts, first, width):
    lane = lanes()
    return jnp.where(
        lane < first + width,
        parts[0],
        jnp.where(lane < first + 2 * width, roll(parts[1], width, 1), roll(parts[2], 2 * width, 1)),
    )


def unpack(received):
    lane = lanes()
    within = lax.rem(lane, FIRST)
    one = jnp.where(within < 16, received[0], received[1])
    within = lax.rem(lane + (SECOND - FIRST % SECOND), SECOND)
    two = jnp.where(
        within < 16,
        received[2],
        jnp.where(
            within < 24, received[3], jnp.where(within < 25, received[4], received[5])
        ),
    )
    blocks = []
    for c in range(3):
        block = jnp.where(lane < FIRST, roll(one, -FIRST * c, 1), roll(two, -SECOND * c, 1))
        blocks.append(jnp.where(lane < FIRST + SECOND, block, 0.0))
    return blocks


def place(side, g):
    return 8 * side + g if g < 8 else 16 + (GROUPS - 8) * side + g - 8


def halves(value):
    high = value.astype(jnp.bfloat16).astype(F32)
    return jnp.concatenate([high, value - high], axis=0).astype(jnp.bfloat16)


def pick(table, index):
    return jnp.take_along_axis(table, index, axis=1, mode="promise_in_bounds")


def up(x):
    return roll(x, -1, 0)


def down(x):
    return roll(x, 1, 0)


def expand(coupling, coupling_down, source):
    series = source
    result = source
    for _ in range(NORDER):
        series = coupling_down * down(series) + coupling * up(series)
        result = result + series
    return result


def dot3(a, b):
    return a[0] * b[0] + a[1] * b[1] + a[2] * b[2]


def constrain(previous, updated, rest, flags, flags_pair):
    old = [x - up(x) for x in previous]
    length = jnp.maximum(jnp.sqrt(dot3(old, old)), 0.2)
    direction = [x / length for x in old]
    coupling = 0.5 * dot3(direction, [up(x) for x in direction]) * flags_pair
    coupling_down = down(coupling)
    links = [x - up(x) for x in updated]
    solution = expand(
        coupling, coupling_down, flags * root_half * (dot3(direction, links) - rest)
    )
    shifts = [x * (root_half * solution) for x in direction]
    updated = [x - s + down(s) for x, s in zip(updated, shifts)]
    links = [x - up(x) for x in updated]
    squared = dot3(links, links)
    target = jnp.sqrt(jnp.maximum(2.0 * rest * rest - squared, 0.25 * rest * rest))
    solution = expand(coupling, coupling_down, flags * root_half * (rest - target))
    shifts = [x * (root_half * solution) for x in direction]
    return [x - s + down(s) for x, s in zip(updated, shifts)]


def kernel(
    sizes,
    pos_in,
    vel_in,
    send_in,
    pair_in,
    flag_in,
    out_pos,
    out_vel,
    out_en,
    cur,
    half_ref,
    rest_ref,
    ids,
    send_ids,
    flag8,
    table,
    back,
    near,
    pair_x,
    pair_f,
    coord_x,
    coord_m,
    force_x,
    force_m,
    got_x,
    got_m,
    ret_x,
    ret_m,
    row,
    plane,
    mid,
    line,
    c_send,
    c_recv,
    f_send,
    f_recv,
    p_send,
    p_recv,
    l_send,
    l_recv,
    token,
    pos_ref,
    vel_ref,
    send_ref,
    pair_ref,
    flag_ref,
    loaded,
):
    me = tuple(lax.axis_index(a) for a in AXES)

    def at(offset):
        return {
            a: lax.rem(me[i] + (offset[i] % sizes[i]), sizes[i])
            for i, a in enumerate(AXES)
            if offset[i] % sizes[i]
        }

    loads = [
        pltpu.make_async_copy(source, target, loaded.at[n])
        for n, (source, target) in enumerate(
            (
                (send_in, send_ref),
                (pos_in, pos_ref),
                (pair_in, pair_ref),
                (vel_in, vel_ref),
                (flag_in, flag_ref),
            )
        )
    ]
    for load in loads:
        load.start()
    barrier = pltpu.get_barrier_semaphore()
    others = partners(sizes)
    for offset in others:
        pl.semaphore_signal(barrier, inc=1, device_id=at(offset), device_id_type=MESH)

    lane = lanes()
    row[...] = jnp.zeros(row.shape, F32)
    loads[0].wait()
    loads[1].wait()
    send_ids[...] = jnp.full(send_ids.shape, -1, jnp.int32)
    send_ids[pl.ds(0, 1), :] = send_ref[:, pl.ds(0, 128)]
    send_ids[pl.ds(1, 1), pl.ds(0, FIRST + SECOND)] = send_ref[:, pl.ds(128, FIRST + SECOND)]
    for c in range(3):
        cur[pl.ds(8 * c, 8), :] = pos_ref[c]

    pl.semaphore_wait(barrier, len(others))

    def prepare():
        for load in loads[2:]:
            load.wait()
        for c in range(3):
            half_ref[pl.ds(8 * c, 8), :] = vel_ref[c]
        ids[...] = jnp.full(ids.shape, CL_PAD, jnp.int32)
        for g in range(GROUPS):
            for side in range(2):
                ids[pl.ds(16 * side + g, 1), :] = pair_ref[pl.ds(side, 1), pl.ds(128 * g, 128)]
        flag8[...] = jnp.zeros(flag8.shape, F32)
        flag8[pl.ds(0, 7), :] = flag_ref[...].astype(F32)
        columns = jnp.transpose(ids[...].astype(F32))
        send_columns = jnp.transpose(send_ids[...].astype(F32))
        wide = lax.broadcasted_iota(jnp.int32, (128, 384), 1).astype(F32)
        for side in range(2):
            value = 12.0 if side == 0 else -12.0
            for g in range(GROUPS):
                column = columns[:, 16 * side + g : 16 * side + g + 1]
                table[pl.ds(128 * place(side, g), 128), :] = jnp.where(
                    wide == column, value, 0.0
                ).astype(jnp.bfloat16)
        for b in range(2):
            back[pl.ds(128 * b, 128), :] = jnp.where(
                wide[:, :128] == send_columns[:, b : b + 1], 1.0, 0.0
            ).astype(jnp.bfloat16)
        links = [pos_ref[c] - up(pos_ref[c]) for c in range(3)]
        rest_ref[...] = jnp.sqrt(dot3(links, links))

    ring = [tuple(sign if a == axis else 0 for a in range(3)) for axis in (0, 1) for sign in (1, -1)]

    def tell():
        for number, offset in enumerate(ring):
            pl.semaphore_signal(
                token.at[number], inc=1, device_id=at(offset), device_id_type=MESH
            )

    def hear():
        for number in range(len(ring)):
            pl.semaphore_wait(token.at[number], 1)

    def coord_copies():
        copies = []
        for number, zone in enumerate(ZONES):
            source = coord_x if number == 0 else coord_m.at[0 if number < 3 else 1]
            target = got_x if number == 0 else got_m.at[number - 1]
            copies.append(
                pltpu.make_async_remote_copy(
                    src_ref=source,
                    dst_ref=target,
                    send_sem=c_send.at[number],
                    recv_sem=c_recv.at[number],
                    device_id=at(tuple(-z for z in zone)),
                    device_id_type=MESH,
                )
            )
        return copies

    def force_copies():
        copies = []
        for number, zone in enumerate(ZONES):
            source = force_x if number == 0 else force_m.at[0 if number < 3 else 1]
            target = ret_x if number == 0 else ret_m.at[number - 1]
            copies.append(
                pltpu.make_async_remote_copy(
                    src_ref=source,
                    dst_ref=target,
                    send_sem=f_send.at[number],
                    recv_sem=f_recv.at[number],
                    device_id=at(zone),
                    device_id_type=MESH,
                )
            )
        return copies

    def step(t, carry):
        send_x = jnp.broadcast_to(send_ids[pl.ds(0, 1), :], (8, 128))
        send_m = jnp.maximum(jnp.broadcast_to(send_ids[pl.ds(1, 1), :], (8, 128)), 0)
        home = [cur[pl.ds(8 * c, 8), :] for c in range(3)]
        chosen = [pick(x, send_m) for x in home]
        in_zone = [(lane >= a) & (lane < b) for a, b in ((0, 16), (16, 24), (24, 40), (40, 48), (48, 49), (49, 50))]
        for c, length in enumerate((CX, CY, CZ)):
            shifted = None
            for number in range(1, 7):
                if ZONES[number][c]:
                    mask = in_zone[number - 1]
                    shifted = mask if shifted is None else shifted | mask
            chosen[c] = chosen[c] + jnp.where(shifted, F32(length), 0.0)
        copies = coord_copies()
        coord_m[1] = side_by_side(chosen, FIRST, SECOND)
        for number in FAR:
            copies[number].start()
        coord_m[0] = side_by_side(chosen, 0, FIRST)
        for number in NEAR:
            copies[number].start()
        for c in range(3):
            value = pick(home[c], send_x)
            coord_x[pl.ds(8 * c, 8), :] = value + F32(CX) if c == 0 else value
        copies[0].start()

        pl.when(t == 0)(prepare)

        @pl.when(t > 0)
        def _():
            hear()
            for copy in force_copies():
                copy.wait_send()

        tell()

        index = [[ids[pl.ds(16 * side + 8 * h, 8), :] for h in range(2)] for side in range(2)]
        low = [[index[s][h] & 127 for h in range(2)] for s in range(2)]
        for r in range(24):
            source = jnp.broadcast_to(cur[pl.ds(r, 1), :], (8, 128))
            for s in range(2):
                for h in range(2):
                    pair_x[s, h, r] = pick(source, low[s][h])

        in_home = [[index[s][h] < 128 for h in range(2)] for s in range(2)]
        in_x = [[index[s][h] < 256 for h in range(2)] for s in range(2)]
        copies[0].wait_recv()
        for r in range(24):
            source = jnp.broadcast_to(got_x[pl.ds(r, 1), :], (8, 128))
            for s in range(2):
                for h in range(2):
                    pair_x[s, h, r] = jnp.where(
                        in_home[s][h], pair_x[s, h, r], pick(source, low[s][h])
                    )

        for number in NEAR + FAR:
            copies[number].wait_recv()
        blocks = unpack([got_m[n] for n in range(6)])
        for c in range(3):
            near[pl.ds(8 * c, 8), :] = blocks[c]
        for r in range(24):
            source = jnp.broadcast_to(near[pl.ds(r, 1), :], (8, 128))
            for s in range(2):
                for h in range(2):
                    pair_x[s, h, r] = jnp.where(
                        in_x[s][h], pair_x[s, h, r], pick(source, low[s][h])
                    )

        energy = jnp.zeros((8, 128), F32)
        lefts = []
        halo = None
        for h in range(2):
            usable = jnp.where(index[0][h] == CL_PAD, 0.0, 1.0)
            distinct = jnp.where(index[0][h] == index[1][h], 0.0, usable)
            second = [[None] * 3 for _ in range(8)]
            for k in range(8):
                xi = [pair_x[0, h, 8 * c + k] for c in range(3)]
                first = [None] * 3
                for l in range(8):
                    d = [xi[c] - pair_x[1, h, 8 * c + l] for c in range(3)]
                    u = jnp.maximum((usable if k < l else distinct) - dot3(d, d), 0.0)
                    uu = u * u
                    energy = energy + uu * u
                    for c in range(3):
                        push = uu * d[c]
                        first[c] = push if l == 0 else first[c] + push
                        second[l][c] = push if k == 0 else second[l][c] + push
                for c in range(3):
                    pair_f[pl.ds((8 * c + k) * 16 + 8 * h, 8), :] = first[c]
            for l in range(8):
                for c in range(3):
                    pair_f[pl.ds(384 + (8 * c + l) * 16 + 8 * h, 8), :] = second[l][c]

            groups = range(8) if h == 0 else range(8, GROUPS)
            left = jnp.concatenate(
                [
                    halves(pair_f[pl.ds(384 * side + g, 24, stride=16), :])
                    for side in range(2)
                    for g in groups
                ],
                axis=1,
            )
            lefts.append(left)
            part = jnp.dot(
                left,
                table[pl.ds(2048 * h, left.shape[1]), pl.ds(128, 256)],
                preferred_element_type=F32,
            )
            halo = part if h == 0 else halo + part

        halo = halo[:24] + halo[24:]
        returns = force_copies()
        beyond = [halo[8 * c : 8 * c + 8, 128:] for c in range(3)]
        force_m[1] = side_by_side(beyond, FIRST, SECOND)
        for number in FAR:
            returns[number].start()
        force_m[0] = side_by_side(beyond, 0, FIRST)
        for number in NEAR:
            returns[number].start()
        force_x[...] = halo[:, :128]
        returns[0].start()
        own = None
        for h in range(2):
            part = jnp.dot(
                lefts[h],
                table[pl.ds(2048 * h, lefts[h].shape[1]), pl.ds(0, 128)],
                preferred_element_type=F32,
            )
            own = part if h == 0 else own + part
        own = own[:24] + own[24:]
        hear()

        @pl.when(t < ITERS)
        def _():
            tell()

        total = jnp.sum(jnp.sum(energy, axis=0, keepdims=True), axis=1, keepdims=True)
        row[...] = jnp.where(lanes(1) == t - 1, 2.0 * total, row[...])
        for copy in copies:
            copy.wait_send()
        for number in (0,) + NEAR + FAR:
            returns[number].wait_recv()
        blocks = unpack([ret_m[n] for n in range(6)])
        came = jnp.concatenate([ret_x[...], jnp.concatenate(blocks, axis=0)], axis=1)
        came = jnp.dot(halves(came), back[...], preferred_element_type=F32)
        force = own + came[:24] + came[24:]
        force = [0.5 * time_step * force[8 * c : 8 * c + 8] for c in range(3)]

        again = jnp.where(t > 0, 1.0, 0.0).astype(F32)
        speed = [half_ref[pl.ds(8 * c, 8), :] + again * force[c] for c in range(3)]
        total = jnp.sum(jnp.sum(dot3(speed, speed), axis=0, keepdims=True), axis=1, keepdims=True)
        row[...] = jnp.where(lanes(1) == KINETIC + t - 1, 0.5 * total, row[...])

        @pl.when(t < ITERS)
        def _():
            flags = flag8[...]
            half = [speed[c] + force[c] for c in range(3)]
            before = [cur[pl.ds(8 * c, 8), :] for c in range(3)]
            moved = constrain(
                before,
                [x + time_step * v for x, v in zip(before, half)],
                rest_ref[...],
                flags,
                flags * up(flags),
            )
            for c in range(3):
                cur[pl.ds(8 * c, 8), :] = moved[c]
                half_ref[pl.ds(8 * c, 8), :] = (moved[c] - before[c]) / time_step

        @pl.when(t == ITERS)
        def _():
            for c in range(3):
                out_pos[c] = cur[pl.ds(8 * c, 8), :]
                out_vel[c] = speed[c]

        return carry

    lax.fori_loop(0, ITERS + 1, step, 0)
    for copy in force_copies():
        copy.wait_send()

    def gather(source, slots, offsets, own, send, recv):
        offsets = sorted(
            offsets, key=lambda o: -sum(min(o[a], sizes[a] - o[a]) for a in range(3))
        )
        copies = []
        for number, offset in enumerate(offsets):
            copies.append(
                pltpu.make_async_remote_copy(
                    src_ref=source,
                    dst_ref=slots.at[own],
                    send_sem=send.at[number],
                    recv_sem=recv.at[number],
                    device_id=at(offset),
                    device_id_type=MESH,
                )
            )
        for copy in copies:
            copy.start()
        slots[own] = source[...]
        for copy in copies:
            copy.wait_recv()
        total = slots[0]
        for n in range(1, slots.shape[0]):
            total = total + slots[n]
        return total, copies

    offsets = [
        (0, y, z) for y in range(sizes[1]) for z in range(sizes[2]) if (y, z) != (0, 0)
    ]
    total, first_copies = gather(row, plane, offsets, me[1] * sizes[2] + me[2], p_send, p_recv)
    mid[...] = total
    offsets = [(x, 0, 0) for x in range(1, sizes[0])]
    total, second_copies = gather(mid, line, offsets, me[0], l_send, l_recv)
    out_en[...] = total
    for copy in first_copies + second_copies:
        copy.wait_send()


CL_PAD = 306
KINETIC = 8
VMEM_LIMIT = 12 << 20


def finish(beads, pos_ref, vel_ref, sum_ref, out_pos, out_vel, out_en, energy, stored):
    stores = [
        pltpu.make_async_copy(source, target, stored.at[n])
        for n, (source, target) in enumerate(
            ((pos_ref, out_pos), (vel_ref, out_vel), (energy, out_en))
        )
    ]
    stores[0].start()
    stores[1].start()
    total = sum_ref[...] / F32(beads)
    for n in range(2):
        energy[pl.ds(n, 1), :] = total[:, KINETIC * n : KINETIC * n + ITERS]
    stores[2].start()
    for store in stores:
        store.wait()


def on_device(sizes, positions, velocities, send_list, pair_list, constraint_flags):
    dma = pltpu.SemaphoreType.DMA
    vmem = pltpu.VMEM
    plane = sizes[1] * sizes[2]
    results = pl.pallas_call(
        functools.partial(kernel, sizes),
        out_shape=(
            jax.ShapeDtypeStruct((3, 8, 128), F32),
            jax.ShapeDtypeStruct((3, 8, 128), F32),
            jax.ShapeDtypeStruct((1, 128), F32),
        ),
        in_specs=[pl.BlockSpec(memory_space=pltpu.HBM)] * 5,
        out_specs=[pl.BlockSpec(memory_space=vmem)] * 3,
        scratch_shapes=[
            vmem((24, 128), F32),
            vmem((24, 128), F32),
            vmem((8, 128), F32),
            vmem((32, 128), jnp.int32),
            vmem((8, 128), jnp.int32),
            vmem((8, 128), F32),
            vmem((2 * SLOTS, 384), jnp.bfloat16),
            vmem((256, 128), jnp.bfloat16),
            vmem((24, 128), F32),
            vmem((2, 2, 24, 8, 128), F32),
            vmem((768, 128), F32),
            vmem((24, 128), F32),
            vmem((2, 8, 128), F32),
            vmem((24, 128), F32),
            vmem((2, 8, 128), F32),
            vmem((24, 128), F32),
            vmem((6, 8, 128), F32),
            vmem((24, 128), F32),
            vmem((6, 8, 128), F32),
            vmem((1, 128), F32),
            vmem((plane, 1, 128), F32),
            vmem((1, 128), F32),
            vmem((sizes[0], 1, 128), F32),
            dma((7,)),
            dma((7,)),
            dma((7,)),
            dma((7,)),
            dma((plane - 1,)),
            dma((plane - 1,)),
            dma((sizes[0] - 1,)),
            dma((sizes[0] - 1,)),
            pltpu.SemaphoreType.REGULAR((4,)),
            vmem((3, 8, 128), F32),
            vmem((3, 8, 128), F32),
            vmem((1, 178), jnp.int32),
            vmem((2, SLOTS), jnp.int32),
            vmem((7, 128), jnp.int32),
            dma((5,)),
        ],
        compiler_params=pltpu.CompilerParams(
            collective_id=0, has_side_effects=True, vmem_limit_bytes=VMEM_LIMIT
        ),
        name="membrane",
    )(
        *[
            pltpu.with_memory_space_constraint(x, pltpu.HBM)
            for x in (
                positions,
                velocities,
                send_list.reshape(1, -1),
                pair_list,
                constraint_flags,
            )
        ]
    )
    position, velocity, energies = pl.pallas_call(
        functools.partial(finish, 8 * 128 * sizes[0] * sizes[1] * sizes[2]),
        out_shape=(
            jax.ShapeDtypeStruct((3, 8, 128), F32),
            jax.ShapeDtypeStruct((3, 8, 128), F32),
            jax.ShapeDtypeStruct((2, ITERS), F32),
        ),
        in_specs=[pl.BlockSpec(memory_space=vmem)] * 3,
        out_specs=[pl.BlockSpec(memory_space=pltpu.HBM)] * 3,
        scratch_shapes=[vmem((2, ITERS), F32), dma((3,))],
        compiler_params=pltpu.CompilerParams(vmem_limit_bytes=1 << 20),
        name="finish",
    )(*results)
    return position, velocity, energies.T


def solution(mesh):
    sizes = tuple(mesh.shape[a] for a in AXES)
    spec = ("runs", "gx", "gy", "gz")
    return jax.shard_map(
        functools.partial(on_device, sizes),
        mesh=mesh,
        in_specs=(
            P(None, None, spec),
            P(None, None, spec),
            P(spec),
            P(None, spec),
            P(None, spec),
        ),
        out_specs=(P(None, None, spec), P(None, None, spec), P("runs", None)),
        check_vma=False,
    )
```

```python
import functools

import jax
import jax.numpy as jnp
from jax import lax
from jax.experimental import pallas as pl
from jax.experimental.pallas import tpu as pltpu
from jax.sharding import PartitionSpec as P

CX, CY, CZ = 1, 8, 16
ITERS = 3
NORDER = 4
time_step = 0.02
root_half = 0.7071067811865476
MESH = pl.DeviceIdType.MESH
ZONES = ((1, 0, 0), (0, 1, 0), (0, 0, 1), (1, 1, 0), (1, 0, 1), (0, 1, 1), (1, 1, 1))
AXES = ("gx", "gy", "gz")
FIRST, SECOND = 24, 26
FAR, NEAR = (3, 6, 4, 5), (1, 2)
GROUPS = 14
SLOTS = 1792
F32 = jnp.float32


def roll(x, by, axis):
    size = x.shape[axis]
    by = by % size
    return x if by == 0 else pltpu.roll(x, by, axis)


def partners(sizes):
    found = set()
    for zone in ZONES:
        for sign in (1, -1):
            found.add(tuple((sign * z) % n for z, n in zip(zone, sizes)))
    found.discard((0, 0, 0))
    return sorted(found)


def lanes(rows=8):
    return lax.broadcasted_iota(jnp.int32, (rows, 128), 1)


def side_by_side(parts, first, width):
    lane = lanes()
    return jnp.where(
        lane < first + width,
        parts[0],
        jnp.where(lane < first + 2 * width, roll(parts[1], width, 1), roll(parts[2], 2 * width, 1)),
    )


def unpack(received):
    lane = lanes()
    within = lax.rem(lane, FIRST)
    one = jnp.where(within < 16, received[0], received[1])
    within = lax.rem(lane + (SECOND - FIRST % SECOND), SECOND)
    two = jnp.where(
        within < 16,
        received[2],
        jnp.where(
            within < 24, received[3], jnp.where(within < 25, received[4], received[5])
        ),
    )
    blocks = []
    for c in range(3):
        block = jnp.where(lane < FIRST, roll(one, -FIRST * c, 1), roll(two, -SECOND * c, 1))
        blocks.append(jnp.where(lane < FIRST + SECOND, block, 0.0))
    return blocks


def place(side, g):
    return 8 * side + g if g < 8 else 16 + (GROUPS - 8) * side + g - 8


def halves(value):
    high = value.astype(jnp.bfloat16).astype(F32)
    return jnp.concatenate([high, value - high], axis=0).astype(jnp.bfloat16)


def pick(table, index):
    return jnp.take_along_axis(table, index, axis=1, mode="promise_in_bounds")


def up(x):
    return roll(x, -1, 0)


def down(x):
    return roll(x, 1, 0)


def expand(coupling, coupling_down, source):
    series = source
    result = source
    for _ in range(NORDER):
        series = coupling_down * down(series) + coupling * up(series)
        result = result + series
    return result


def dot3(a, b):
    return a[0] * b[0] + a[1] * b[1] + a[2] * b[2]


def constrain(previous, updated, rest, flags, flags_pair):
    old = [x - up(x) for x in previous]
    length = jnp.maximum(jnp.sqrt(dot3(old, old)), 0.2)
    direction = [x / length for x in old]
    coupling = 0.5 * dot3(direction, [up(x) for x in direction]) * flags_pair
    coupling_down = down(coupling)
    links = [x - up(x) for x in updated]
    solution = expand(
        coupling, coupling_down, flags * root_half * (dot3(direction, links) - rest)
    )
    shifts = [x * (root_half * solution) for x in direction]
    updated = [x - s + down(s) for x, s in zip(updated, shifts)]
    links = [x - up(x) for x in updated]
    squared = dot3(links, links)
    target = jnp.sqrt(jnp.maximum(2.0 * rest * rest - squared, 0.25 * rest * rest))
    solution = expand(coupling, coupling_down, flags * root_half * (rest - target))
    shifts = [x * (root_half * solution) for x in direction]
    return [x - s + down(s) for x, s in zip(updated, shifts)]


def kernel(
    sizes,
    pos_in,
    vel_in,
    send_in,
    pair_in,
    flag_in,
    out_pos,
    out_vel,
    out_en,
    cur,
    half_ref,
    rest_ref,
    ids,
    send_ids,
    flag8,
    table,
    back,
    near,
    pair_x,
    pair_f,
    coord_x,
    coord_m,
    force_x,
    force_m,
    got_x,
    got_m,
    ret_x,
    ret_m,
    row,
    plane,
    mid,
    line,
    c_send,
    c_recv,
    f_send,
    f_recv,
    p_send,
    p_recv,
    l_send,
    l_recv,
    token,
    pos_ref,
    vel_ref,
    send_ref,
    pair_ref,
    flag_ref,
    loaded,
    blocks_ref,
    rows_ref,
    speed_ref,
):
    me = tuple(lax.axis_index(a) for a in AXES)

    def at(offset):
        return {
            a: lax.rem(me[i] + (offset[i] % sizes[i]), sizes[i])
            for i, a in enumerate(AXES)
            if offset[i] % sizes[i]
        }

    loads = [
        pltpu.make_async_copy(source, target, loaded.at[n])
        for n, (source, target) in enumerate(
            (
                (send_in, send_ref),
                (pos_in, pos_ref),
                (pair_in, pair_ref),
                (vel_in, vel_ref),
                (flag_in, flag_ref),
            )
        )
    ]
    for load in loads:
        load.start()
    barrier = pltpu.get_barrier_semaphore()
    others = partners(sizes)
    for offset in others:
        pl.semaphore_signal(barrier, inc=1, device_id=at(offset), device_id_type=MESH)

    lane = lanes()
    row[...] = jnp.zeros(row.shape, F32)
    loads[0].wait()
    loads[1].wait()
    send_ids[...] = jnp.full(send_ids.shape, -1, jnp.int32)
    send_ids[pl.ds(0, 1), :] = send_ref[:, pl.ds(0, 128)]
    send_ids[pl.ds(1, 1), pl.ds(0, FIRST + SECOND)] = send_ref[:, pl.ds(128, FIRST + SECOND)]
    for c in range(3):
        cur[pl.ds(8 * c, 8), :] = pos_ref[c]

    pl.semaphore_wait(barrier, len(others))

    def prepare():
        for load in loads[2:]:
            load.wait()
        for c in range(3):
            half_ref[pl.ds(8 * c, 8), :] = vel_ref[c]
        ids[...] = jnp.full(ids.shape, CL_PAD, jnp.int32)
        for g in range(GROUPS):
            for side in range(2):
                ids[pl.ds(16 * side + g, 1), :] = pair_ref[pl.ds(side, 1), pl.ds(128 * g, 128)]
        flag8[...] = jnp.zeros(flag8.shape, F32)
        flag8[pl.ds(0, 7), :] = flag_ref[...].astype(F32)
        columns = jnp.transpose(ids[...].astype(F32))
        send_columns = jnp.transpose(send_ids[...].astype(F32))
        wide = lax.broadcasted_iota(jnp.int32, (128, 384), 1).astype(F32)
        for side in range(2):
            value = 12.0 if side == 0 else -12.0
            for g in range(GROUPS):
                column = columns[:, 16 * side + g : 16 * side + g + 1]
                table[pl.ds(128 * place(side, g), 128), :] = jnp.where(
                    wide == column, value, 0.0
                ).astype(jnp.bfloat16)
        for b in range(2):
            back[pl.ds(128 * b, 128), :] = jnp.where(
                wide[:, :128] == send_columns[:, b : b + 1], 1.0, 0.0
            ).astype(jnp.bfloat16)
        links = [pos_ref[c] - up(pos_ref[c]) for c in range(3)]
        rest_ref[...] = jnp.sqrt(dot3(links, links))

    ring = [tuple(sign if a == axis else 0 for a in range(3)) for axis in (0, 1) for sign in (1, -1)]

    def tell():
        for number, offset in enumerate(ring):
            pl.semaphore_signal(
                token.at[number], inc=1, device_id=at(offset), device_id_type=MESH
            )

    def hear():
        for number in range(len(ring)):
            pl.semaphore_wait(token.at[number], 1)

    def coord_copies():
        copies = []
        for number, zone in enumerate(ZONES):
            source = coord_x if number == 0 else coord_m.at[0 if number < 3 else 1]
            target = got_x if number == 0 else got_m.at[number - 1]
            copies.append(
                pltpu.make_async_remote_copy(
                    src_ref=source,
                    dst_ref=target,
                    send_sem=c_send.at[0 if number == 0 else 1],
                    recv_sem=c_recv.at[0 if number == 0 else 1],
                    device_id=at(tuple(-z for z in zone)),
                    device_id_type=MESH,
                )
            )
        return copies

    def force_copies():
        copies = []
        for number, zone in enumerate(ZONES):
            source = force_x if number == 0 else force_m.at[0 if number < 3 else 1]
            target = ret_x if number == 0 else ret_m.at[number - 1]
            copies.append(
                pltpu.make_async_remote_copy(
                    src_ref=source,
                    dst_ref=target,
                    send_sem=f_send.at[0 if number == 0 else 1],
                    recv_sem=f_recv.at[0 if number == 0 else 1],
                    device_id=at(zone),
                    device_id_type=MESH,
                )
            )
        return copies

    def drain(sem, ref):
        pltpu.make_async_copy(ref, ref, sem).wait()

    def kinetic(speed, number):
        total = jnp.sum(
            jnp.sum(dot3(speed, speed), axis=0, keepdims=True), axis=1, keepdims=True
        )
        row[...] = jnp.where(lanes(1) == KINETIC + number, 0.5 * total, row[...])

    def step(t, carry):
        send_x = jnp.broadcast_to(send_ids[pl.ds(0, 1), :], (8, 128))
        send_m = jnp.maximum(jnp.broadcast_to(send_ids[pl.ds(1, 1), :], (8, 128)), 0)
        home = [cur[pl.ds(8 * c, 8), :] for c in range(3)]
        chosen = [pick(x, send_m) for x in home]
        in_zone = [(lane >= a) & (lane < b) for a, b in ((0, 16), (16, 24), (24, 40), (40, 48), (48, 49), (49, 50))]
        for c, length in enumerate((CX, CY, CZ)):
            shifted = None
            for number in range(1, 7):
                if ZONES[number][c]:
                    mask = in_zone[number - 1]
                    shifted = mask if shifted is None else shifted | mask
            chosen[c] = chosen[c] + jnp.where(shifted, F32(length), 0.0)
        copies = coord_copies()
        coord_m[1] = side_by_side(chosen, FIRST, SECOND)
        for number in FAR:
            copies[number].start()
        coord_m[0] = side_by_side(chosen, 0, FIRST)
        for number in NEAR:
            copies[number].start()
        for c in range(3):
            value = pick(home[c], send_x)
            coord_x[pl.ds(8 * c, 8), :] = value + F32(CX) if c == 0 else value
        copies[0].start()

        pl.when(t == 0)(prepare)

        @pl.when(t > 0)
        def _():
            hear()
            force_copies()[0].wait_send()
            drain(f_send.at[1], blocks_ref)
            kinetic([speed_ref[pl.ds(8 * c, 8), :] for c in range(3)], t - 2)

        tell()

        index = [[ids[pl.ds(16 * side + 8 * h, 8), :] for h in range(2)] for side in range(2)]
        low = [[index[s][h] & 127 for h in range(2)] for s in range(2)]
        for r in range(24):
            source = jnp.broadcast_to(cur[pl.ds(r, 1), :], (8, 128))
            for s in range(2):
                for h in range(2):
                    pair_x[s, h, r] = pick(source, low[s][h])

        in_home = [[index[s][h] < 128 for h in range(2)] for s in range(2)]
        in_x = [[index[s][h] < 256 for h in range(2)] for s in range(2)]
        copies[0].wait_recv()
        for r in range(24):
            source = jnp.broadcast_to(got_x[pl.ds(r, 1), :], (8, 128))
            for s in range(2):
                for h in range(2):
                    pair_x[s, h, r] = jnp.where(
                        in_home[s][h], pair_x[s, h, r], pick(source, low[s][h])
                    )

        drain(c_recv.at[1], blocks_ref)
        blocks = unpack([got_m[n] for n in range(6)])
        for c in range(3):
            near[pl.ds(8 * c, 8), :] = blocks[c]

        def complete(r, h):
            source = jnp.broadcast_to(near[pl.ds(r, 1), :], (8, 128))
            for s in range(2):
                pair_x[s, h, r] = jnp.where(
                    in_x[s][h], pair_x[s, h, r], pick(source, low[s][h])
                )

        for r in range(24):
            complete(r, 0)

        energy = jnp.zeros((8, 128), F32)
        lefts = []
        halo = None
        for h in range(2):
            usable = jnp.where(index[0][h] == CL_PAD, 0.0, 1.0)
            distinct = jnp.where(index[0][h] == index[1][h], 0.0, usable)
            second = [[None] * 3 for _ in range(8)]
            for k in range(8):
                xi = [pair_x[0, h, 8 * c + k] for c in range(3)]
                first = [None] * 3
                for l in range(8):
                    d = [xi[c] - pair_x[1, h, 8 * c + l] for c in range(3)]
                    u = jnp.maximum((usable if k < l else distinct) - dot3(d, d), 0.0)
                    uu = u * u
                    energy = energy + uu * u
                    for c in range(3):
                        push = uu * d[c]
                        first[c] = push if l == 0 else first[c] + push
                        second[l][c] = push if k == 0 else second[l][c] + push
                for c in range(3):
                    pair_f[pl.ds((8 * c + k) * 16 + 8 * h, 8), :] = first[c]
                if h == 0:
                    for r in range(3 * k, 3 * k + 3):
                        complete(r, 1)
            for l in range(8):
                for c in range(3):
                    pair_f[pl.ds(384 + (8 * c + l) * 16 + 8 * h, 8), :] = second[l][c]

            groups = range(8) if h == 0 else range(8, GROUPS)
            left = jnp.concatenate(
                [
                    halves(pair_f[pl.ds(384 * side + g, 24, stride=16), :])
                    for side in range(2)
                    for g in groups
                ],
                axis=1,
            )
            lefts.append(left)
            part = jnp.dot(
                left,
                table[pl.ds(2048 * h, left.shape[1]), pl.ds(128, 256)],
                preferred_element_type=F32,
            )
            halo = part if h == 0 else halo + part

        halo = halo[:24] + halo[24:]
        returns = force_copies()
        beyond = [halo[8 * c : 8 * c + 8, 128:] for c in range(3)]
        force_m[1] = side_by_side(beyond, FIRST, SECOND)
        for number in FAR:
            returns[number].start()
        force_m[0] = side_by_side(beyond, 0, FIRST)
        for number in NEAR:
            returns[number].start()
        force_x[...] = halo[:, :128]
        returns[0].start()
        own = None
        for h in range(2):
            part = jnp.dot(
                lefts[h],
                table[pl.ds(2048 * h, lefts[h].shape[1]), pl.ds(0, 128)],
                preferred_element_type=F32,
            )
            own = part if h == 0 else own + part
        own = own[:24] + own[24:]
        hear()

        @pl.when(t < ITERS)
        def _():
            tell()

        total = jnp.sum(jnp.sum(energy, axis=0, keepdims=True), axis=1, keepdims=True)
        row[...] = jnp.where(lanes(1) == t - 1, 2.0 * total, row[...])
        copies[0].wait_send()
        drain(c_send.at[1], blocks_ref)
        returns[0].wait_recv()
        came = jnp.dot(
            halves(ret_x[...]), back[pl.ds(0, 128), :], preferred_element_type=F32
        )
        own = own + came[:24] + came[24:]
        drain(f_recv.at[1], blocks_ref)
        came = jnp.concatenate(unpack([ret_m[n] for n in range(6)]), axis=0)
        came = jnp.dot(halves(came), back[pl.ds(128, 128), :], preferred_element_type=F32)
        force = own + came[:24] + came[24:]
        force = [0.5 * time_step * force[8 * c : 8 * c + 8] for c in range(3)]

        again = jnp.where(t > 0, 1.0, 0.0).astype(F32)
        speed = [half_ref[pl.ds(8 * c, 8), :] + again * force[c] for c in range(3)]

        @pl.when(t < ITERS)
        def _():
            flags = flag8[...]
            half = [speed[c] + force[c] for c in range(3)]
            before = [cur[pl.ds(8 * c, 8), :] for c in range(3)]
            moved = constrain(
                before,
                [x + time_step * v for x, v in zip(before, half)],
                rest_ref[...],
                flags,
                flags * up(flags),
            )
            for c in range(3):
                cur[pl.ds(8 * c, 8), :] = moved[c]
                half_ref[pl.ds(8 * c, 8), :] = (moved[c] - before[c]) / time_step
                speed_ref[pl.ds(8 * c, 8), :] = speed[c]

        @pl.when(t == ITERS)
        def _():
            kinetic(speed, ITERS - 1)
            for c in range(3):
                out_pos[c] = cur[pl.ds(8 * c, 8), :]
                out_vel[c] = speed[c]

        return carry

    lax.fori_loop(0, ITERS + 1, step, 0)
    def distance(offset):
        return sum(min(o, n - o) for o, n in zip(offset, sizes))

    def copy_row(source, target, offset, send, recv):
        pltpu.make_async_remote_copy(
            src_ref=source,
            dst_ref=target,
            send_sem=send,
            recv_sem=recv,
            device_id=at(offset),
            device_id_type=MESH,
        ).start()

    def total_of(slots):
        total = slots[0]
        for n in range(1, slots.shape[0]):
            total = total + slots[n]
        return total

    offsets = [(0, y, z) for y in range(sizes[1]) for z in range(sizes[2]) if y or z]
    own = me[1] * sizes[2] + me[2]
    for offset in sorted(offsets, key=distance, reverse=True):
        copy_row(row, plane.at[own], offset, p_send.at[0], p_recv.at[0])
    plane[own] = row[...]
    force_copies()[0].wait_send()
    drain(f_send.at[1], blocks_ref)
    drain(p_recv.at[0], rows_ref.at[pl.ds(0, len(offsets))])
    mid[...] = total_of(plane)
    offsets = sorted([(x, 0, 0) for x in range(1, sizes[0])], key=distance)
    lead = me[2] == sizes[2] - 1

    @pl.when(lead)
    def _():
        for x, _, _ in offsets:
            for z in range(sizes[2]):
                copy_row(mid, line.at[me[0]], (x, 0, z), l_send.at[z], l_recv.at[0])

    line[me[0]] = mid[...]
    drain(p_send.at[0], rows_ref.at[pl.ds(0, plane.shape[0] - 1)])
    drain(l_recv.at[0], rows_ref.at[pl.ds(0, len(offsets))])
    out_en[...] = total_of(line)

    @pl.when(lead)
    def _():
        for z in range(sizes[2]):
            drain(l_send.at[z], rows_ref.at[pl.ds(0, len(offsets))])


CL_PAD = 306
KINETIC = 8
VMEM_LIMIT = 12 << 20


def finish(beads, pos_ref, vel_ref, sum_ref, out_pos, out_vel, out_en, energy, stored):
    stores = [
        pltpu.make_async_copy(source, target, stored.at[n])
        for n, (source, target) in enumerate(
            ((pos_ref, out_pos), (vel_ref, out_vel), (energy, out_en))
        )
    ]
    stores[0].start()
    stores[1].start()
    total = sum_ref[...] / F32(beads)
    for n in range(2):
        energy[pl.ds(n, 1), :] = total[:, KINETIC * n : KINETIC * n + ITERS]
    stores[2].start()
    for store in stores:
        store.wait()


def on_device(sizes, positions, velocities, send_list, pair_list, constraint_flags):
    dma = pltpu.SemaphoreType.DMA
    vmem = pltpu.VMEM
    plane = sizes[1] * sizes[2]
    results = pl.pallas_call(
        functools.partial(kernel, sizes),
        out_shape=(
            jax.ShapeDtypeStruct((3, 8, 128), F32),
            jax.ShapeDtypeStruct((3, 8, 128), F32),
            jax.ShapeDtypeStruct((1, 128), F32),
        ),
        in_specs=[pl.BlockSpec(memory_space=pltpu.HBM)] * 5,
        out_specs=[pl.BlockSpec(memory_space=vmem)] * 3,
        scratch_shapes=[
            vmem((24, 128), F32),
            vmem((24, 128), F32),
            vmem((8, 128), F32),
            vmem((32, 128), jnp.int32),
            vmem((8, 128), jnp.int32),
            vmem((8, 128), F32),
            vmem((2 * SLOTS, 384), jnp.bfloat16),
            vmem((256, 128), jnp.bfloat16),
            vmem((24, 128), F32),
            vmem((2, 2, 24, 8, 128), F32),
            vmem((768, 128), F32),
            vmem((24, 128), F32),
            vmem((2, 8, 128), F32),
            vmem((24, 128), F32),
            vmem((2, 8, 128), F32),
            vmem((24, 128), F32),
            vmem((6, 8, 128), F32),
            vmem((24, 128), F32),
            vmem((6, 8, 128), F32),
            vmem((1, 128), F32),
            vmem((plane, 1, 128), F32),
            vmem((1, 128), F32),
            vmem((sizes[0], 1, 128), F32),
            dma((2,)),
            dma((2,)),
            dma((2,)),
            dma((2,)),
            dma((1,)),
            dma((1,)),
            dma((sizes[2],)),
            dma((1,)),
            pltpu.SemaphoreType.REGULAR((4,)),
            vmem((3, 8, 128), F32),
            vmem((3, 8, 128), F32),
            vmem((1, 178), jnp.int32),
            vmem((2, SLOTS), jnp.int32),
            vmem((7, 128), jnp.int32),
            dma((5,)),
            vmem((6, 8, 128), F32),
            vmem((max(plane, sizes[0]) - 1, 1, 128), F32),
            vmem((24, 128), F32),
        ],
        compiler_params=pltpu.CompilerParams(
            collective_id=0, has_side_effects=True, vmem_limit_bytes=VMEM_LIMIT
        ),
        name="membrane",
    )(
        *[
            pltpu.with_memory_space_constraint(x, pltpu.HBM)
            for x in (
                positions,
                velocities,
                send_list.reshape(1, -1),
                pair_list,
                constraint_flags,
            )
        ]
    )
    position, velocity, energies = pl.pallas_call(
        functools.partial(finish, 8 * 128 * sizes[0] * sizes[1] * sizes[2]),
        out_shape=(
            jax.ShapeDtypeStruct((3, 8, 128), F32),
            jax.ShapeDtypeStruct((3, 8, 128), F32),
            jax.ShapeDtypeStruct((2, ITERS), F32),
        ),
        in_specs=[pl.BlockSpec(memory_space=vmem)] * 3,
        out_specs=[pl.BlockSpec(memory_space=pltpu.HBM)] * 3,
        scratch_shapes=[vmem((2, ITERS), F32), dma((3,))],
        compiler_params=pltpu.CompilerParams(vmem_limit_bytes=1 << 20),
        name="finish",
    )(*results)
    return position, velocity, energies.T


def solution(mesh):
    sizes = tuple(mesh.shape[a] for a in AXES)
    spec = ("runs", "gx", "gy", "gz")
    return jax.shard_map(
        functools.partial(on_device, sizes),
        mesh=mesh,
        in_specs=(
            P(None, None, spec),
            P(None, None, spec),
            P(spec),
            P(None, spec),
            P(None, spec),
        ),
        out_specs=(P(None, None, spec), P(None, None, spec), P("runs", None)),
        check_vma=False,
    )
```

```python
import functools

import jax
import jax.numpy as jnp
from jax import lax
from jax.experimental import pallas as pl
from jax.experimental.pallas import tpu as pltpu
from jax.sharding import PartitionSpec as P

CX, CY, CZ = 1, 8, 16
ITERS = 3
NORDER = 4
time_step = 0.02
root_half = 0.7071067811865476
MESH = pl.DeviceIdType.MESH
ZONES = ((1, 0, 0), (0, 1, 0), (0, 0, 1), (1, 1, 0), (1, 0, 1), (0, 1, 1), (1, 1, 1))
AXES = ("gx", "gy", "gz")
FIRST, SECOND = 24, 26
FAR, NEAR = (3, 6, 4, 5), (1, 2)
GROUPS = 14
SLOTS = 1792
F32 = jnp.float32


def roll(x, by, axis):
    size = x.shape[axis]
    by = by % size
    return x if by == 0 else pltpu.roll(x, by, axis)


def partners(sizes):
    found = set()
    for zone in ZONES:
        for sign in (1, -1):
            found.add(tuple((sign * z) % n for z, n in zip(zone, sizes)))
    found.discard((0, 0, 0))
    return sorted(found, key=lambda o: (-sum(min(a, n - a) for a, n in zip(o, sizes)), o))


def lanes(rows=8):
    return lax.broadcasted_iota(jnp.int32, (rows, 128), 1)


def side_by_side(parts, first, width):
    lane = lanes()
    return jnp.where(
        lane < first + width,
        parts[0],
        jnp.where(lane < first + 2 * width, roll(parts[1], width, 1), roll(parts[2], 2 * width, 1)),
    )


def merge_near(received):
    within = lax.rem(lanes(), FIRST)
    return jnp.where(within < 16, received[0], received[1])


def merge_far(received):
    within = lax.rem(lanes() + (SECOND - FIRST % SECOND), SECOND)
    return jnp.where(
        within < 16,
        received[0],
        jnp.where(within < 24, received[1], jnp.where(within < 25, received[2], received[3])),
    )


def place(side, g):
    return 8 * side + g if g < 8 else 16 + (GROUPS - 8) * side + g - 8


def halves(value):
    high = value.astype(jnp.bfloat16).astype(F32)
    return jnp.concatenate([high, value - high], axis=0).astype(jnp.bfloat16)


def pick(table, index):
    return jnp.take_along_axis(table, index, axis=1, mode="promise_in_bounds")


def up(x):
    return roll(x, -1, 0)


def down(x):
    return roll(x, 1, 0)


def dot3(a, b):
    return a[0] * b[0] + a[1] * b[1] + a[2] * b[2]


def lag(x, by):
    return roll(x, -by, 0)


def expansion(coupling):
    coupling_down = down(coupling)
    power = {0: None}
    weights = {0: jnp.ones(coupling.shape, F32)}
    for _ in range(NORDER):
        later = {}
        for m, weight in power.items():
            lower = coupling_down if weight is None else coupling_down * down(weight)
            upper = coupling if weight is None else coupling * up(weight)
            for where_to, term in ((m - 1, lower), (m + 1, upper)):
                later[where_to] = later[where_to] + term if where_to in later else term
        power = later
        for m, weight in power.items():
            weights[m] = weights[m] + weight if m in weights else weight
    return [weights[m] for m in range(-NORDER, NORDER + 1)]


def expand(weights, source):
    terms = [w * lag(source, m - NORDER) for m, w in enumerate(weights)]
    while len(terms) > 1:
        terms = [
            terms[n] + terms[n + 1] if n + 1 < len(terms) else terms[n]
            for n in range(0, len(terms), 2)
        ]
    return terms[0]


def link_frame(previous, flags_pair):
    old = [x - up(x) for x in previous]
    length = jnp.maximum(jnp.sqrt(dot3(old, old)), 0.2)
    direction = [x / length for x in old]
    coupling = 0.5 * dot3(direction, [up(x) for x in direction]) * flags_pair
    return direction, expansion(coupling)


def constrain(updated, direction, weights, rest, flags):
    links = [x - up(x) for x in updated]
    solution = expand(weights, flags * root_half * (dot3(direction, links) - rest))
    shifts = [x * (root_half * solution) for x in direction]
    updated = [x - s + down(s) for x, s in zip(updated, shifts)]
    links = [x - up(x) for x in updated]
    squared = dot3(links, links)
    target = jnp.sqrt(jnp.maximum(2.0 * rest * rest - squared, 0.25 * rest * rest))
    solution = expand(weights, flags * root_half * (rest - target))
    shifts = [x * (root_half * solution) for x in direction]
    return [x - s + down(s) for x, s in zip(updated, shifts)]


def kernel(
    sizes,
    pos_in,
    vel_in,
    send_in,
    pair_in,
    flag_in,
    out_pos,
    out_vel,
    out_en,
    cur,
    half_ref,
    rest_ref,
    ids,
    send_ids,
    flag8,
    table,
    back,
    back2,
    near,
    frame,
    pair_x,
    pair_f,
    coord_x,
    coord_m,
    force_x,
    force_m,
    got_x,
    got_m,
    ret_x,
    ret_m,
    row,
    plane,
    mid,
    line,
    c_send,
    c_recv,
    f_send,
    f_recv,
    p_send,
    p_recv,
    l_send,
    l_recv,
    token,
    pos_ref,
    vel_ref,
    send_ref,
    pair_ref,
    flag_ref,
    loaded,
    blocks_ref,
    rows_ref,
    speed_ref,
):
    me = tuple(lax.axis_index(a) for a in AXES)

    def at(offset):
        return {
            a: lax.rem(me[i] + (offset[i] % sizes[i]), sizes[i])
            for i, a in enumerate(AXES)
            if offset[i] % sizes[i]
        }

    loads = [
        pltpu.make_async_copy(source, target, loaded.at[n])
        for n, (source, target) in enumerate(
            (
                (send_in, send_ref),
                (pos_in, pos_ref),
                (pair_in, pair_ref),
                (vel_in, vel_ref),
                (flag_in, flag_ref),
            )
        )
    ]
    for load in loads[:2]:
        load.start()
    barrier = pltpu.get_barrier_semaphore()
    others = partners(sizes)
    for offset in others:
        pl.semaphore_signal(barrier, inc=1, device_id=at(offset), device_id_type=MESH)
    for load in loads[2:]:
        load.start()

    lane = lanes()
    row[...] = jnp.zeros(row.shape, F32)
    loads[0].wait()
    loads[1].wait()
    send_ids[...] = jnp.full(send_ids.shape, -1, jnp.int32)
    send_ids[pl.ds(0, 1), :] = send_ref[:, pl.ds(0, 128)]
    send_ids[pl.ds(1, 1), pl.ds(0, FIRST + SECOND)] = send_ref[:, pl.ds(128, FIRST + SECOND)]
    for c in range(3):
        cur[pl.ds(8 * c, 8), :] = pos_ref[c]

    def prepare():
        for load in loads[2:]:
            load.wait()
        for c in range(3):
            half_ref[pl.ds(8 * c, 8), :] = vel_ref[c]
        ids[...] = jnp.full(ids.shape, CL_PAD, jnp.int32)
        for g in range(GROUPS):
            for side in range(2):
                ids[pl.ds(16 * side + g, 1), :] = pair_ref[pl.ds(side, 1), pl.ds(128 * g, 128)]
        flag8[...] = jnp.zeros(flag8.shape, F32)
        flag8[pl.ds(0, 7), :] = flag_ref[...].astype(F32)
        columns = jnp.transpose(ids[...].astype(F32))
        entry = jnp.broadcast_to(send_ids[pl.ds(1, 1), :], (8, 128))
        goals = [entry + 128 * c for c in range(3)]
        for n, (first, width) in enumerate(((0, FIRST), (FIRST, SECOND))):
            goal = side_by_side(goals, first, width)
            goal = jnp.where((lane >= first) & (lane < first + 3 * width), goal, -1)
            send_ids[pl.ds(2 + n, 1), :] = goal[:1]
        send_columns = jnp.transpose(send_ids[...].astype(F32))
        wide = lax.broadcasted_iota(jnp.int32, (128, 384), 1).astype(F32)
        for side in range(2):
            value = 12.0 if side == 0 else -12.0
            for g in range(GROUPS):
                column = columns[:, 16 * side + g : 16 * side + g + 1]
                table[pl.ds(128 * place(side, g), 128), :] = jnp.where(
                    wide == column, value, 0.0
                ).astype(jnp.bfloat16)
        back[...] = jnp.where(wide[:, :128] == send_columns[:, 0:1], 1.0, 0.0).astype(jnp.bfloat16)
        for b in range(2):
            back2[pl.ds(128 * b, 128), :] = jnp.where(
                wide == send_columns[:, 2 + b : 3 + b], 1.0, 0.0
            ).astype(jnp.bfloat16)
        links = [pos_ref[c] - up(pos_ref[c]) for c in range(3)]
        rest_ref[...] = jnp.sqrt(dot3(links, links))

    ring = [tuple(sign if a == axis else 0 for a in range(3)) for axis in (0, 1) for sign in (1, -1)]

    def tell():
        for number, offset in enumerate(ring):
            pl.semaphore_signal(
                token.at[number], inc=1, device_id=at(offset), device_id_type=MESH
            )

    def hear():
        for number in range(len(ring)):
            pl.semaphore_wait(token.at[number], 1)

    def coord_copies():
        copies = []
        for number, zone in enumerate(ZONES):
            source = coord_x if number == 0 else coord_m.at[0 if number < 3 else 1]
            target = got_x if number == 0 else got_m.at[number - 1]
            copies.append(
                pltpu.make_async_remote_copy(
                    src_ref=source,
                    dst_ref=target,
                    send_sem=c_send.at[0 if number == 0 else 1],
                    recv_sem=c_recv.at[0 if number == 0 else 1 if number in NEAR else 2],
                    device_id=at(tuple(-z for z in zone)),
                    device_id_type=MESH,
                )
            )
        return copies

    def force_copies():
        copies = []
        for number, zone in enumerate(ZONES):
            source = force_x if number == 0 else force_m.at[0 if number < 3 else 1]
            target = ret_x if number == 0 else ret_m.at[number - 1]
            copies.append(
                pltpu.make_async_remote_copy(
                    src_ref=source,
                    dst_ref=target,
                    send_sem=f_send.at[0 if number == 0 else 1],
                    recv_sem=f_recv.at[0 if number == 0 else 1],
                    device_id=at(zone),
                    device_id_type=MESH,
                )
            )
        return copies

    def drain(sem, ref):
        pltpu.make_async_copy(ref, ref, sem).wait()

    def kinetic(speed, number):
        total = jnp.sum(
            jnp.sum(dot3(speed, speed), axis=0, keepdims=True), axis=1, keepdims=True
        )
        row[...] = jnp.where(lanes(1) == KINETIC + number, 0.5 * total, row[...])

    def send_coords(home, ready=None):
        send_x = jnp.broadcast_to(send_ids[pl.ds(0, 1), :], (8, 128))
        send_m = jnp.maximum(jnp.broadcast_to(send_ids[pl.ds(1, 1), :], (8, 128)), 0)
        chosen = [pick(x, send_m) for x in home]
        edges = (0, 16, 24, 40, 48, 49, 50)
        for c, length in enumerate((CX, CY, CZ)):
            shifted = None
            for number in range(1, 7):
                if ZONES[number][c]:
                    mask = (lane >= edges[number - 1]) & (lane < edges[number])
                    shifted = mask if shifted is None else shifted | mask
            chosen[c] = chosen[c] + jnp.where(shifted, F32(length), 0.0)
        copies = coord_copies()
        coord_m[1] = side_by_side(chosen, FIRST, SECOND)
        if ready is not None:
            ready()
        for number in FAR:
            copies[number].start()
        coord_m[0] = side_by_side(chosen, 0, FIRST)
        for number in NEAR:
            copies[number].start()
        for c in range(3):
            value = pick(home[c], send_x)
            coord_x[pl.ds(8 * c, 8), :] = value + F32(CX) if c == 0 else value
        copies[0].start()

    send_coords(
        [pos_ref[c] for c in range(3)], lambda: pl.semaphore_wait(barrier, len(others))
    )

    def step(t, carry):
        copies = coord_copies()
        pl.when(t == 0)(prepare)

        @pl.when(t > 0)
        def _():
            hear()
            force_copies()[0].wait_send()
            drain(f_send.at[1], blocks_ref)
            kinetic([speed_ref[pl.ds(8 * c, 8), :] for c in range(3)], t - 2)

        tell()

        index = [[ids[pl.ds(16 * side + 8 * h, 8), :] for h in range(2)] for side in range(2)]
        low = [[index[s][h] & 127 for h in range(2)] for s in range(2)]
        for r in range(24):
            source = jnp.broadcast_to(cur[pl.ds(r, 1), :], (8, 128))
            for s in range(2):
                for h in range(2):
                    pair_x[s, h, r] = pick(source, low[s][h])

        in_home = [[index[s][h] < 128 for h in range(2)] for s in range(2)]
        in_x = [[index[s][h] < 256 for h in range(2)] for s in range(2)]
        copies[0].wait_recv()
        for r in range(24):
            source = jnp.broadcast_to(got_x[pl.ds(r, 1), :], (8, 128))
            for s in range(2):
                for h in range(2):
                    pair_x[s, h, r] = jnp.where(
                        in_home[s][h], pair_x[s, h, r], pick(source, low[s][h])
                    )

        drain(c_recv.at[1], blocks_ref.at[pl.ds(0, 2)])
        in_near = [[index[s][h] < 256 + FIRST for h in range(2)] for s in range(2)]

        def places(width):
            return [[[(low[s][h] + width * c) & 127 for c in range(3)] for h in range(2)] for s in range(2)]

        near_place, far_place = places(FIRST), places(SECOND)
        near[pl.ds(0, 8), :] = merge_near([got_m[n] for n in range(2)])
        for k in range(8):
            source = jnp.broadcast_to(near[pl.ds(k, 1), :], (8, 128))
            for c in range(3):
                for s in range(2):
                    for h in range(2):
                        pair_x[s, h, 8 * c + k] = jnp.where(
                            in_x[s][h],
                            pair_x[s, h, 8 * c + k],
                            pick(source, near_place[s][h][c]),
                        )

        drain(c_recv.at[2], blocks_ref.at[pl.ds(0, 4)])
        near[pl.ds(8, 8), :] = merge_far([got_m[n] for n in range(2, 6)])

        def complete(k, h):
            source = jnp.broadcast_to(near[pl.ds(8 + k, 1), :], (8, 128))
            for c in range(3):
                for s in range(2):
                    pair_x[s, h, 8 * c + k] = jnp.where(
                        in_near[s][h],
                        pair_x[s, h, 8 * c + k],
                        pick(source, far_place[s][h][c]),
                    )

        for k in range(8):
            complete(k, 0)

        energy = jnp.zeros((8, 128), F32)
        lefts = []
        halo = None
        for h in range(2):
            usable = jnp.where(index[0][h] == CL_PAD, 0.0, 1.0)
            distinct = jnp.where(index[0][h] == index[1][h], 0.0, usable)
            second = [[None] * 3 for _ in range(8)]
            for k in range(8):
                xi = [pair_x[0, h, 8 * c + k] for c in range(3)]
                first = [None] * 3
                for l in range(8):
                    d = [xi[c] - pair_x[1, h, 8 * c + l] for c in range(3)]
                    u = jnp.maximum((usable if k < l else distinct) - dot3(d, d), 0.0)
                    uu = u * u
                    energy = energy + uu * u
                    for c in range(3):
                        push = uu * d[c]
                        first[c] = push if l == 0 else first[c] + push
                        second[l][c] = push if k == 0 else second[l][c] + push
                for c in range(3):
                    pair_f[pl.ds((8 * c + k) * 16 + 8 * h, 8), :] = first[c]
                if h == 0:
                    complete(k, 1)
            for l in range(8):
                for c in range(3):
                    pair_f[pl.ds(384 + (8 * c + l) * 16 + 8 * h, 8), :] = second[l][c]

            groups = range(8) if h == 0 else range(8, GROUPS)
            left = jnp.concatenate(
                [
                    halves(pair_f[pl.ds(384 * side + g, 24, stride=16), :])
                    for side in range(2)
                    for g in groups
                ],
                axis=1,
            )
            lefts.append(left)
            part = jnp.dot(
                left,
                table[pl.ds(2048 * h, left.shape[1]), pl.ds(128, 256)],
                preferred_element_type=F32,
            )
            halo = part if h == 0 else halo + part

        halo = halo[:24] + halo[24:]
        returns = force_copies()
        beyond = [halo[8 * c : 8 * c + 8, 128:] for c in range(3)]
        force_m[1] = side_by_side(beyond, FIRST, SECOND)
        for number in FAR:
            returns[number].start()
        force_m[0] = side_by_side(beyond, 0, FIRST)
        for number in NEAR:
            returns[number].start()
        force_x[...] = halo[:, :128]
        returns[0].start()
        own = None
        for h in range(2):
            part = jnp.dot(
                lefts[h],
                table[pl.ds(2048 * h, lefts[h].shape[1]), pl.ds(0, 128)],
                preferred_element_type=F32,
            )
            own = part if h == 0 else own + part
        own = own[:24] + own[24:]
        hear()

        @pl.when(t < ITERS)
        def _():
            tell()

        total = jnp.sum(jnp.sum(energy, axis=0, keepdims=True), axis=1, keepdims=True)
        row[...] = jnp.where(lanes(1) == t - 1, 2.0 * total, row[...])
        flags = flag8[...]
        direction, weights = link_frame(
            [cur[pl.ds(8 * c, 8), :] for c in range(3)], flags * up(flags)
        )
        for n, value in enumerate(direction + weights):
            frame[pl.ds(8 * n, 8), :] = value

        copies[0].wait_send()
        drain(c_send.at[1], blocks_ref)
        returns[0].wait_recv()
        came = jnp.dot(
            halves(ret_x[...]), back[...], preferred_element_type=F32
        )
        own = own + came[:24] + came[24:]
        drain(f_recv.at[1], blocks_ref)
        received = [ret_m[n] for n in range(6)]
        came = jnp.concatenate([merge_near(received[:2]), merge_far(received[2:])], axis=1)
        came = jnp.dot(halves(came), back2[...], preferred_element_type=F32)
        came = came[:8] + came[8:]
        force = [
            0.5 * time_step * (own[8 * c : 8 * c + 8] + came[:, 128 * c : 128 * c + 128])
            for c in range(3)
        ]

        again = jnp.where(t > 0, 1.0, 0.0).astype(F32)
        speed = [half_ref[pl.ds(8 * c, 8), :] + again * force[c] for c in range(3)]

        @pl.when(t < ITERS)
        def _():
            half = [speed[c] + force[c] for c in range(3)]
            before = [cur[pl.ds(8 * c, 8), :] for c in range(3)]
            moved = constrain(
                [x + time_step * v for x, v in zip(before, half)],
                [frame[pl.ds(8 * n, 8), :] for n in range(3)],
                [frame[pl.ds(8 * n, 8), :] for n in range(3, 3 + 2 * NORDER + 1)],
                rest_ref[...],
                flag8[...],
            )
            send_coords(moved)
            for c in range(3):
                cur[pl.ds(8 * c, 8), :] = moved[c]
                half_ref[pl.ds(8 * c, 8), :] = (moved[c] - before[c]) / time_step
                speed_ref[pl.ds(8 * c, 8), :] = speed[c]

        @pl.when(t == ITERS)
        def _():
            kinetic(speed, ITERS - 1)
            for c in range(3):
                out_pos[c] = cur[pl.ds(8 * c, 8), :]
                out_vel[c] = speed[c]

        return carry

    lax.fori_loop(0, ITERS + 1, step, 0)
    def distance(offset):
        return sum(min(o, n - o) for o, n in zip(offset, sizes))

    def copy_row(source, target, offset, send, recv):
        pltpu.make_async_remote_copy(
            src_ref=source,
            dst_ref=target,
            send_sem=send,
            recv_sem=recv,
            device_id=at(offset),
            device_id_type=MESH,
        ).start()

    def total_of(slots):
        total = slots[0]
        for n in range(1, slots.shape[0]):
            total = total + slots[n]
        return total

    offsets = [(0, y, z) for y in range(sizes[1]) for z in range(sizes[2]) if y or z]
    own = me[1] * sizes[2] + me[2]
    for offset in sorted(offsets, key=distance, reverse=True):
        copy_row(row, plane.at[own], offset, p_send.at[0], p_recv.at[0])
    plane[own] = row[...]
    force_copies()[0].wait_send()
    drain(f_send.at[1], blocks_ref)
    drain(p_recv.at[0], rows_ref.at[pl.ds(0, len(offsets))])
    mid[...] = total_of(plane)
    offsets = sorted([(x, 0, 0) for x in range(1, sizes[0])], key=distance)
    lead = me[2] == sizes[2] - 1

    @pl.when(lead)
    def _():
        for x, _, _ in offsets:
            for z in range(sizes[2]):
                copy_row(mid, line.at[me[0]], (x, 0, z), l_send.at[z], l_recv.at[0])

    line[me[0]] = mid[...]
    drain(p_send.at[0], rows_ref.at[pl.ds(0, plane.shape[0] - 1)])
    drain(l_recv.at[0], rows_ref.at[pl.ds(0, len(offsets))])
    out_en[...] = total_of(line)

    @pl.when(lead)
    def _():
        for z in range(sizes[2]):
            drain(l_send.at[z], rows_ref.at[pl.ds(0, len(offsets))])


CL_PAD = 306
KINETIC = 8
VMEM_LIMIT = 12 << 20


def finish(beads, pos_ref, vel_ref, sum_ref, out_pos, out_vel, out_en, energy, stored):
    stores = [
        pltpu.make_async_copy(source, target, stored.at[n])
        for n, (source, target) in enumerate(
            ((pos_ref, out_pos), (vel_ref, out_vel), (energy, out_en))
        )
    ]
    stores[0].start()
    stores[1].start()
    total = sum_ref[...] / F32(beads)
    for n in range(2):
        energy[pl.ds(n, 1), :] = total[:, KINETIC * n : KINETIC * n + ITERS]
    stores[2].start()
    for store in stores:
        store.wait()


def on_device(sizes, positions, velocities, send_list, pair_list, constraint_flags):
    dma = pltpu.SemaphoreType.DMA
    vmem = pltpu.VMEM
    plane = sizes[1] * sizes[2]
    results = pl.pallas_call(
        functools.partial(kernel, sizes),
        out_shape=(
            jax.ShapeDtypeStruct((3, 8, 128), F32),
            jax.ShapeDtypeStruct((3, 8, 128), F32),
            jax.ShapeDtypeStruct((1, 128), F32),
        ),
        in_specs=[pl.BlockSpec(memory_space=pltpu.HBM)] * 5,
        out_specs=[pl.BlockSpec(memory_space=vmem)] * 3,
        scratch_shapes=[
            vmem((24, 128), F32),
            vmem((24, 128), F32),
            vmem((8, 128), F32),
            vmem((32, 128), jnp.int32),
            vmem((8, 128), jnp.int32),
            vmem((8, 128), F32),
            vmem((2 * SLOTS, 384), jnp.bfloat16),
            vmem((128, 128), jnp.bfloat16),
            vmem((256, 384), jnp.bfloat16),
            vmem((16, 128), F32),
            vmem((24 + 8 * (2 * NORDER + 1), 128), F32),
            vmem((2, 2, 24, 8, 128), F32),
            vmem((768, 128), F32),
            vmem((24, 128), F32),
            vmem((2, 8, 128), F32),
            vmem((24, 128), F32),
            vmem((2, 8, 128), F32),
            vmem((24, 128), F32),
            vmem((6, 8, 128), F32),
            vmem((24, 128), F32),
            vmem((6, 8, 128), F32),
            vmem((1, 128), F32),
            vmem((plane, 1, 128), F32),
            vmem((1, 128), F32),
            vmem((sizes[0], 1, 128), F32),
            dma((2,)),
            dma((3,)),
            dma((2,)),
            dma((2,)),
            dma((1,)),
            dma((1,)),
            dma((sizes[2],)),
            dma((1,)),
            pltpu.SemaphoreType.REGULAR((4,)),
            vmem((3, 8, 128), F32),
            vmem((3, 8, 128), F32),
            vmem((1, 178), jnp.int32),
            vmem((2, SLOTS), jnp.int32),
            vmem((7, 128), jnp.int32),
            dma((5,)),
            vmem((6, 8, 128), F32),
            vmem((max(plane, sizes[0]) - 1, 1, 128), F32),
            vmem((24, 128), F32),
        ],
        compiler_params=pltpu.CompilerParams(
            collective_id=0, has_side_effects=True, vmem_limit_bytes=VMEM_LIMIT
        ),
        name="membrane",
    )(
        *[
            pltpu.with_memory_space_constraint(x, pltpu.HBM)
            for x in (
                positions,
                velocities,
                send_list.reshape(1, -1),
                pair_list,
                constraint_flags,
            )
        ]
    )
    position, velocity, energies = pl.pallas_call(
        functools.partial(finish, 8 * 128 * sizes[0] * sizes[1] * sizes[2]),
        out_shape=(
            jax.ShapeDtypeStruct((3, 8, 128), F32),
            jax.ShapeDtypeStruct((3, 8, 128), F32),
            jax.ShapeDtypeStruct((2, ITERS), F32),
        ),
        in_specs=[pl.BlockSpec(memory_space=vmem)] * 3,
        out_specs=[pl.BlockSpec(memory_space=pltpu.HBM)] * 3,
        scratch_shapes=[vmem((2, ITERS), F32), dma((3,))],
        compiler_params=pltpu.CompilerParams(vmem_limit_bytes=1 << 20),
        name="finish",
    )(*results)
    return position, velocity, energies.T


def solution(mesh):
    sizes = tuple(mesh.shape[a] for a in AXES)
    spec = ("runs", "gx", "gy", "gz")
    return jax.shard_map(
        functools.partial(on_device, sizes),
        mesh=mesh,
        in_specs=(
            P(None, None, spec),
            P(None, None, spec),
            P(spec),
            P(None, spec),
            P(None, spec),
        ),
        out_specs=(P(None, None, spec), P(None, None, spec), P("runs", None)),
        check_vma=False,
    )
```

```python
import functools

import jax
import jax.numpy as jnp
from jax import lax
from jax.experimental import pallas as pl
from jax.experimental.pallas import tpu as pltpu
from jax.sharding import PartitionSpec as P

CX, CY, CZ = 1, 8, 16
ITERS = 3
NORDER = 4
time_step = 0.02
root_half = 0.7071067811865476
MESH = pl.DeviceIdType.MESH
ZONES = ((1, 0, 0), (0, 1, 0), (0, 0, 1), (1, 1, 0), (1, 0, 1), (0, 1, 1), (1, 1, 1))
AXES = ("gx", "gy", "gz")
FIRST, SECOND = 24, 26
FAR, NEAR = (3, 6, 4, 5), (1, 2)
GROUPS = 14
SLOTS = 1792
PITCH = 24
F32 = jnp.float32


def roll(x, by, axis):
    size = x.shape[axis]
    by = by % size
    return x if by == 0 else pltpu.roll(x, by, axis)


def partners(sizes):
    found = set()
    for zone in ZONES:
        for sign in (1, -1):
            found.add(tuple((sign * z) % n for z, n in zip(zone, sizes)))
    found.discard((0, 0, 0))
    return sorted(found, key=lambda o: (-sum(min(a, n - a) for a, n in zip(o, sizes)), o))


def lanes(rows=8):
    return lax.broadcasted_iota(jnp.int32, (rows, 128), 1)


def side_by_side(parts, first, width):
    lane = lanes()
    return jnp.where(
        lane < first + width,
        parts[0],
        jnp.where(lane < first + 2 * width, roll(parts[1], width, 1), roll(parts[2], 2 * width, 1)),
    )


def merge(zone, received):
    block = received[0]
    for n in range(1, len(received)):
        block = jnp.where(zone >= n, received[n], block)
    return block


def place(side, g):
    return 8 * side + g if g < 8 else 16 + (GROUPS - 8) * side + g - 8


def halves(value):
    high = value.astype(jnp.bfloat16).astype(F32)
    return jnp.concatenate([high, value - high], axis=0).astype(jnp.bfloat16)


def pick(table, index):
    return jnp.take_along_axis(table, index, axis=1, mode="promise_in_bounds")


def up(x):
    return roll(x, -1, 0)


def down(x):
    return roll(x, 1, 0)


def dot3(a, b):
    return a[0] * b[0] + a[1] * b[1] + a[2] * b[2]


def lag(x, by):
    return roll(x, -by, 0)


def expansion(coupling):
    coupling_down = down(coupling)
    power = {0: None}
    weights = {0: jnp.ones(coupling.shape, F32)}
    for _ in range(NORDER):
        later = {}
        for m, weight in power.items():
            lower = coupling_down if weight is None else coupling_down * down(weight)
            upper = coupling if weight is None else coupling * up(weight)
            for where_to, term in ((m - 1, lower), (m + 1, upper)):
                later[where_to] = later[where_to] + term if where_to in later else term
        power = later
        for m, weight in power.items():
            weights[m] = weights[m] + weight if m in weights else weight
    return [weights[m] for m in range(-NORDER, NORDER + 1)]


def expand(weights, source):
    terms = [w * lag(source, m - NORDER) for m, w in enumerate(weights)]
    while len(terms) > 1:
        terms = [
            terms[n] + terms[n + 1] if n + 1 < len(terms) else terms[n]
            for n in range(0, len(terms), 2)
        ]
    return terms[0]


def link_frame(previous, flags_pair):
    old = [x - up(x) for x in previous]
    length = jnp.maximum(jnp.sqrt(dot3(old, old)), 0.2)
    direction = [x / length for x in old]
    coupling = 0.5 * dot3(direction, [up(x) for x in direction]) * flags_pair
    return direction, expansion(coupling)


def constrain(updated, direction, weights, rest, flags):
    links = [x - up(x) for x in updated]
    solution = expand(weights, flags * root_half * (dot3(direction, links) - rest))
    shifts = [x * (root_half * solution) for x in direction]
    updated = [x - s + down(s) for x, s in zip(updated, shifts)]
    links = [x - (s + s) + (down(s) + up(s)) for x, s in zip(links, shifts)]
    squared = dot3(links, links)
    target = jnp.sqrt(jnp.maximum(2.0 * rest * rest - squared, 0.25 * rest * rest))
    solution = expand(weights, flags * root_half * (rest - target))
    shifts = [x * (root_half * solution) for x in direction]
    return [x - s + down(s) for x, s in zip(updated, shifts)]


def kernel(
    sizes,
    pos_in,
    vel_in,
    send_in,
    pair_in,
    flag_in,
    out_pos,
    out_vel,
    out_en,
    cur,
    half_ref,
    rest_ref,
    ids,
    send_ids,
    flag8,
    table,
    back,
    back2,
    near,
    frame,
    pair_x,
    pair_f,
    coord_x,
    coord_m,
    force_x,
    force_m,
    got_x,
    got_m,
    ret_x,
    ret_m,
    row,
    plane,
    mid,
    line,
    c_send,
    c_recv,
    f_send,
    f_recv,
    p_send,
    p_recv,
    l_send,
    l_recv,
    token,
    pos_ref,
    vel_ref,
    send_ref,
    pair_ref,
    flag_ref,
    loaded,
    blocks_ref,
    rows_ref,
    speed_ref,
    packed,
    shift,
):
    me = tuple(lax.axis_index(a) for a in AXES)

    def at(offset):
        return {
            a: lax.rem(me[i] + (offset[i] % sizes[i]), sizes[i])
            for i, a in enumerate(AXES)
            if offset[i] % sizes[i]
        }

    loads = [
        pltpu.make_async_copy(source, target, loaded.at[n])
        for n, (source, target) in enumerate(
            (
                (send_in, send_ref),
                (pos_in, pos_ref),
                (pair_in, pair_ref),
                (vel_in, vel_ref),
                (flag_in, flag_ref),
            )
        )
    ]
    for load in loads[:2]:
        load.start()
    barrier = pltpu.get_barrier_semaphore()
    others = partners(sizes)
    for offset in others:
        pl.semaphore_signal(barrier, inc=1, device_id=at(offset), device_id_type=MESH)
    for load in loads[2:]:
        load.start()

    lane = lanes()
    row[...] = jnp.zeros(row.shape, F32)
    loads[0].wait()
    loads[1].wait()
    send_ids[...] = jnp.full(send_ids.shape, -1, jnp.int32)
    send_ids[pl.ds(0, 1), :] = send_ref[:, pl.ds(0, 128)]
    send_ids[pl.ds(1, 1), pl.ds(0, FIRST + SECOND)] = send_ref[:, pl.ds(128, FIRST + SECOND)]
    for c in range(3):
        cur[pl.ds(8 * c, 8), :] = pos_ref[c]

    def prepare():
        for load in loads[2:]:
            load.wait()
        for c in range(3):
            half_ref[pl.ds(8 * c, 8), :] = vel_ref[c]
        ids[...] = jnp.full(ids.shape, CL_PAD, jnp.int32)
        for g in range(GROUPS):
            for side in range(2):
                ids[pl.ds(16 * side + g, 1), :] = pair_ref[pl.ds(side, 1), pl.ds(128 * g, 128)]
        flag8[...] = jnp.zeros(flag8.shape, F32)
        flag8[pl.ds(0, 7), :] = flag_ref[...].astype(F32)
        columns = jnp.transpose(ids[...].astype(F32))
        entry = jnp.broadcast_to(send_ids[pl.ds(1, 1), :], (8, 128))
        goals = [entry + 128 * c for c in range(3)]
        for n, (first, width) in enumerate(((0, FIRST), (FIRST, SECOND))):
            goal = side_by_side(goals, first, width)
            goal = jnp.where((lane >= first) & (lane < first + 3 * width), goal, -1)
            send_ids[pl.ds(2 + n, 1), :] = goal[:1]
        send_columns = jnp.transpose(send_ids[...].astype(F32))
        wide = lax.broadcasted_iota(jnp.int32, (128, 384), 1).astype(F32)
        for side in range(2):
            value = 12.0 if side == 0 else -12.0
            for g in range(GROUPS):
                column = columns[:, 16 * side + g : 16 * side + g + 1]
                table[pl.ds(128 * place(side, g), 128), :] = jnp.where(
                    wide == column, value, 0.0
                ).astype(jnp.bfloat16)
        back[...] = jnp.where(wide[:, :128] == send_columns[:, 0:1], 1.0, 0.0).astype(jnp.bfloat16)
        for b in range(2):
            back2[pl.ds(128 * b, 128), :] = jnp.where(
                wide == send_columns[:, 2 + b : 3 + b], 1.0, 0.0
            ).astype(jnp.bfloat16)
        links = [pos_ref[c] - up(pos_ref[c]) for c in range(3)]
        rest_ref[...] = jnp.sqrt(dot3(links, links))

    ring = [tuple(sign if a == axis else 0 for a in range(3)) for axis in (0, 1) for sign in (1, -1)]

    def tell():
        for number, offset in enumerate(ring):
            pl.semaphore_signal(
                token.at[number], inc=1, device_id=at(offset), device_id_type=MESH
            )

    def hear():
        for number in range(len(ring)):
            pl.semaphore_wait(token.at[number], 1)

    def coord_copies():
        copies = []
        for number, zone in enumerate(ZONES):
            source = coord_x if number == 0 else coord_m.at[0 if number < 3 else 1]
            target = got_x if number == 0 else got_m.at[number - 1]
            copies.append(
                pltpu.make_async_remote_copy(
                    src_ref=source,
                    dst_ref=target,
                    send_sem=c_send.at[0 if number == 0 else 1],
                    recv_sem=c_recv.at[0 if number == 0 else 1 if number in NEAR else 2],
                    device_id=at(tuple(-z for z in zone)),
                    device_id_type=MESH,
                )
            )
        return copies

    def force_copies():
        copies = []
        for number, zone in enumerate(ZONES):
            source = force_x if number == 0 else force_m.at[0 if number < 3 else 1]
            target = ret_x if number == 0 else ret_m.at[number - 1]
            copies.append(
                pltpu.make_async_remote_copy(
                    src_ref=source,
                    dst_ref=target,
                    send_sem=f_send.at[0 if number == 0 else 1],
                    recv_sem=f_recv.at[0 if number == 0 else 1 if number in NEAR else 2],
                    device_id=at(zone),
                    device_id_type=MESH,
                )
            )
        return copies

    def drain(sem, ref):
        pltpu.make_async_copy(ref, ref, sem).wait()

    def kinetic(speed, number):
        total = jnp.sum(
            jnp.sum(dot3(speed, speed), axis=0, keepdims=True), axis=1, keepdims=True
        )
        row[...] = jnp.where(lanes(1) == KINETIC + number, 0.5 * total, row[...])

    edges = (0, 16, 24, 40, 48, 49, 50)
    entry = jnp.broadcast_to(send_ids[pl.ds(1, 1), :], (8, 128))
    for n, (first, width) in enumerate(((0, FIRST), (FIRST, SECOND))):
        zone = jnp.zeros((8, 128), jnp.int32)
        offset = [jnp.zeros((8, 128), F32) for _ in range(3)]
        for number in range(1, 7):
            begin = edges[number - 1]
            inside = (lane >= begin) & (lane < edges[number])
            zone = jnp.where(inside, number - 1 if n == 0 else number - 3, zone)
            for c, length in enumerate((CX, CY, CZ)):
                if ZONES[number][c]:
                    offset[c] = jnp.where(inside, F32(length), offset[c])
        packed[n] = side_by_side([zone] * 3, first, width)
        packed[2 + n] = jnp.maximum(side_by_side([entry] * 3, first, width), 0)
        shift[n] = side_by_side(offset, first, width)

    def chosen(n, home):
        first, width = ((0, FIRST), (FIRST, SECOND))[n]
        index = packed[2 + n]
        picked = [pick(x, index) for x in home]
        return shift[n] + jnp.where(
            lane < first + width,
            picked[0],
            jnp.where(lane < first + 2 * width, picked[1], picked[2]),
        )

    def send_coords(home, ready=None):
        send_x = jnp.broadcast_to(send_ids[pl.ds(0, 1), :], (8, 128))
        copies = coord_copies()
        coord_m[1] = chosen(1, home)
        if ready is not None:
            ready()
        for number in FAR:
            copies[number].start()
        coord_m[0] = chosen(0, home)
        for number in NEAR:
            copies[number].start()
        for c in range(3):
            value = pick(home[c], send_x)
            coord_x[pl.ds(8 * c, 8), :] = value + F32(CX) if c == 0 else value
        copies[0].start()

    send_coords(
        [pos_ref[c] for c in range(3)], lambda: pl.semaphore_wait(barrier, len(others))
    )

    def step(t, carry):
        copies = coord_copies()
        pl.when(t == 0)(prepare)

        @pl.when(t > 0)
        def _():
            hear()
            force_copies()[0].wait_send()
            drain(f_send.at[1], blocks_ref)
            kinetic([speed_ref[pl.ds(8 * c, 8), :] for c in range(3)], t - 2)

        tell()

        index = [[ids[pl.ds(16 * side + 8 * h, 8), :] for h in range(2)] for side in range(2)]
        low = [[index[s][h] & 127 for h in range(2)] for s in range(2)]
        for r in range(24):
            source = jnp.broadcast_to(cur[pl.ds(r, 1), :], (8, 128))
            for s in range(2):
                for h in range(2):
                    pair_x[s, h, r] = pick(source, low[s][h])

        in_home = [[index[s][h] < 128 for h in range(2)] for s in range(2)]
        in_x = [[index[s][h] < 256 for h in range(2)] for s in range(2)]
        copies[0].wait_recv()
        for r in range(24):
            source = jnp.broadcast_to(got_x[pl.ds(r, 1), :], (8, 128))
            for s in range(2):
                for h in range(2):
                    pair_x[s, h, r] = jnp.where(
                        in_home[s][h], pair_x[s, h, r], pick(source, low[s][h])
                    )

        drain(c_recv.at[1], blocks_ref.at[pl.ds(0, 2)])
        in_near = [[index[s][h] < 256 + FIRST for h in range(2)] for s in range(2)]

        def places(width):
            return [[[(low[s][h] + width * c) & 127 for c in range(3)] for h in range(2)] for s in range(2)]

        near_place, far_place = places(FIRST), places(SECOND)
        near[pl.ds(0, 8), :] = merge(packed[0], [got_m[n] for n in range(2)])
        for k in range(8):
            source = jnp.broadcast_to(near[pl.ds(k, 1), :], (8, 128))
            for c in range(3):
                for s in range(2):
                    for h in range(2):
                        pair_x[s, h, 8 * c + k] = jnp.where(
                            in_x[s][h],
                            pair_x[s, h, 8 * c + k],
                            pick(source, near_place[s][h][c]),
                        )

        drain(c_recv.at[2], blocks_ref.at[pl.ds(0, 4)])
        near[pl.ds(8, 8), :] = merge(packed[1], [got_m[n] for n in range(2, 6)])

        def complete(k, h):
            source = jnp.broadcast_to(near[pl.ds(8 + k, 1), :], (8, 128))
            for c in range(3):
                for s in range(2):
                    pair_x[s, h, 8 * c + k] = jnp.where(
                        in_near[s][h],
                        pair_x[s, h, 8 * c + k],
                        pick(source, far_place[s][h][c]),
                    )

        for k in range(8):
            complete(k, 0)

        energy = jnp.zeros((8, 128), F32)
        lefts = []
        halo = None
        for h in range(2):
            usable = jnp.where(index[0][h] == CL_PAD, 0.0, 1.0)
            distinct = jnp.where(index[0][h] == index[1][h], 0.0, usable)
            second = [[None] * 3 for _ in range(8)]
            for k in range(8):
                xi = [pair_x[0, h, 8 * c + k] for c in range(3)]
                first = [None] * 3
                for l in range(8):
                    d = [xi[c] - pair_x[1, h, 8 * c + l] for c in range(3)]
                    u = jnp.maximum((usable if k < l else distinct) - dot3(d, d), 0.0)
                    uu = u * u
                    energy = energy + uu * u
                    for c in range(3):
                        push = uu * d[c]
                        first[c] = push if l == 0 else first[c] + push
                        second[l][c] = push if k == 0 else second[l][c] + push
                for c in range(3):
                    pair_f[pl.ds((8 * c + k) * PITCH + 8 * h, 8), :] = first[c]
                if h == 0:
                    complete(k, 1)
            for l in range(8):
                for c in range(3):
                    pair_f[pl.ds((24 + 8 * c + l) * PITCH + 8 * h, 8), :] = second[l][c]

            groups = range(8) if h == 0 else range(8, GROUPS)
            left = jnp.concatenate(
                [
                    halves(pair_f[pl.ds(24 * PITCH * side + g, 24, stride=PITCH), :])
                    for side in range(2)
                    for g in groups
                ],
                axis=1,
            )
            lefts.append(left)
            part = jnp.dot(
                left,
                table[pl.ds(2048 * h, left.shape[1]), pl.ds(128, 256)],
                preferred_element_type=F32,
            )
            halo = part if h == 0 else halo + part

        halo = halo[:24] + halo[24:]
        returns = force_copies()
        beyond = [halo[8 * c : 8 * c + 8, 128:] for c in range(3)]
        force_m[1] = side_by_side(beyond, FIRST, SECOND)
        for number in FAR:
            returns[number].start()
        force_m[0] = side_by_side(beyond, 0, FIRST)
        for number in NEAR:
            returns[number].start()
        force_x[...] = halo[:, :128]
        returns[0].start()
        own = None
        for h in range(2):
            part = jnp.dot(
                lefts[h],
                table[pl.ds(2048 * h, lefts[h].shape[1]), pl.ds(0, 128)],
                preferred_element_type=F32,
            )
            own = part if h == 0 else own + part
        own = own[:24] + own[24:]
        hear()

        @pl.when(t < ITERS)
        def _():
            tell()

        total = jnp.sum(jnp.sum(energy, axis=0, keepdims=True), axis=1, keepdims=True)
        row[...] = jnp.where(lanes(1) == t - 1, 2.0 * total, row[...])
        flags = flag8[...]
        direction, weights = link_frame(
            [cur[pl.ds(8 * c, 8), :] for c in range(3)], flags * up(flags)
        )
        for n, value in enumerate(direction + weights):
            frame[pl.ds(8 * n, 8), :] = value

        copies[0].wait_send()
        drain(c_send.at[1], blocks_ref)
        returns[0].wait_recv()
        came = jnp.dot(
            halves(ret_x[...]), back[...], preferred_element_type=F32
        )
        own = own + came[:24] + came[24:]
        drain(f_recv.at[1], blocks_ref.at[pl.ds(0, 2)])
        came = merge(packed[0], [ret_m[n] for n in range(2)])
        came = jnp.dot(halves(came), back2[pl.ds(0, 128), :], preferred_element_type=F32)
        came = came[:8] + came[8:]
        own = [
            own[8 * c : 8 * c + 8] + came[:, 128 * c : 128 * c + 128] for c in range(3)
        ]
        drain(f_recv.at[2], blocks_ref.at[pl.ds(0, 4)])
        came = merge(packed[1], [ret_m[n] for n in range(2, 6)])
        came = jnp.dot(halves(came), back2[pl.ds(128, 128), :], preferred_element_type=F32)
        came = came[:8] + came[8:]
        force = [
            0.5 * time_step * (own[c] + came[:, 128 * c : 128 * c + 128])
            for c in range(3)
        ]

        again = jnp.where(t > 0, 1.0, 0.0).astype(F32)
        speed = [half_ref[pl.ds(8 * c, 8), :] + again * force[c] for c in range(3)]

        @pl.when(t < ITERS)
        def _():
            half = [speed[c] + force[c] for c in range(3)]
            before = [cur[pl.ds(8 * c, 8), :] for c in range(3)]
            moved = constrain(
                [x + time_step * v for x, v in zip(before, half)],
                [frame[pl.ds(8 * n, 8), :] for n in range(3)],
                [frame[pl.ds(8 * n, 8), :] for n in range(3, 3 + 2 * NORDER + 1)],
                rest_ref[...],
                flag8[...],
            )
            send_coords(moved)
            for c in range(3):
                cur[pl.ds(8 * c, 8), :] = moved[c]
                half_ref[pl.ds(8 * c, 8), :] = (moved[c] - before[c]) / time_step
                speed_ref[pl.ds(8 * c, 8), :] = speed[c]

        @pl.when(t == ITERS)
        def _():
            kinetic(speed, ITERS - 1)
            for c in range(3):
                out_pos[c] = cur[pl.ds(8 * c, 8), :]
                out_vel[c] = speed[c]

        return carry

    lax.fori_loop(0, ITERS + 1, step, 0)
    def distance(offset):
        return sum(min(o, n - o) for o, n in zip(offset, sizes))

    def copy_row(source, target, offset, send, recv):
        pltpu.make_async_remote_copy(
            src_ref=source,
            dst_ref=target,
            send_sem=send,
            recv_sem=recv,
            device_id=at(offset),
            device_id_type=MESH,
        ).start()

    def total_of(slots):
        total = slots[0]
        for n in range(1, slots.shape[0]):
            total = total + slots[n]
        return total

    offsets = [(0, y, z) for y in range(sizes[1]) for z in range(sizes[2]) if y or z]
    own = me[1] * sizes[2] + me[2]
    for offset in sorted(offsets, key=distance, reverse=True):
        copy_row(row, plane.at[own], offset, p_send.at[0], p_recv.at[0])
    plane[own] = row[...]
    force_copies()[0].wait_send()
    drain(f_send.at[1], blocks_ref)
    drain(p_recv.at[0], rows_ref.at[pl.ds(0, len(offsets))])
    mid[...] = total_of(plane)
    offsets = sorted([(x, 0, 0) for x in range(1, sizes[0])], key=distance)
    lead = me[2] == sizes[2] - 1

    @pl.when(lead)
    def _():
        for x, _, _ in offsets:
            for z in range(sizes[2]):
                copy_row(mid, line.at[me[0]], (x, 0, z), l_send.at[z], l_recv.at[0])

    line[me[0]] = mid[...]
    drain(p_send.at[0], rows_ref.at[pl.ds(0, plane.shape[0] - 1)])
    drain(l_recv.at[0], rows_ref.at[pl.ds(0, len(offsets))])
    out_en[...] = total_of(line)

    @pl.when(lead)
    def _():
        for z in range(sizes[2]):
            drain(l_send.at[z], rows_ref.at[pl.ds(0, len(offsets))])


CL_PAD = 306
KINETIC = 8
VMEM_LIMIT = 12 << 20


def finish(beads, pos_ref, vel_ref, sum_ref, out_pos, out_vel, out_en, energy, stored):
    stores = [
        pltpu.make_async_copy(source, target, stored.at[n])
        for n, (source, target) in enumerate(
            ((pos_ref, out_pos), (vel_ref, out_vel), (energy, out_en))
        )
    ]
    stores[0].start()
    stores[1].start()
    total = sum_ref[...] / F32(beads)
    for n in range(2):
        energy[pl.ds(n, 1), :] = total[:, KINETIC * n : KINETIC * n + ITERS]
    stores[2].start()
    for store in stores:
        store.wait()


def on_device(sizes, positions, velocities, send_list, pair_list, constraint_flags):
    dma = pltpu.SemaphoreType.DMA
    vmem = pltpu.VMEM
    plane = sizes[1] * sizes[2]
    results = pl.pallas_call(
        functools.partial(kernel, sizes),
        out_shape=(
            jax.ShapeDtypeStruct((3, 8, 128), F32),
            jax.ShapeDtypeStruct((3, 8, 128), F32),
            jax.ShapeDtypeStruct((1, 128), F32),
        ),
        in_specs=[pl.BlockSpec(memory_space=pltpu.HBM)] * 5,
        out_specs=[pl.BlockSpec(memory_space=vmem)] * 3,
        scratch_shapes=[
            vmem((24, 128), F32),
            vmem((24, 128), F32),
            vmem((8, 128), F32),
            vmem((32, 128), jnp.int32),
            vmem((8, 128), jnp.int32),
            vmem((8, 128), F32),
            vmem((2 * SLOTS, 384), jnp.bfloat16),
            vmem((128, 128), jnp.bfloat16),
            vmem((256, 384), jnp.bfloat16),
            vmem((16, 128), F32),
            vmem((24 + 8 * (2 * NORDER + 1), 128), F32),
            vmem((2, 2, 24, 8, 128), F32),
            vmem((48 * PITCH, 128), F32),
            vmem((24, 128), F32),
            vmem((2, 8, 128), F32),
            vmem((24, 128), F32),
            vmem((2, 8, 128), F32),
            vmem((24, 128), F32),
            vmem((6, 8, 128), F32),
            vmem((24, 128), F32),
            vmem((6, 8, 128), F32),
            vmem((1, 128), F32),
            vmem((plane, 1, 128), F32),
            vmem((1, 128), F32),
            vmem((sizes[0], 1, 128), F32),
            dma((2,)),
            dma((3,)),
            dma((2,)),
            dma((3,)),
            dma((1,)),
            dma((1,)),
            dma((sizes[2],)),
            dma((1,)),
            pltpu.SemaphoreType.REGULAR((4,)),
            vmem((3, 8, 128), F32),
            vmem((3, 8, 128), F32),
            vmem((1, 178), jnp.int32),
            vmem((2, SLOTS), jnp.int32),
            vmem((7, 128), jnp.int32),
            dma((5,)),
            vmem((6, 8, 128), F32),
            vmem((max(plane, sizes[0]) - 1, 1, 128), F32),
            vmem((24, 128), F32),
            vmem((4, 8, 128), jnp.int32),
            vmem((2, 8, 128), F32),
        ],
        compiler_params=pltpu.CompilerParams(
            collective_id=0, has_side_effects=True, vmem_limit_bytes=VMEM_LIMIT
        ),
        name="membrane",
    )(
        *[
            pltpu.with_memory_space_constraint(x, pltpu.HBM)
            for x in (
                positions,
                velocities,
                send_list.reshape(1, -1),
                pair_list,
                constraint_flags,
            )
        ]
    )
    position, velocity, energies = pl.pallas_call(
        functools.partial(finish, 8 * 128 * sizes[0] * sizes[1] * sizes[2]),
        out_shape=(
            jax.ShapeDtypeStruct((3, 8, 128), F32),
            jax.ShapeDtypeStruct((3, 8, 128), F32),
            jax.ShapeDtypeStruct((2, ITERS), F32),
        ),
        in_specs=[pl.BlockSpec(memory_space=vmem)] * 3,
        out_specs=[pl.BlockSpec(memory_space=pltpu.HBM)] * 3,
        scratch_shapes=[vmem((2, ITERS), F32), dma((3,))],
        compiler_params=pltpu.CompilerParams(vmem_limit_bytes=1 << 20),
        name="finish",
    )(*results)
    return position, velocity, energies.T


def solution(mesh):
    sizes = tuple(mesh.shape[a] for a in AXES)
    spec = ("runs", "gx", "gy", "gz")
    return jax.shard_map(
        functools.partial(on_device, sizes),
        mesh=mesh,
        in_specs=(
            P(None, None, spec),
            P(None, None, spec),
            P(spec),
            P(None, spec),
            P(None, spec),
        ),
        out_specs=(P(None, None, spec), P(None, None, spec), P("runs", None)),
        check_vma=False,
    )
```

```python
import functools

import jax
import jax.numpy as jnp
from jax import lax
from jax.experimental import pallas as pl
from jax.experimental.pallas import tpu as pltpu
from jax.sharding import PartitionSpec as P

CX, CY, CZ = 1, 8, 16
ITERS = 3
NORDER = 4
time_step = 0.02
root_half = 0.7071067811865476
MESH = pl.DeviceIdType.MESH
ZONES = ((1, 0, 0), (0, 1, 0), (0, 0, 1), (1, 1, 0), (1, 0, 1), (0, 1, 1), (1, 1, 1))
AXES = ("gx", "gy", "gz")
FIRST, SECOND = 24, 26
FAR, NEAR = (3, 6, 4, 5), (1, 2)
GROUPS = 14
SLOTS = 1792
PITCH = 24
F32 = jnp.float32


def roll(x, by, axis):
    size = x.shape[axis]
    by = by % size
    return x if by == 0 else pltpu.roll(x, by, axis)


def lanes(rows=8):
    return lax.broadcasted_iota(jnp.int32, (rows, 128), 1)


def side_by_side(parts, first, width):
    lane = lanes()
    return jnp.where(
        lane < first + width,
        parts[0],
        jnp.where(lane < first + 2 * width, roll(parts[1], width, 1), roll(parts[2], 2 * width, 1)),
    )


def merge(zone, received):
    block = received[0]
    for n in range(1, len(received)):
        block = jnp.where(zone >= n, received[n], block)
    return block


def place(side, g):
    return 8 * side + g if g < 8 else 16 + (GROUPS - 8) * side + g - 8


def halves(value):
    high = value.astype(jnp.bfloat16).astype(F32)
    return jnp.concatenate([high, value - high], axis=0).astype(jnp.bfloat16)


def pick(table, index):
    return jnp.take_along_axis(table, index, axis=1, mode="promise_in_bounds")


def up(x):
    return roll(x, -1, 0)


def down(x):
    return roll(x, 1, 0)


def dot3(a, b):
    return a[0] * b[0] + a[1] * b[1] + a[2] * b[2]


def lag(x, by):
    return roll(x, -by, 0)


def expansion(coupling):
    coupling_down = down(coupling)
    power = {0: None}
    weights = {0: jnp.ones(coupling.shape, F32)}
    for _ in range(NORDER):
        later = {}
        for m, weight in power.items():
            lower = coupling_down if weight is None else coupling_down * down(weight)
            upper = coupling if weight is None else coupling * up(weight)
            for where_to, term in ((m - 1, lower), (m + 1, upper)):
                later[where_to] = later[where_to] + term if where_to in later else term
        power = later
        for m, weight in power.items():
            weights[m] = weights[m] + weight if m in weights else weight
    return [weights[m] for m in range(-NORDER, NORDER + 1)]


def expand(weights, source):
    terms = [w * lag(source, m - NORDER) for m, w in enumerate(weights)]
    while len(terms) > 1:
        terms = [
            terms[n] + terms[n + 1] if n + 1 < len(terms) else terms[n]
            for n in range(0, len(terms), 2)
        ]
    return terms[0]


def link_frame(previous, flags_pair):
    old = [x - up(x) for x in previous]
    length = jnp.maximum(jnp.sqrt(dot3(old, old)), 0.2)
    direction = [x / length for x in old]
    coupling = 0.5 * dot3(direction, [up(x) for x in direction]) * flags_pair
    return direction, expansion(coupling)


def constrain(updated, direction, weights, rest, flags):
    links = [x - up(x) for x in updated]
    solution = expand(weights, flags * root_half * (dot3(direction, links) - rest))
    shifts = [x * (root_half * solution) for x in direction]
    updated = [x - s + down(s) for x, s in zip(updated, shifts)]
    links = [x - (s + s) + (down(s) + up(s)) for x, s in zip(links, shifts)]
    squared = dot3(links, links)
    target = jnp.sqrt(jnp.maximum(2.0 * rest * rest - squared, 0.25 * rest * rest))
    solution = expand(weights, flags * root_half * (rest - target))
    shifts = [x * (root_half * solution) for x in direction]
    return [x - s + down(s) for x, s in zip(updated, shifts)]


def kernel(
    sizes,
    pos_in,
    vel_in,
    send_in,
    pair_in,
    flag_in,
    out_pos,
    out_vel,
    out_en,
    cur,
    half_ref,
    rest_ref,
    ids,
    send_ids,
    flag8,
    table,
    back,
    back2,
    near,
    frame,
    pair_x,
    pair_f,
    coord_x,
    coord_m,
    force_x,
    force_m,
    got_x,
    got_m,
    ret_x,
    ret_m,
    row,
    plane,
    mid,
    line,
    c_send,
    c_recv,
    f_send,
    f_recv,
    p_send,
    p_recv,
    l_send,
    l_recv,
    token,
    pos_ref,
    vel_ref,
    send_ref,
    pair_ref,
    flag_ref,
    loaded,
    blocks_ref,
    rows_ref,
    speed_ref,
    packed,
    shift,
):
    me = tuple(lax.axis_index(a) for a in AXES)

    def at(offset):
        return {
            a: lax.rem(me[i] + (offset[i] % sizes[i]), sizes[i])
            for i, a in enumerate(AXES)
            if offset[i] % sizes[i]
        }

    loads = [
        pltpu.make_async_copy(source, target, loaded.at[n])
        for n, (source, target) in enumerate(
            (
                (send_in, send_ref),
                (pos_in, pos_ref),
                (pair_in, pair_ref),
                (vel_in, vel_ref),
                (flag_in, flag_ref),
            )
        )
    ]
    for load in loads[:2]:
        load.start()
    barrier = pltpu.get_barrier_semaphore()
    for number in FAR + (0,) + NEAR:
        pl.semaphore_signal(
            barrier, inc=1, device_id=at(ZONES[number]), device_id_type=MESH
        )
    for load in loads[2:]:
        load.start()

    lane = lanes()
    row[...] = jnp.zeros(row.shape, F32)
    loads[0].wait()
    loads[1].wait()
    send_ids[...] = jnp.full(send_ids.shape, -1, jnp.int32)
    send_ids[pl.ds(0, 1), :] = send_ref[:, pl.ds(0, 128)]
    send_ids[pl.ds(1, 1), pl.ds(0, FIRST + SECOND)] = send_ref[:, pl.ds(128, FIRST + SECOND)]
    for c in range(3):
        cur[pl.ds(8 * c, 8), :] = pos_ref[c]

    def prepare():
        for load in loads[2:]:
            load.wait()
        for c in range(3):
            half_ref[pl.ds(8 * c, 8), :] = vel_ref[c]
        ids[...] = jnp.full(ids.shape, CL_PAD, jnp.int32)
        for g in range(GROUPS):
            for side in range(2):
                ids[pl.ds(16 * side + g, 1), :] = pair_ref[pl.ds(side, 1), pl.ds(128 * g, 128)]
        flag8[...] = jnp.zeros(flag8.shape, F32)
        flag8[pl.ds(0, 7), :] = flag_ref[...].astype(F32)
        columns = jnp.transpose(ids[...].astype(F32))
        entry = jnp.broadcast_to(send_ids[pl.ds(1, 1), :], (8, 128))
        goals = [entry + 128 * c for c in range(3)]
        for n, (first, width) in enumerate(((0, FIRST), (FIRST, SECOND))):
            goal = side_by_side(goals, first, width)
            goal = jnp.where((lane >= first) & (lane < first + 3 * width), goal, -1)
            send_ids[pl.ds(2 + n, 1), :] = goal[:1]
        send_columns = jnp.transpose(send_ids[...].astype(F32))
        wide = lax.broadcasted_iota(jnp.int32, (128, 384), 1).astype(F32)
        for side in range(2):
            value = 12.0 if side == 0 else -12.0
            for g in range(GROUPS):
                column = columns[:, 16 * side + g : 16 * side + g + 1]
                table[pl.ds(128 * place(side, g), 128), :] = jnp.where(
                    wide == column, value, 0.0
                ).astype(jnp.bfloat16)
        back[...] = jnp.where(wide[:, :128] == send_columns[:, 0:1], 1.0, 0.0).astype(jnp.bfloat16)
        for b in range(2):
            back2[pl.ds(128 * b, 128), :] = jnp.where(
                wide == send_columns[:, 2 + b : 3 + b], 1.0, 0.0
            ).astype(jnp.bfloat16)
        links = [pos_ref[c] - up(pos_ref[c]) for c in range(3)]
        rest_ref[...] = jnp.sqrt(dot3(links, links))

    ring = [tuple(sign if a == axis else 0 for a in range(3)) for axis in (0, 1) for sign in (1, -1)]

    def tell():
        for number, offset in enumerate(ring):
            pl.semaphore_signal(
                token.at[number], inc=1, device_id=at(offset), device_id_type=MESH
            )

    def hear():
        for number in range(len(ring)):
            pl.semaphore_wait(token.at[number], 1)

    def coord_copies():
        copies = []
        for number, zone in enumerate(ZONES):
            source = coord_x if number == 0 else coord_m.at[0 if number < 3 else 1]
            target = got_x if number == 0 else got_m.at[number - 1]
            copies.append(
                pltpu.make_async_remote_copy(
                    src_ref=source,
                    dst_ref=target,
                    send_sem=c_send.at[0 if number == 0 else 1],
                    recv_sem=c_recv.at[0 if number == 0 else 1 if number in NEAR else 2],
                    device_id=at(tuple(-z for z in zone)),
                    device_id_type=MESH,
                )
            )
        return copies

    def force_copies():
        copies = []
        for number, zone in enumerate(ZONES):
            source = force_x if number == 0 else force_m.at[0 if number < 3 else 1]
            target = ret_x if number == 0 else ret_m.at[number - 1]
            copies.append(
                pltpu.make_async_remote_copy(
                    src_ref=source,
                    dst_ref=target,
                    send_sem=f_send.at[0 if number == 0 else 1],
                    recv_sem=f_recv.at[0 if number == 0 else 1 if number in NEAR else 2],
                    device_id=at(zone),
                    device_id_type=MESH,
                )
            )
        return copies

    def drain(sem, ref):
        pltpu.make_async_copy(ref, ref, sem).wait()

    def kinetic(speed, number):
        total = jnp.sum(
            jnp.sum(dot3(speed, speed), axis=0, keepdims=True), axis=1, keepdims=True
        )
        row[...] = jnp.where(lanes(1) == KINETIC + number, 0.5 * total, row[...])

    edges = (0, 16, 24, 40, 48, 49, 50)
    entry = jnp.broadcast_to(send_ids[pl.ds(1, 1), :], (8, 128))
    for n, (first, width) in enumerate(((0, FIRST), (FIRST, SECOND))):
        zone = jnp.zeros((8, 128), jnp.int32)
        offset = [jnp.zeros((8, 128), F32) for _ in range(3)]
        for number in range(1, 7):
            begin = edges[number - 1]
            inside = (lane >= begin) & (lane < edges[number])
            zone = jnp.where(inside, number - 1 if n == 0 else number - 3, zone)
            for c, length in enumerate((CX, CY, CZ)):
                if ZONES[number][c]:
                    offset[c] = jnp.where(inside, F32(length), offset[c])
        packed[n] = side_by_side([zone] * 3, first, width)
        packed[2 + n] = jnp.maximum(side_by_side([entry] * 3, first, width), 0)
        shift[n] = side_by_side(offset, first, width)

    def chosen(n, home):
        first, width = ((0, FIRST), (FIRST, SECOND))[n]
        index = packed[2 + n]
        picked = [pick(x, index) for x in home]
        return shift[n] + jnp.where(
            lane < first + width,
            picked[0],
            jnp.where(lane < first + 2 * width, picked[1], picked[2]),
        )

    def build_x(home):
        send_x = jnp.broadcast_to(send_ids[pl.ds(0, 1), :], (8, 128))
        for c in range(3):
            value = pick(home[c], send_x)
            coord_x[pl.ds(8 * c, 8), :] = value + F32(CX) if c == 0 else value

    def send_coords(home):
        copies = coord_copies()
        coord_m[1] = chosen(1, home)
        for number in FAR:
            copies[number].start()
        coord_m[0] = chosen(0, home)
        for number in NEAR:
            copies[number].start()
        build_x(home)
        copies[0].start()

    start = [pos_ref[c] for c in range(3)]
    coord_m[1] = chosen(1, start)
    coord_m[0] = chosen(0, start)
    build_x(start)
    pl.semaphore_wait(barrier, len(ZONES))
    copies = coord_copies()
    for number in FAR + NEAR + (0,):
        copies[number].start()

    def step(t, carry):
        copies = coord_copies()
        pl.when(t == 0)(prepare)

        @pl.when(t > 0)
        def _():
            pl.when(t > 1)(hear)
            tell()
            force_copies()[0].wait_send()
            drain(f_send.at[1], blocks_ref)
            kinetic([speed_ref[pl.ds(8 * c, 8), :] for c in range(3)], t - 2)

        index = [[ids[pl.ds(16 * side + 8 * h, 8), :] for h in range(2)] for side in range(2)]
        low = [[index[s][h] & 127 for h in range(2)] for s in range(2)]
        for r in range(24):
            source = jnp.broadcast_to(cur[pl.ds(r, 1), :], (8, 128))
            for s in range(2):
                for h in range(2):
                    pair_x[s, h, r] = pick(source, low[s][h])

        in_home = [[index[s][h] < 128 for h in range(2)] for s in range(2)]
        in_x = [[index[s][h] < 256 for h in range(2)] for s in range(2)]
        copies[0].wait_recv()
        for r in range(24):
            source = jnp.broadcast_to(got_x[pl.ds(r, 1), :], (8, 128))
            for s in range(2):
                for h in range(2):
                    pair_x[s, h, r] = jnp.where(
                        in_home[s][h], pair_x[s, h, r], pick(source, low[s][h])
                    )

        drain(c_recv.at[1], blocks_ref.at[pl.ds(0, 2)])
        in_near = [[index[s][h] < 256 + FIRST for h in range(2)] for s in range(2)]

        def places(width):
            return [[[(low[s][h] + width * c) & 127 for c in range(3)] for h in range(2)] for s in range(2)]

        near_place, far_place = places(FIRST), places(SECOND)
        near[pl.ds(0, 8), :] = merge(packed[0], [got_m[n] for n in range(2)])
        for k in range(8):
            source = jnp.broadcast_to(near[pl.ds(k, 1), :], (8, 128))
            for c in range(3):
                for s in range(2):
                    for h in range(2):
                        pair_x[s, h, 8 * c + k] = jnp.where(
                            in_x[s][h],
                            pair_x[s, h, 8 * c + k],
                            pick(source, near_place[s][h][c]),
                        )

        drain(c_recv.at[2], blocks_ref.at[pl.ds(0, 4)])
        near[pl.ds(8, 8), :] = merge(packed[1], [got_m[n] for n in range(2, 6)])

        def complete(k, h):
            source = jnp.broadcast_to(near[pl.ds(8 + k, 1), :], (8, 128))
            for c in range(3):
                for s in range(2):
                    pair_x[s, h, 8 * c + k] = jnp.where(
                        in_near[s][h],
                        pair_x[s, h, 8 * c + k],
                        pick(source, far_place[s][h][c]),
                    )

        for k in range(8):
            complete(k, 0)

        energy = jnp.zeros((8, 128), F32)
        lefts = []
        parts = []
        for h in range(2):
            usable = jnp.where(index[0][h] == CL_PAD, 0.0, 1.0)
            distinct = jnp.where(index[0][h] == index[1][h], 0.0, usable)
            second = [[None] * 3 for _ in range(8)]
            for k in range(8):
                xi = [pair_x[0, h, 8 * c + k] for c in range(3)]
                first = [None] * 3
                for l in range(8):
                    d = [xi[c] - pair_x[1, h, 8 * c + l] for c in range(3)]
                    u = jnp.maximum((usable if k < l else distinct) - dot3(d, d), 0.0)
                    uu = u * u
                    energy = energy + uu * u
                    for c in range(3):
                        push = uu * d[c]
                        first[c] = push if l == 0 else first[c] + push
                        second[l][c] = push if k == 0 else second[l][c] + push
                for c in range(3):
                    pair_f[pl.ds((8 * c + k) * PITCH + 8 * h, 8), :] = first[c]
                if h == 0:
                    complete(k, 1)
            for l in range(8):
                for c in range(3):
                    pair_f[pl.ds((24 + 8 * c + l) * PITCH + 8 * h, 8), :] = second[l][c]

            groups = range(8) if h == 0 else range(8, GROUPS)
            left = jnp.concatenate(
                [
                    halves(pair_f[pl.ds(24 * PITCH * side + g, 24, stride=PITCH), :])
                    for side in range(2)
                    for g in groups
                ],
                axis=1,
            )
            lefts.append(left)
            parts.append(
                jnp.dot(
                    left,
                    table[pl.ds(2048 * h, left.shape[1]), pl.ds(128 if h == 0 else 256, 256 if h == 0 else 128)],
                    preferred_element_type=F32,
                )
            )

        halo = parts[0][:, 128:] + parts[1]
        halo = halo[:24] + halo[24:]
        returns = force_copies()
        beyond = [halo[8 * c : 8 * c + 8] for c in range(3)]
        force_m[1] = side_by_side(beyond, FIRST, SECOND)
        for number in FAR:
            returns[number].start()
        force_m[0] = side_by_side(beyond, 0, FIRST)
        for number in NEAR:
            returns[number].start()
        rest = jnp.dot(
            lefts[1],
            table[pl.ds(2048, lefts[1].shape[1]), pl.ds(0, 256)],
            preferred_element_type=F32,
        )
        halo = parts[0][:, :128] + rest[:, 128:]
        force_x[...] = halo[:24] + halo[24:]
        returns[0].start()
        own = rest[:, :128] + jnp.dot(
            lefts[0], table[pl.ds(0, 2048), pl.ds(0, 128)], preferred_element_type=F32
        )
        own = own[:24] + own[24:]
        @pl.when(t > 0)
        def _():
            hear()
            tell()

        total = jnp.sum(jnp.sum(energy, axis=0, keepdims=True), axis=1, keepdims=True)
        row[...] = jnp.where(lanes(1) == t - 1, 2.0 * total, row[...])
        flags = flag8[...]
        direction, weights = link_frame(
            [cur[pl.ds(8 * c, 8), :] for c in range(3)], flags * up(flags)
        )
        for n, value in enumerate(direction + weights):
            frame[pl.ds(8 * n, 8), :] = value

        copies[0].wait_send()
        drain(c_send.at[1], blocks_ref)
        returns[0].wait_recv()
        came = jnp.dot(
            halves(ret_x[...]), back[...], preferred_element_type=F32
        )
        own = own + came[:24] + came[24:]
        drain(f_recv.at[1], blocks_ref.at[pl.ds(0, 2)])
        came = merge(packed[0], [ret_m[n] for n in range(2)])
        came = jnp.dot(halves(came), back2[pl.ds(0, 128), :], preferred_element_type=F32)
        came = came[:8] + came[8:]
        own = [
            own[8 * c : 8 * c + 8] + came[:, 128 * c : 128 * c + 128] for c in range(3)
        ]
        drain(f_recv.at[2], blocks_ref.at[pl.ds(0, 4)])
        came = merge(packed[1], [ret_m[n] for n in range(2, 6)])
        came = jnp.dot(halves(came), back2[pl.ds(128, 128), :], preferred_element_type=F32)
        came = came[:8] + came[8:]
        force = [
            0.5 * time_step * (own[c] + came[:, 128 * c : 128 * c + 128])
            for c in range(3)
        ]

        again = jnp.where(t > 0, 1.0, 0.0).astype(F32)
        speed = [half_ref[pl.ds(8 * c, 8), :] + again * force[c] for c in range(3)]

        @pl.when(t < ITERS)
        def _():
            half = [speed[c] + force[c] for c in range(3)]
            before = [cur[pl.ds(8 * c, 8), :] for c in range(3)]
            moved = constrain(
                [x + time_step * v for x, v in zip(before, half)],
                [frame[pl.ds(8 * n, 8), :] for n in range(3)],
                [frame[pl.ds(8 * n, 8), :] for n in range(3, 3 + 2 * NORDER + 1)],
                rest_ref[...],
                flag8[...],
            )
            send_coords(moved)
            for c in range(3):
                cur[pl.ds(8 * c, 8), :] = moved[c]
                half_ref[pl.ds(8 * c, 8), :] = (moved[c] - before[c]) / time_step
                speed_ref[pl.ds(8 * c, 8), :] = speed[c]

        @pl.when(t == ITERS)
        def _():
            kinetic(speed, ITERS - 1)
            for c in range(3):
                out_pos[c] = cur[pl.ds(8 * c, 8), :]
                out_vel[c] = speed[c]

        return carry

    lax.fori_loop(0, ITERS + 1, step, 0)
    def distance(offset):
        return sum(min(o, n - o) for o, n in zip(offset, sizes))

    def copy_row(source, target, offset, send, recv):
        pltpu.make_async_remote_copy(
            src_ref=source,
            dst_ref=target,
            send_sem=send,
            recv_sem=recv,
            device_id=at(offset),
            device_id_type=MESH,
        ).start()

    def total_of(slots):
        total = slots[0]
        for n in range(1, slots.shape[0]):
            total = total + slots[n]
        return total

    offsets = [(0, y, z) for y in range(sizes[1]) for z in range(sizes[2]) if y or z]
    own = me[1] * sizes[2] + me[2]
    for offset in sorted(offsets, key=distance, reverse=True):
        copy_row(row, plane.at[own], offset, p_send.at[0], p_recv.at[0])
    plane[own] = row[...]
    hear()
    tell()
    force_copies()[0].wait_send()
    drain(f_send.at[1], blocks_ref)
    hear()
    drain(p_recv.at[0], rows_ref.at[pl.ds(0, len(offsets))])
    mid[...] = total_of(plane)
    offsets = sorted([(x, 0, 0) for x in range(1, sizes[0])], key=distance)
    lead = me[2] == sizes[2] - 1

    @pl.when(lead)
    def _():
        for x, _, _ in offsets:
            for z in range(sizes[2]):
                copy_row(mid, line.at[me[0]], (x, 0, z), l_send.at[z], l_recv.at[0])

    line[me[0]] = mid[...]
    drain(p_send.at[0], rows_ref.at[pl.ds(0, plane.shape[0] - 1)])
    drain(l_recv.at[0], rows_ref.at[pl.ds(0, len(offsets))])
    out_en[...] = total_of(line)

    @pl.when(lead)
    def _():
        for z in range(sizes[2]):
            drain(l_send.at[z], rows_ref.at[pl.ds(0, len(offsets))])


CL_PAD = 306
KINETIC = 8
VMEM_LIMIT = 12 << 20


def finish(beads, pos_ref, vel_ref, sum_ref, out_pos, out_vel, out_en, energy, stored):
    stores = [
        pltpu.make_async_copy(source, target, stored.at[n])
        for n, (source, target) in enumerate(
            ((pos_ref, out_pos), (vel_ref, out_vel), (energy, out_en))
        )
    ]
    stores[0].start()
    stores[1].start()
    total = sum_ref[...] / F32(beads)
    for n in range(2):
        energy[pl.ds(n, 1), :] = total[:, KINETIC * n : KINETIC * n + ITERS]
    stores[2].start()
    for store in stores:
        store.wait()


def on_device(sizes, positions, velocities, send_list, pair_list, constraint_flags):
    dma = pltpu.SemaphoreType.DMA
    vmem = pltpu.VMEM
    plane = sizes[1] * sizes[2]
    results = pl.pallas_call(
        functools.partial(kernel, sizes),
        out_shape=(
            jax.ShapeDtypeStruct((3, 8, 128), F32),
            jax.ShapeDtypeStruct((3, 8, 128), F32),
            jax.ShapeDtypeStruct((1, 128), F32),
        ),
        in_specs=[pl.BlockSpec(memory_space=pltpu.HBM)] * 5,
        out_specs=[pl.BlockSpec(memory_space=vmem)] * 3,
        scratch_shapes=[
            vmem((24, 128), F32),
            vmem((24, 128), F32),
            vmem((8, 128), F32),
            vmem((32, 128), jnp.int32),
            vmem((8, 128), jnp.int32),
            vmem((8, 128), F32),
            vmem((2 * SLOTS, 384), jnp.bfloat16),
            vmem((128, 128), jnp.bfloat16),
            vmem((256, 384), jnp.bfloat16),
            vmem((16, 128), F32),
            vmem((24 + 8 * (2 * NORDER + 1), 128), F32),
            vmem((2, 2, 24, 8, 128), F32),
            vmem((48 * PITCH, 128), F32),
            vmem((24, 128), F32),
            vmem((2, 8, 128), F32),
            vmem((24, 128), F32),
            vmem((2, 8, 128), F32),
            vmem((24, 128), F32),
            vmem((6, 8, 128), F32),
            vmem((24, 128), F32),
            vmem((6, 8, 128), F32),
            vmem((1, 128), F32),
            vmem((plane, 1, 128), F32),
            vmem((1, 128), F32),
            vmem((sizes[0], 1, 128), F32),
            dma((2,)),
            dma((3,)),
            dma((2,)),
            dma((3,)),
            dma((1,)),
            dma((1,)),
            dma((sizes[2],)),
            dma((1,)),
            pltpu.SemaphoreType.REGULAR((4,)),
            vmem((3, 8, 128), F32),
            vmem((3, 8, 128), F32),
            vmem((1, 178), jnp.int32),
            vmem((2, SLOTS), jnp.int32),
            vmem((7, 128), jnp.int32),
            dma((5,)),
            vmem((6, 8, 128), F32),
            vmem((max(plane, sizes[0]) - 1, 1, 128), F32),
            vmem((24, 128), F32),
            vmem((4, 8, 128), jnp.int32),
            vmem((2, 8, 128), F32),
        ],
        compiler_params=pltpu.CompilerParams(
            collective_id=0, has_side_effects=True, vmem_limit_bytes=VMEM_LIMIT
        ),
        name="membrane",
    )(
        *[
            pltpu.with_memory_space_constraint(x, pltpu.HBM)
            for x in (
                positions,
                velocities,
                send_list.reshape(1, -1),
                pair_list,
                constraint_flags,
            )
        ]
    )
    position, velocity, energies = pl.pallas_call(
        functools.partial(finish, 8 * 128 * sizes[0] * sizes[1] * sizes[2]),
        out_shape=(
            jax.ShapeDtypeStruct((3, 8, 128), F32),
            jax.ShapeDtypeStruct((3, 8, 128), F32),
            jax.ShapeDtypeStruct((2, ITERS), F32),
        ),
        in_specs=[pl.BlockSpec(memory_space=vmem)] * 3,
        out_specs=[pl.BlockSpec(memory_space=pltpu.HBM)] * 3,
        scratch_shapes=[vmem((2, ITERS), F32), dma((3,))],
        compiler_params=pltpu.CompilerParams(vmem_limit_bytes=1 << 20),
        name="finish",
    )(*results)
    return position, velocity, energies.T


def solution(mesh):
    sizes = tuple(mesh.shape[a] for a in AXES)
    spec = ("runs", "gx", "gy", "gz")
    return jax.shard_map(
        functools.partial(on_device, sizes),
        mesh=mesh,
        in_specs=(
            P(None, None, spec),
            P(None, None, spec),
            P(spec),
            P(None, spec),
            P(None, spec),
        ),
        out_specs=(P(None, None, spec), P(None, None, spec), P("runs", None)),
        check_vma=False,
    )
```

```python
import functools

import jax
import jax.numpy as jnp
from jax import lax
from jax.experimental import pallas as pl
from jax.experimental.pallas import tpu as pltpu
from jax.sharding import PartitionSpec as P

CX, CY, CZ = 1, 8, 16
ITERS = 3
NORDER = 4
time_step = 0.02
root_half = 0.7071067811865476
MESH = pl.DeviceIdType.MESH
ZONES = ((1, 0, 0), (0, 1, 0), (0, 0, 1), (1, 1, 0), (1, 0, 1), (0, 1, 1), (1, 1, 1))
AXES = ("gx", "gy", "gz")
FIRST, SECOND = 24, 26
FAR, NEAR = (3, 6, 4, 5), (1, 2)
GROUPS = 14
SLOTS = 1792
PITCH = 24
F32 = jnp.float32


def roll(x, by, axis):
    size = x.shape[axis]
    by = by % size
    return x if by == 0 else pltpu.roll(x, by, axis)


def lanes(rows=8):
    return lax.broadcasted_iota(jnp.int32, (rows, 128), 1)


def side_by_side(parts, first, width):
    lane = lanes()
    return jnp.where(
        lane < first + width,
        parts[0],
        jnp.where(lane < first + 2 * width, roll(parts[1], width, 1), roll(parts[2], 2 * width, 1)),
    )


def merge(zone, received):
    block = received[0]
    for n in range(1, len(received)):
        block = jnp.where(zone >= n, received[n], block)
    return block


PASSES = ((0, 8), (8, 4), (12, 2))


def place(side, g):
    for begin, width in PASSES:
        if g < begin + width:
            return 2 * begin + width * side + g - begin


def pass_of(g):
    return max(n for n, (begin, _) in enumerate(PASSES) if begin <= g)


def where_is(side, p, c, k):
    width = PASSES[p][1]
    return sum(3 * w for _, w in PASSES[:p]) + c * width + k if side == 0 else 42 + 24 * p + 8 * c + k


def rows_of(row, width, k):
    sublane = lax.broadcasted_iota(jnp.int32, (8, 128), 0)
    value = jnp.broadcast_to(row(k), (8, 128))
    for n in range(1, 8 // width):
        value = jnp.where(sublane >= n * width, jnp.broadcast_to(row(k + n * width), (8, 128)), value)
    return value


def halves(value):
    high = value.astype(jnp.bfloat16).astype(F32)
    return jnp.concatenate([high, value - high], axis=0).astype(jnp.bfloat16)


def pick(table, index):
    return jnp.take_along_axis(table, index, axis=1, mode="promise_in_bounds")


def up(x):
    return roll(x, -1, 0)


def down(x):
    return roll(x, 1, 0)


def dot3(a, b):
    return a[0] * b[0] + a[1] * b[1] + a[2] * b[2]


def lag(x, by):
    return roll(x, -by, 0)


def expansion(coupling):
    coupling_down = down(coupling)
    power = {0: None}
    weights = {0: jnp.ones(coupling.shape, F32)}
    for _ in range(NORDER):
        later = {}
        for m, weight in power.items():
            lower = coupling_down if weight is None else coupling_down * down(weight)
            upper = coupling if weight is None else coupling * up(weight)
            for where_to, term in ((m - 1, lower), (m + 1, upper)):
                later[where_to] = later[where_to] + term if where_to in later else term
        power = later
        for m, weight in power.items():
            weights[m] = weights[m] + weight if m in weights else weight
    return [weights[m] for m in range(-NORDER, NORDER + 1)]


def expand(weights, source):
    terms = [w * lag(source, m - NORDER) for m, w in enumerate(weights)]
    while len(terms) > 1:
        terms = [
            terms[n] + terms[n + 1] if n + 1 < len(terms) else terms[n]
            for n in range(0, len(terms), 2)
        ]
    return terms[0]


def link_frame(previous, flags_pair):
    old = [x - up(x) for x in previous]
    length = jnp.maximum(jnp.sqrt(dot3(old, old)), 0.2)
    direction = [x / length for x in old]
    coupling = 0.5 * dot3(direction, [up(x) for x in direction]) * flags_pair
    return direction, expansion(coupling)


def constrain(updated, direction, weights, rest, flags):
    links = [x - up(x) for x in updated]
    solution = expand(weights, flags * root_half * (dot3(direction, links) - rest))
    shifts = [x * (root_half * solution) for x in direction]
    updated = [x - s + down(s) for x, s in zip(updated, shifts)]
    links = [x - (s + s) + (down(s) + up(s)) for x, s in zip(links, shifts)]
    squared = dot3(links, links)
    target = jnp.sqrt(jnp.maximum(2.0 * rest * rest - squared, 0.25 * rest * rest))
    solution = expand(weights, flags * root_half * (rest - target))
    shifts = [x * (root_half * solution) for x in direction]
    return [x - s + down(s) for x, s in zip(updated, shifts)]


def kernel(
    sizes,
    pos_in,
    vel_in,
    send_in,
    pair_in,
    flag_in,
    out_pos,
    out_vel,
    out_en,
    cur,
    half_ref,
    rest_ref,
    ids,
    send_ids,
    flag8,
    table,
    back,
    back2,
    near,
    frame,
    pair_x,
    pair_f,
    coord_x,
    coord_m,
    force_x,
    force_m,
    got_x,
    got_m,
    ret_x,
    ret_m,
    row,
    plane,
    mid,
    line,
    c_send,
    c_recv,
    f_send,
    f_recv,
    p_send,
    p_recv,
    l_send,
    l_recv,
    token,
    pos_ref,
    vel_ref,
    send_ref,
    pair_ref,
    flag_ref,
    loaded,
    blocks_ref,
    rows_ref,
    speed_ref,
    packed,
    shift,
):
    me = tuple(lax.axis_index(a) for a in AXES)

    def at(offset):
        return {
            a: lax.rem(me[i] + (offset[i] % sizes[i]), sizes[i])
            for i, a in enumerate(AXES)
            if offset[i] % sizes[i]
        }

    loads = [
        pltpu.make_async_copy(source, target, loaded.at[n])
        for n, (source, target) in enumerate(
            (
                (send_in, send_ref),
                (pos_in, pos_ref),
                (pair_in, pair_ref),
                (vel_in, vel_ref),
                (flag_in, flag_ref),
            )
        )
    ]
    for load in loads[:2]:
        load.start()
    barrier = pltpu.get_barrier_semaphore()
    for number in FAR + (0,) + NEAR:
        pl.semaphore_signal(
            barrier, inc=1, device_id=at(ZONES[number]), device_id_type=MESH
        )
    for load in loads[2:]:
        load.start()

    lane = lanes()
    row[...] = jnp.zeros(row.shape, F32)
    loads[0].wait()
    loads[1].wait()
    send_ids[...] = jnp.full(send_ids.shape, -1, jnp.int32)
    send_ids[pl.ds(0, 1), :] = send_ref[:, pl.ds(0, 128)]
    send_ids[pl.ds(1, 1), pl.ds(0, FIRST + SECOND)] = send_ref[:, pl.ds(128, FIRST + SECOND)]
    for c in range(3):
        cur[pl.ds(8 * c, 8), :] = pos_ref[c]

    def prepare():
        for load in loads[2:]:
            load.wait()
        for c in range(3):
            half_ref[pl.ds(8 * c, 8), :] = vel_ref[c]
        for side in range(2):
            for p, (begin, width) in enumerate(PASSES):
                for n in range(8):
                    g = begin + n % width
                    ids[pl.ds(24 * side + 8 * p + n, 1), :] = pair_ref[
                        pl.ds(side, 1), pl.ds(128 * g, 128)
                    ]
        flag8[...] = jnp.zeros(flag8.shape, F32)
        flag8[pl.ds(0, 7), :] = flag_ref[...].astype(F32)
        columns = jnp.transpose(ids[...].astype(F32))
        entry = jnp.broadcast_to(send_ids[pl.ds(1, 1), :], (8, 128))
        goals = [entry + 128 * c for c in range(3)]
        for n, (first, width) in enumerate(((0, FIRST), (FIRST, SECOND))):
            goal = side_by_side(goals, first, width)
            goal = jnp.where((lane >= first) & (lane < first + 3 * width), goal, -1)
            send_ids[pl.ds(2 + n, 1), :] = goal[:1]
        send_columns = jnp.transpose(send_ids[...].astype(F32))
        wide = lax.broadcasted_iota(jnp.int32, (128, 384), 1).astype(F32)
        for side in range(2):
            value = 12.0 if side == 0 else -12.0
            for g in range(GROUPS):
                at_row = 24 * side + 8 * pass_of(g) + g - PASSES[pass_of(g)][0]
                column = columns[:, at_row : at_row + 1]
                table[pl.ds(128 * place(side, g), 128), :] = jnp.where(
                    wide == column, value, 0.0
                ).astype(jnp.bfloat16)
        back[...] = jnp.where(wide[:, :128] == send_columns[:, 0:1], 1.0, 0.0).astype(jnp.bfloat16)
        for b in range(2):
            back2[pl.ds(128 * b, 128), :] = jnp.where(
                wide == send_columns[:, 2 + b : 3 + b], 1.0, 0.0
            ).astype(jnp.bfloat16)
        links = [pos_ref[c] - up(pos_ref[c]) for c in range(3)]
        rest_ref[...] = jnp.sqrt(dot3(links, links))

    ring = [tuple(sign if a == axis else 0 for a in range(3)) for axis in (0, 1) for sign in (1, -1)]

    def tell():
        for number, offset in enumerate(ring):
            pl.semaphore_signal(
                token.at[number], inc=1, device_id=at(offset), device_id_type=MESH
            )

    def hear():
        for number in range(len(ring)):
            pl.semaphore_wait(token.at[number], 1)

    def coord_copies():
        copies = []
        for number, zone in enumerate(ZONES):
            source = coord_x if number == 0 else coord_m.at[0 if number < 3 else 1]
            target = got_x if number == 0 else got_m.at[number - 1]
            copies.append(
                pltpu.make_async_remote_copy(
                    src_ref=source,
                    dst_ref=target,
                    send_sem=c_send.at[0 if number == 0 else 1],
                    recv_sem=c_recv.at[0 if number == 0 else 1 if number in NEAR else 2],
                    device_id=at(tuple(-z for z in zone)),
                    device_id_type=MESH,
                )
            )
        return copies

    def force_copies():
        copies = []
        for number, zone in enumerate(ZONES):
            source = force_x if number == 0 else force_m.at[0 if number < 3 else 1]
            target = ret_x if number == 0 else ret_m.at[number - 1]
            copies.append(
                pltpu.make_async_remote_copy(
                    src_ref=source,
                    dst_ref=target,
                    send_sem=f_send.at[0 if number == 0 else 1],
                    recv_sem=f_recv.at[0 if number == 0 else 1 if number in NEAR else 2],
                    device_id=at(zone),
                    device_id_type=MESH,
                )
            )
        return copies

    def drain(sem, ref):
        pltpu.make_async_copy(ref, ref, sem).wait()

    def kinetic(speed, number):
        total = jnp.sum(
            jnp.sum(dot3(speed, speed), axis=0, keepdims=True), axis=1, keepdims=True
        )
        row[...] = jnp.where(lanes(1) == KINETIC + number, 0.5 * total, row[...])

    edges = (0, 16, 24, 40, 48, 49, 50)
    entry = jnp.broadcast_to(send_ids[pl.ds(1, 1), :], (8, 128))
    for n, (first, width) in enumerate(((0, FIRST), (FIRST, SECOND))):
        zone = jnp.zeros((8, 128), jnp.int32)
        offset = [jnp.zeros((8, 128), F32) for _ in range(3)]
        for number in range(1, 7):
            begin = edges[number - 1]
            inside = (lane >= begin) & (lane < edges[number])
            zone = jnp.where(inside, number - 1 if n == 0 else number - 3, zone)
            for c, length in enumerate((CX, CY, CZ)):
                if ZONES[number][c]:
                    offset[c] = jnp.where(inside, F32(length), offset[c])
        packed[n] = side_by_side([zone] * 3, first, width)
        packed[2 + n] = jnp.maximum(side_by_side([entry] * 3, first, width), 0)
        shift[n] = side_by_side(offset, first, width)

    def chosen(n, home):
        first, width = ((0, FIRST), (FIRST, SECOND))[n]
        index = packed[2 + n]
        picked = [pick(x, index) for x in home]
        return shift[n] + jnp.where(
            lane < first + width,
            picked[0],
            jnp.where(lane < first + 2 * width, picked[1], picked[2]),
        )

    def build_x(home):
        send_x = jnp.broadcast_to(send_ids[pl.ds(0, 1), :], (8, 128))
        for c in range(3):
            value = pick(home[c], send_x)
            coord_x[pl.ds(8 * c, 8), :] = value + F32(CX) if c == 0 else value

    def send_coords(home):
        copies = coord_copies()
        coord_m[1] = chosen(1, home)
        for number in FAR:
            copies[number].start()
        coord_m[0] = chosen(0, home)
        for number in NEAR:
            copies[number].start()
        build_x(home)
        copies[0].start()

    start = [pos_ref[c] for c in range(3)]
    coord_m[1] = chosen(1, start)
    coord_m[0] = chosen(0, start)
    build_x(start)
    pl.semaphore_wait(barrier, len(ZONES))
    copies = coord_copies()
    for number in FAR + NEAR + (0,):
        copies[number].start()

    def step(t, carry):
        copies = coord_copies()
        pl.when(t == 0)(prepare)

        @pl.when(t > 0)
        def _():
            pl.when(t > 1)(hear)
            tell()
            force_copies()[0].wait_send()
            drain(f_send.at[1], blocks_ref)
            kinetic([speed_ref[pl.ds(8 * c, 8), :] for c in range(3)], t - 2)

        index = [[ids[pl.ds(24 * side + 8 * p, 8), :] for p in range(3)] for side in range(2)]
        low = [[x & 127 for x in side] for side in index]

        def gather(row, keep, places, which):
            for side, p, k in which:
                width = PASSES[p][1]
                for c in range(3):
                    if side == 0:
                        source = rows_of(lambda n: row(c, n), width, k)
                    else:
                        source = jnp.broadcast_to(row(c, k), (8, 128))
                    slot = where_is(side, p, c, k)
                    value = pick(source, places[side][p][c])
                    if keep is not None:
                        value = jnp.where(keep[side][p], pair_x[slot], value)
                    pair_x[slot] = value

        def blocks_of(passes):
            return [(1, p, k) for k in range(8) for p in passes] + [
                (0, p, k) for p in passes for k in range(PASSES[p][1])
            ]

        everywhere = [[[x] * 3 for x in side] for side in low]
        gather(lambda c, k: cur[pl.ds(8 * c + k, 1), :], None, everywhere, blocks_of(range(3)))

        in_home = [[x < 128 for x in side] for side in index]
        in_x = [[x < 256 for x in side] for side in index]
        in_near = [[x < 256 + FIRST for x in side] for side in index]
        near_place, far_place = [
            [[[(x + width * c) & 127 for c in range(3)] for x in side] for side in low]
            for width in (FIRST, SECOND)
        ]
        copies[0].wait_recv()
        gather(lambda c, k: got_x[pl.ds(8 * c + k, 1), :], in_home, everywhere, blocks_of(range(3)))

        drain(c_recv.at[1], blocks_ref.at[pl.ds(0, 2)])
        near[pl.ds(0, 8), :] = merge(packed[0], [got_m[n] for n in range(2)])
        gather(lambda c, k: near[pl.ds(k, 1), :], in_x, near_place, blocks_of(range(3)))

        drain(c_recv.at[2], blocks_ref.at[pl.ds(0, 4)])
        near[pl.ds(8, 8), :] = merge(packed[1], [got_m[n] for n in range(2, 6)])

        def complete(which):
            gather(lambda c, k: near[pl.ds(8 + k, 1), :], in_near, far_place, which)

        complete(blocks_of(range(1)))

        energy = jnp.zeros((8, 128), F32)
        sublane = lax.broadcasted_iota(jnp.int32, (8, 128), 0)
        lefts = []
        parts = []
        for p, (begin, width) in enumerate(PASSES):
            usable = jnp.where(index[0][p] == CL_PAD, 0.0, 1.0)
            distinct = jnp.where(index[0][p] == index[1][p], 0.0, usable)
            limits = [distinct]
            for n in range(1, 8 // width):
                limits.append(jnp.where(sublane < n * width, usable, distinct))
            limits.append(usable)
            second = [[None] * 3 for _ in range(8)]
            for k in range(width):
                xi = [pair_x[where_is(0, p, c, k)] for c in range(3)]
                first = [None] * 3
                for l in range(8):
                    limit = limits[min(max(-((k - l) // width), 0), 8 // width)]
                    d = [xi[c] - pair_x[where_is(1, p, c, l)] for c in range(3)]
                    u = jnp.maximum(limit - dot3(d, d), 0.0)
                    uu = u * u
                    energy = energy + uu * u
                    for c in range(3):
                        push = uu * d[c]
                        first[c] = push if l == 0 else first[c] + push
                        second[l][c] = push if k == 0 else second[l][c] + push
                for n in range(8 // width):
                    for c in range(3):
                        pair_f[pl.ds((8 * c + k + n * width) * PITCH + begin, width), :] = roll(
                            first[c], -n * width, 0
                        )[:width]
                if p == 0:
                    complete(
                        [(1, 1, k), (1, 2, k)]
                        + ([(0, 1, k)] if k < 4 else [(0, 2, k - 4)] if k < 6 else [])
                    )
            for l in range(8):
                for c in range(3):
                    value = second[l][c]
                    turn = 4
                    while turn >= width:
                        value = value + roll(value, turn, 0)
                        turn //= 2
                    pair_f[pl.ds((24 + 8 * c + l) * PITCH + begin, width), :] = value[:width]
            left = jnp.concatenate(
                [
                    halves(pair_f[pl.ds(24 * PITCH * side + g, 24, stride=PITCH), :])
                    for side in range(2)
                    for g in range(begin, begin + width)
                ],
                axis=1,
            )
            lefts.append(left)
            parts.append(
                jnp.dot(
                    left,
                    table[
                        pl.ds(256 * begin, left.shape[1]),
                        pl.ds(128 if p == 0 else 256, 256 if p == 0 else 128),
                    ],
                    preferred_element_type=F32,
                )
            )

        halo = parts[0][:, 128:] + parts[1] + parts[2]
        halo = halo[:24] + halo[24:]
        returns = force_copies()
        beyond = [halo[8 * c : 8 * c + 8] for c in range(3)]
        force_m[1] = side_by_side(beyond, FIRST, SECOND)
        for number in FAR:
            returns[number].start()
        force_m[0] = side_by_side(beyond, 0, FIRST)
        for number in NEAR:
            returns[number].start()
        rest = jnp.dot(
            jnp.concatenate(lefts[1:], axis=1),
            table[pl.ds(2048, 1536), pl.ds(0, 256)],
            preferred_element_type=F32,
        )
        halo = parts[0][:, :128] + rest[:, 128:]
        force_x[...] = halo[:24] + halo[24:]
        returns[0].start()
        own = rest[:, :128] + jnp.dot(
            lefts[0], table[pl.ds(0, 2048), pl.ds(0, 128)], preferred_element_type=F32
        )
        own = own[:24] + own[24:]
        @pl.when(t > 0)
        def _():
            hear()
            tell()

        total = jnp.sum(jnp.sum(energy, axis=0, keepdims=True), axis=1, keepdims=True)
        row[...] = jnp.where(lanes(1) == t - 1, 2.0 * total, row[...])
        flags = flag8[...]
        direction, weights = link_frame(
            [cur[pl.ds(8 * c, 8), :] for c in range(3)], flags * up(flags)
        )
        for n, value in enumerate(direction + weights):
            frame[pl.ds(8 * n, 8), :] = value

        copies[0].wait_send()
        drain(c_send.at[1], blocks_ref)
        returns[0].wait_recv()
        came = jnp.dot(
            halves(ret_x[...]), back[...], preferred_element_type=F32
        )
        own = own + came[:24] + came[24:]
        drain(f_recv.at[1], blocks_ref.at[pl.ds(0, 2)])
        came = merge(packed[0], [ret_m[n] for n in range(2)])
        came = jnp.dot(halves(came), back2[pl.ds(0, 128), :], preferred_element_type=F32)
        came = came[:8] + came[8:]
        own = [
            own[8 * c : 8 * c + 8] + came[:, 128 * c : 128 * c + 128] for c in range(3)
        ]
        drain(f_recv.at[2], blocks_ref.at[pl.ds(0, 4)])
        came = merge(packed[1], [ret_m[n] for n in range(2, 6)])
        came = jnp.dot(halves(came), back2[pl.ds(128, 128), :], preferred_element_type=F32)
        came = came[:8] + came[8:]
        force = [
            0.5 * time_step * (own[c] + came[:, 128 * c : 128 * c + 128])
            for c in range(3)
        ]

        again = jnp.where(t > 0, 1.0, 0.0).astype(F32)
        speed = [half_ref[pl.ds(8 * c, 8), :] + again * force[c] for c in range(3)]

        @pl.when(t < ITERS)
        def _():
            half = [speed[c] + force[c] for c in range(3)]
            before = [cur[pl.ds(8 * c, 8), :] for c in range(3)]
            moved = constrain(
                [x + time_step * v for x, v in zip(before, half)],
                [frame[pl.ds(8 * n, 8), :] for n in range(3)],
                [frame[pl.ds(8 * n, 8), :] for n in range(3, 3 + 2 * NORDER + 1)],
                rest_ref[...],
                flag8[...],
            )
            send_coords(moved)
            for c in range(3):
                cur[pl.ds(8 * c, 8), :] = moved[c]
                half_ref[pl.ds(8 * c, 8), :] = (moved[c] - before[c]) / time_step
                speed_ref[pl.ds(8 * c, 8), :] = speed[c]

        @pl.when(t == ITERS)
        def _():
            kinetic(speed, ITERS - 1)
            for c in range(3):
                out_pos[c] = cur[pl.ds(8 * c, 8), :]
                out_vel[c] = speed[c]

        return carry

    lax.fori_loop(0, ITERS + 1, step, 0)
    def distance(offset):
        return sum(min(o, n - o) for o, n in zip(offset, sizes))

    def copy_row(source, target, offset, send, recv):
        pltpu.make_async_remote_copy(
            src_ref=source,
            dst_ref=target,
            send_sem=send,
            recv_sem=recv,
            device_id=at(offset),
            device_id_type=MESH,
        ).start()

    def total_of(slots):
        terms = [slots[n] for n in range(slots.shape[0])]
        while len(terms) > 1:
            terms = [
                terms[n] + terms[n + 1] if n + 1 < len(terms) else terms[n]
                for n in range(0, len(terms), 2)
            ]
        return terms[0]

    offsets = [(0, y, z) for y in range(sizes[1]) for z in range(sizes[2]) if y or z]
    own = me[1] * sizes[2] + me[2]
    for offset in sorted(offsets, key=distance, reverse=True):
        copy_row(row, plane.at[own], offset, p_send.at[0], p_recv.at[0])
    plane[own] = row[...]
    hear()
    tell()
    force_copies()[0].wait_send()
    drain(f_send.at[1], blocks_ref)
    hear()
    drain(p_recv.at[0], rows_ref.at[pl.ds(0, len(offsets))])
    mid[...] = total_of(plane)
    offsets = sorted([(x, 0, 0) for x in range(1, sizes[0])], key=distance)
    lead = me[2] == sizes[2] - 1

    @pl.when(lead)
    def _():
        for x, _, _ in offsets:
            for z in range(sizes[2]):
                copy_row(mid, line.at[me[0]], (x, 0, z), l_send.at[z], l_recv.at[0])

    line[me[0]] = mid[...]
    drain(p_send.at[0], rows_ref.at[pl.ds(0, plane.shape[0] - 1)])
    drain(l_recv.at[0], rows_ref.at[pl.ds(0, len(offsets))])
    out_en[...] = total_of(line)

    @pl.when(lead)
    def _():
        for z in range(sizes[2]):
            drain(l_send.at[z], rows_ref.at[pl.ds(0, len(offsets))])


CL_PAD = 306
KINETIC = 8
VMEM_LIMIT = 12 << 20


def finish(beads, pos_ref, vel_ref, sum_ref, out_pos, out_vel, out_en, energy, stored):
    stores = [
        pltpu.make_async_copy(source, target, stored.at[n])
        for n, (source, target) in enumerate(
            ((pos_ref, out_pos), (vel_ref, out_vel), (energy, out_en))
        )
    ]
    stores[0].start()
    stores[1].start()
    total = sum_ref[...] / F32(beads)
    for n in range(2):
        energy[pl.ds(n, 1), :] = total[:, KINETIC * n : KINETIC * n + ITERS]
    stores[2].start()
    for store in stores:
        store.wait()


def on_device(sizes, positions, velocities, send_list, pair_list, constraint_flags):
    dma = pltpu.SemaphoreType.DMA
    vmem = pltpu.VMEM
    plane = sizes[1] * sizes[2]
    results = pl.pallas_call(
        functools.partial(kernel, sizes),
        out_shape=(
            jax.ShapeDtypeStruct((3, 8, 128), F32),
            jax.ShapeDtypeStruct((3, 8, 128), F32),
            jax.ShapeDtypeStruct((1, 128), F32),
        ),
        in_specs=[pl.BlockSpec(memory_space=pltpu.HBM)] * 5,
        out_specs=[pl.BlockSpec(memory_space=vmem)] * 3,
        scratch_shapes=[
            vmem((24, 128), F32),
            vmem((24, 128), F32),
            vmem((8, 128), F32),
            vmem((48, 128), jnp.int32),
            vmem((8, 128), jnp.int32),
            vmem((8, 128), F32),
            vmem((2 * SLOTS, 384), jnp.bfloat16),
            vmem((128, 128), jnp.bfloat16),
            vmem((256, 384), jnp.bfloat16),
            vmem((16, 128), F32),
            vmem((24 + 8 * (2 * NORDER + 1), 128), F32),
            vmem((114, 8, 128), F32),
            vmem((48 * PITCH, 128), F32),
            vmem((24, 128), F32),
            vmem((2, 8, 128), F32),
            vmem((24, 128), F32),
            vmem((2, 8, 128), F32),
            vmem((24, 128), F32),
            vmem((6, 8, 128), F32),
            vmem((24, 128), F32),
            vmem((6, 8, 128), F32),
            vmem((1, 128), F32),
            vmem((plane, 1, 128), F32),
            vmem((1, 128), F32),
            vmem((sizes[0], 1, 128), F32),
            dma((2,)),
            dma((3,)),
            dma((2,)),
            dma((3,)),
            dma((1,)),
            dma((1,)),
            dma((sizes[2],)),
            dma((1,)),
            pltpu.SemaphoreType.REGULAR((4,)),
            vmem((3, 8, 128), F32),
            vmem((3, 8, 128), F32),
            vmem((1, 178), jnp.int32),
            vmem((2, SLOTS), jnp.int32),
            vmem((7, 128), jnp.int32),
            dma((5,)),
            vmem((6, 8, 128), F32),
            vmem((max(plane, sizes[0]) - 1, 1, 128), F32),
            vmem((24, 128), F32),
            vmem((4, 8, 128), jnp.int32),
            vmem((2, 8, 128), F32),
        ],
        compiler_params=pltpu.CompilerParams(
            collective_id=0, has_side_effects=True, vmem_limit_bytes=VMEM_LIMIT
        ),
        name="membrane",
    )(
        *[
            pltpu.with_memory_space_constraint(x, pltpu.HBM)
            for x in (
                positions,
                velocities,
                send_list.reshape(1, -1),
                pair_list,
                constraint_flags,
            )
        ]
    )
    position, velocity, energies = pl.pallas_call(
        functools.partial(finish, 8 * 128 * sizes[0] * sizes[1] * sizes[2]),
        out_shape=(
            jax.ShapeDtypeStruct((3, 8, 128), F32),
            jax.ShapeDtypeStruct((3, 8, 128), F32),
            jax.ShapeDtypeStruct((2, ITERS), F32),
        ),
        in_specs=[pl.BlockSpec(memory_space=vmem)] * 3,
        out_specs=[pl.BlockSpec(memory_space=pltpu.HBM)] * 3,
        scratch_shapes=[vmem((2, ITERS), F32), dma((3,))],
        compiler_params=pltpu.CompilerParams(vmem_limit_bytes=1 << 20),
        name="finish",
    )(*results)
    return position, velocity, energies.T


def solution(mesh):
    sizes = tuple(mesh.shape[a] for a in AXES)
    spec = ("runs", "gx", "gy", "gz")
    return jax.shard_map(
        functools.partial(on_device, sizes),
        mesh=mesh,
        in_specs=(
            P(None, None, spec),
            P(None, None, spec),
            P(spec),
            P(None, spec),
            P(None, spec),
        ),
        out_specs=(P(None, None, spec), P(None, None, spec), P("runs", None)),
        check_vma=False,
    )
```

```python
import functools

import jax
import jax.numpy as jnp
from jax import lax
from jax.experimental import pallas as pl
from jax.experimental.pallas import tpu as pltpu
from jax.sharding import PartitionSpec as P

CX, CY, CZ = 1, 8, 16
ITERS = 3
NORDER = 4
time_step = 0.02
root_half = 0.7071067811865476
MESH = pl.DeviceIdType.MESH
ZONES = ((1, 0, 0), (0, 1, 0), (0, 0, 1), (1, 1, 0), (1, 0, 1), (0, 1, 1), (1, 1, 1))
AXES = ("gx", "gy", "gz")
FIRST, SECOND = 24, 26
FAR, NEAR = (3, 6, 4, 5), (1, 2)
GROUPS = 14
SLOTS = 1792
PITCH = 24
F32 = jnp.float32


def roll(x, by, axis):
    size = x.shape[axis]
    by = by % size
    return x if by == 0 else pltpu.roll(x, by, axis)


def lanes(rows=8):
    return lax.broadcasted_iota(jnp.int32, (rows, 128), 1)


def side_by_side(parts, first, width):
    lane = lanes()
    return jnp.where(
        lane < first + width,
        parts[0],
        jnp.where(lane < first + 2 * width, roll(parts[1], width, 1), roll(parts[2], 2 * width, 1)),
    )


def merge(zone, received):
    block = received[0]
    for n in range(1, len(received)):
        block = jnp.where(zone >= n, received[n], block)
    return block


PASSES = ((0, 8), (8, 4), (12, 2))


def place(side, g):
    for begin, width in PASSES:
        if g < begin + width:
            return 2 * begin + width * side + g - begin


def pass_of(g):
    return max(n for n, (begin, _) in enumerate(PASSES) if begin <= g)


def where_is(side, p, c, k):
    width = PASSES[p][1]
    return sum(3 * w for _, w in PASSES[:p]) + c * width + k if side == 0 else 42 + 24 * p + 8 * c + k


def rows_of(row, width, k):
    sublane = lax.broadcasted_iota(jnp.int32, (8, 128), 0)
    value = jnp.broadcast_to(row(k), (8, 128))
    for n in range(1, 8 // width):
        value = jnp.where(sublane >= n * width, jnp.broadcast_to(row(k + n * width), (8, 128)), value)
    return value


def halves(value):
    high = value.astype(jnp.bfloat16).astype(F32)
    return jnp.concatenate([high, value - high], axis=0).astype(jnp.bfloat16)


def pick(table, index):
    return jnp.take_along_axis(table, index, axis=1, mode="promise_in_bounds")


def up(x):
    return roll(x, -1, 0)


def down(x):
    return roll(x, 1, 0)


def dot3(a, b):
    return a[0] * b[0] + a[1] * b[1] + a[2] * b[2]


def lag(x, by):
    return roll(x, -by, 0)


def expansion(coupling):
    coupling_down = down(coupling)
    power = {0: None}
    weights = {0: jnp.ones(coupling.shape, F32)}
    for _ in range(NORDER):
        later = {}
        for m, weight in power.items():
            lower = coupling_down if weight is None else coupling_down * down(weight)
            upper = coupling if weight is None else coupling * up(weight)
            for where_to, term in ((m - 1, lower), (m + 1, upper)):
                later[where_to] = later[where_to] + term if where_to in later else term
        power = later
        for m, weight in power.items():
            weights[m] = weights[m] + weight if m in weights else weight
    return [weights[m] for m in range(-NORDER, NORDER + 1)]


def expand(weights, source):
    terms = [w * lag(source, m - NORDER) for m, w in enumerate(weights)]
    while len(terms) > 1:
        terms = [
            terms[n] + terms[n + 1] if n + 1 < len(terms) else terms[n]
            for n in range(0, len(terms), 2)
        ]
    return terms[0]


def link_frame(previous, flags_pair):
    old = [x - up(x) for x in previous]
    length = jnp.maximum(jnp.sqrt(dot3(old, old)), 0.2)
    direction = [x / length for x in old]
    coupling = 0.5 * dot3(direction, [up(x) for x in direction]) * flags_pair
    return direction, expansion(coupling)


def constrain(updated, direction, weights, rest, flags):
    links = [x - up(x) for x in updated]
    solution = expand(weights, flags * root_half * (dot3(direction, links) - rest))
    shifts = [x * (root_half * solution) for x in direction]
    updated = [x - s + down(s) for x, s in zip(updated, shifts)]
    links = [x - (s + s) + (down(s) + up(s)) for x, s in zip(links, shifts)]
    squared = dot3(links, links)
    target = jnp.sqrt(jnp.maximum(2.0 * rest * rest - squared, 0.25 * rest * rest))
    solution = expand(weights, flags * root_half * (rest - target))
    shifts = [x * (root_half * solution) for x in direction]
    return [x - s + down(s) for x, s in zip(updated, shifts)]


def kernel(
    sizes,
    pos_in,
    vel_in,
    send_in,
    pair_in,
    flag_in,
    out_pos,
    out_vel,
    out_en,
    cur,
    half_ref,
    rest_ref,
    ids,
    send_ids,
    flag8,
    table,
    back,
    back2,
    near,
    frame,
    pair_x,
    pair_f,
    coord_x,
    coord_m,
    force_x,
    force_m,
    got_x,
    got_m,
    ret_x,
    ret_m,
    row,
    plane,
    mid,
    line,
    c_send,
    c_recv,
    f_send,
    f_recv,
    p_send,
    p_recv,
    l_send,
    l_recv,
    token,
    pos_ref,
    vel_ref,
    send_ref,
    pair_ref,
    flag_ref,
    loaded,
    blocks_ref,
    rows_ref,
    speed_ref,
    packed,
    shift,
):
    me = tuple(lax.axis_index(a) for a in AXES)

    def at(offset):
        return {
            a: lax.rem(me[i] + (offset[i] % sizes[i]), sizes[i])
            for i, a in enumerate(AXES)
            if offset[i] % sizes[i]
        }

    loads = [
        pltpu.make_async_copy(source, target, loaded.at[n])
        for n, (source, target) in enumerate(
            (
                (send_in, send_ref),
                (pos_in, pos_ref),
                (pair_in, pair_ref),
                (vel_in, vel_ref),
                (flag_in, flag_ref),
            )
        )
    ]
    for load in loads[:2]:
        load.start()
    barrier = pltpu.get_barrier_semaphore()
    for number in FAR + (0,) + NEAR:
        pl.semaphore_signal(
            barrier, inc=1, device_id=at(ZONES[number]), device_id_type=MESH
        )
    for load in loads[2:]:
        load.start()

    lane = lanes()
    row[...] = jnp.zeros(row.shape, F32)
    loads[0].wait()
    loads[1].wait()
    send_ids[...] = jnp.full(send_ids.shape, -1, jnp.int32)
    send_ids[pl.ds(0, 1), :] = send_ref[:, pl.ds(0, 128)]
    send_ids[pl.ds(1, 1), pl.ds(0, FIRST + SECOND)] = send_ref[:, pl.ds(128, FIRST + SECOND)]
    for c in range(3):
        cur[pl.ds(8 * c, 8), :] = pos_ref[c]

    def prepare():
        for load in loads[2:]:
            load.wait()
        for c in range(3):
            half_ref[pl.ds(8 * c, 8), :] = vel_ref[c]
        for side in range(2):
            for p, (begin, width) in enumerate(PASSES):
                for n in range(8):
                    g = begin + n % width
                    ids[pl.ds(24 * side + 8 * p + n, 1), :] = pair_ref[
                        pl.ds(side, 1), pl.ds(128 * g, 128)
                    ]
        flag8[...] = jnp.zeros(flag8.shape, F32)
        flag8[pl.ds(0, 7), :] = flag_ref[...].astype(F32)
        columns = jnp.transpose(ids[...].astype(F32))
        entry = jnp.broadcast_to(send_ids[pl.ds(1, 1), :], (8, 128))
        goals = [entry + 128 * c for c in range(3)]
        for n, (first, width) in enumerate(((0, FIRST), (FIRST, SECOND))):
            goal = side_by_side(goals, first, width)
            goal = jnp.where((lane >= first) & (lane < first + 3 * width), goal, -1)
            send_ids[pl.ds(2 + n, 1), :] = goal[:1]
        send_columns = jnp.transpose(send_ids[...].astype(F32))
        wide = lax.broadcasted_iota(jnp.int32, (128, 384), 1).astype(F32)
        for side in range(2):
            value = 12.0 if side == 0 else -12.0
            for g in range(GROUPS):
                at_row = 24 * side + 8 * pass_of(g) + g - PASSES[pass_of(g)][0]
                column = columns[:, at_row : at_row + 1]
                table[pl.ds(128 * place(side, g), 128), :] = jnp.where(
                    wide == column, value, 0.0
                ).astype(jnp.bfloat16)
        back[...] = jnp.where(wide[:, :128] == send_columns[:, 0:1], 1.0, 0.0).astype(jnp.bfloat16)
        for b in range(2):
            back2[pl.ds(128 * b, 128), :] = jnp.where(
                wide == send_columns[:, 2 + b : 3 + b], 1.0, 0.0
            ).astype(jnp.bfloat16)
        links = [pos_ref[c] - up(pos_ref[c]) for c in range(3)]
        rest_ref[...] = jnp.sqrt(dot3(links, links))

    ring = [tuple(sign if a == axis else 0 for a in range(3)) for axis in (0, 1) for sign in (1, -1)]

    def tell():
        for number, offset in enumerate(ring):
            pl.semaphore_signal(
                token.at[number], inc=1, device_id=at(offset), device_id_type=MESH
            )

    def hear():
        for number in range(len(ring)):
            pl.semaphore_wait(token.at[number], 1)

    def coord_copies():
        copies = []
        for number, zone in enumerate(ZONES):
            source = coord_x if number == 0 else coord_m.at[0 if number < 3 else 1]
            target = got_x if number == 0 else got_m.at[number - 1]
            copies.append(
                pltpu.make_async_remote_copy(
                    src_ref=source,
                    dst_ref=target,
                    send_sem=c_send.at[0 if number == 0 else 1],
                    recv_sem=c_recv.at[0 if number == 0 else 1 if number in NEAR else 2],
                    device_id=at(tuple(-z for z in zone)),
                    device_id_type=MESH,
                )
            )
        return copies

    def force_copies():
        copies = []
        for number, zone in enumerate(ZONES):
            source = force_x if number == 0 else force_m.at[0 if number < 3 else 1]
            target = ret_x if number == 0 else ret_m.at[number - 1]
            copies.append(
                pltpu.make_async_remote_copy(
                    src_ref=source,
                    dst_ref=target,
                    send_sem=f_send.at[0 if number == 0 else 1],
                    recv_sem=f_recv.at[0 if number == 0 else 1 if number in NEAR else 2],
                    device_id=at(zone),
                    device_id_type=MESH,
                )
            )
        return copies

    def drain(sem, ref):
        pltpu.make_async_copy(ref, ref, sem).wait()

    def kinetic(speed, number):
        total = jnp.sum(
            jnp.sum(dot3(speed, speed), axis=0, keepdims=True), axis=1, keepdims=True
        )
        row[...] = jnp.where(lanes(1) == KINETIC + number, 0.5 * total, row[...])

    edges = (0, 16, 24, 40, 48, 49, 50)
    entry = jnp.broadcast_to(send_ids[pl.ds(1, 1), :], (8, 128))
    for n, (first, width) in enumerate(((0, FIRST), (FIRST, SECOND))):
        zone = jnp.zeros((8, 128), jnp.int32)
        offset = [jnp.zeros((8, 128), F32) for _ in range(3)]
        for number in range(1, 7):
            begin = edges[number - 1]
            inside = (lane >= begin) & (lane < edges[number])
            zone = jnp.where(inside, number - 1 if n == 0 else number - 3, zone)
            for c, length in enumerate((CX, CY, CZ)):
                if ZONES[number][c]:
                    offset[c] = jnp.where(inside, F32(length), offset[c])
        packed[n] = side_by_side([zone] * 3, first, width)
        packed[2 + n] = jnp.maximum(side_by_side([entry] * 3, first, width), 0)
        shift[n] = side_by_side(offset, first, width)

    def chosen(n, home):
        first, width = ((0, FIRST), (FIRST, SECOND))[n]
        index = packed[2 + n]
        picked = [pick(x, index) for x in home]
        return shift[n] + jnp.where(
            lane < first + width,
            picked[0],
            jnp.where(lane < first + 2 * width, picked[1], picked[2]),
        )

    def build_x(home):
        send_x = jnp.broadcast_to(send_ids[pl.ds(0, 1), :], (8, 128))
        for c in range(3):
            value = pick(home[c], send_x)
            coord_x[pl.ds(8 * c, 8), :] = value + F32(CX) if c == 0 else value

    def send_coords(home):
        copies = coord_copies()
        coord_m[1] = chosen(1, home)
        for number in FAR:
            copies[number].start()
        coord_m[0] = chosen(0, home)
        for number in NEAR:
            copies[number].start()
        build_x(home)
        copies[0].start()

    start = [pos_ref[c] for c in range(3)]
    coord_m[1] = chosen(1, start)
    coord_m[0] = chosen(0, start)
    build_x(start)
    pl.semaphore_wait(barrier, len(ZONES))
    copies = coord_copies()
    for number in FAR + NEAR + (0,):
        copies[number].start()

    def step(t, carry):
        copies = coord_copies()
        pl.when(t == 0)(prepare)

        @pl.when(t > 0)
        def _():
            pl.when(t > 1)(hear)
            tell()
            force_copies()[0].wait_send()
            drain(f_send.at[1], blocks_ref)
            kinetic([speed_ref[pl.ds(8 * c, 8), :] for c in range(3)], t - 2)

        index = [[ids[pl.ds(24 * side + 8 * p, 8), :] for p in range(3)] for side in range(2)]
        low = [[x & 127 for x in side] for side in index]

        def gather(row, keep, places, which):
            for side, p, k in which:
                width = PASSES[p][1]
                for c in range(3):
                    if side == 0:
                        source = rows_of(lambda n: row(c, n), width, k)
                    else:
                        source = jnp.broadcast_to(row(c, k), (8, 128))
                    slot = where_is(side, p, c, k)
                    value = pick(source, places[side][p][c])
                    if keep is not None:
                        value = jnp.where(keep[side][p], pair_x[slot], value)
                    pair_x[slot] = value

        def blocks_of(passes):
            return [(1, p, k) for k in range(8) for p in passes] + [
                (0, p, k) for p in passes for k in range(PASSES[p][1])
            ]

        everywhere = [[[x] * 3 for x in side] for side in low]
        gather(lambda c, k: cur[pl.ds(8 * c + k, 1), :], None, everywhere, blocks_of(range(3)))

        not_x = [[(x < 128) | (x >= 256) for x in side] for side in index]
        in_x = [[x < 256 for x in side] for side in index]
        in_near = [[x < 256 + FIRST for x in side] for side in index]
        near_place, far_place = [
            [[[(x + width * c) & 127 for c in range(3)] for x in side] for side in low]
            for width in (FIRST, SECOND)
        ]
        drain(c_recv.at[1], blocks_ref.at[pl.ds(0, 2)])
        near[pl.ds(0, 8), :] = merge(packed[0], [got_m[n] for n in range(2)])
        gather(lambda c, k: near[pl.ds(k, 1), :], in_x, near_place, blocks_of(range(3)))

        copies[0].wait_recv()
        gather(lambda c, k: got_x[pl.ds(8 * c + k, 1), :], not_x, everywhere, blocks_of(range(3)))

        drain(c_recv.at[2], blocks_ref.at[pl.ds(0, 4)])
        near[pl.ds(8, 8), :] = merge(packed[1], [got_m[n] for n in range(2, 6)])

        def complete(which):
            gather(lambda c, k: near[pl.ds(8 + k, 1), :], in_near, far_place, which)

        complete(blocks_of(range(1)))

        energy = jnp.zeros((8, 128), F32)
        sublane = lax.broadcasted_iota(jnp.int32, (8, 128), 0)
        lefts = []
        parts = []
        for p, (begin, width) in enumerate(PASSES):
            usable = jnp.where(index[0][p] == CL_PAD, 0.0, 1.0)
            distinct = jnp.where(index[0][p] == index[1][p], 0.0, usable)
            limits = [distinct]
            for n in range(1, 8 // width):
                limits.append(jnp.where(sublane < n * width, usable, distinct))
            limits.append(usable)
            second = [[None] * 3 for _ in range(8)]
            for k in range(width):
                xi = [pair_x[where_is(0, p, c, k)] for c in range(3)]
                first = [None] * 3
                for l in range(8):
                    limit = limits[min(max(-((k - l) // width), 0), 8 // width)]
                    d = [xi[c] - pair_x[where_is(1, p, c, l)] for c in range(3)]
                    u = jnp.maximum(limit - dot3(d, d), 0.0)
                    uu = u * u
                    energy = energy + uu * u
                    for c in range(3):
                        push = uu * d[c]
                        first[c] = push if l == 0 else first[c] + push
                        second[l][c] = push if k == 0 else second[l][c] + push
                for n in range(8 // width):
                    for c in range(3):
                        pair_f[pl.ds((8 * c + k + n * width) * PITCH + begin, width), :] = roll(
                            first[c], -n * width, 0
                        )[:width]
                if p == 0:
                    complete(
                        [(1, 1, k), (1, 2, k)]
                        + ([(0, 1, k)] if k < 4 else [(0, 2, k - 4)] if k < 6 else [])
                    )
            for l in range(8):
                for c in range(3):
                    value = second[l][c]
                    turn = 4
                    while turn >= width:
                        value = value + roll(value, turn, 0)
                        turn //= 2
                    pair_f[pl.ds((24 + 8 * c + l) * PITCH + begin, width), :] = value[:width]
            left = jnp.concatenate(
                [
                    halves(pair_f[pl.ds(24 * PITCH * side + g, 24, stride=PITCH), :])
                    for side in range(2)
                    for g in range(begin, begin + width)
                ],
                axis=1,
            )
            lefts.append(left)
            parts.append(
                jnp.dot(
                    left,
                    table[
                        pl.ds(256 * begin, left.shape[1]),
                        pl.ds(128 if p == 0 else 256, 256 if p == 0 else 128),
                    ],
                    preferred_element_type=F32,
                )
            )

        halo = parts[0][:, 128:] + parts[1] + parts[2]
        halo = halo[:24] + halo[24:]
        returns = force_copies()
        beyond = [halo[8 * c : 8 * c + 8] for c in range(3)]
        force_m[1] = side_by_side(beyond, FIRST, SECOND)
        for number in FAR:
            returns[number].start()
        force_m[0] = side_by_side(beyond, 0, FIRST)
        for number in NEAR:
            returns[number].start()
        rest = jnp.dot(
            jnp.concatenate(lefts[1:], axis=1),
            table[pl.ds(2048, 1536), pl.ds(0, 256)],
            preferred_element_type=F32,
        )
        halo = parts[0][:, :128] + rest[:, 128:]
        force_x[...] = halo[:24] + halo[24:]
        returns[0].start()
        own = rest[:, :128] + jnp.dot(
            lefts[0], table[pl.ds(0, 2048), pl.ds(0, 128)], preferred_element_type=F32
        )
        own = own[:24] + own[24:]
        @pl.when(t > 0)
        def _():
            hear()
            tell()

        total = jnp.sum(jnp.sum(energy, axis=0, keepdims=True), axis=1, keepdims=True)
        row[...] = jnp.where(lanes(1) == t - 1, 2.0 * total, row[...])
        flags = flag8[...]
        direction, weights = link_frame(
            [cur[pl.ds(8 * c, 8), :] for c in range(3)], flags * up(flags)
        )
        for n, value in enumerate(direction + weights):
            frame[pl.ds(8 * n, 8), :] = value

        copies[0].wait_send()
        drain(c_send.at[1], blocks_ref)
        returns[0].wait_recv()
        came = jnp.dot(
            halves(ret_x[...]), back[...], preferred_element_type=F32
        )
        own = own + came[:24] + came[24:]
        drain(f_recv.at[1], blocks_ref.at[pl.ds(0, 2)])
        came = merge(packed[0], [ret_m[n] for n in range(2)])
        came = jnp.dot(halves(came), back2[pl.ds(0, 128), :], preferred_element_type=F32)
        came = came[:8] + came[8:]
        own = [
            own[8 * c : 8 * c + 8] + came[:, 128 * c : 128 * c + 128] for c in range(3)
        ]
        drain(f_recv.at[2], blocks_ref.at[pl.ds(0, 4)])
        came = merge(packed[1], [ret_m[n] for n in range(2, 6)])
        came = jnp.dot(halves(came), back2[pl.ds(128, 128), :], preferred_element_type=F32)
        came = came[:8] + came[8:]
        force = [
            0.5 * time_step * (own[c] + came[:, 128 * c : 128 * c + 128])
            for c in range(3)
        ]

        again = jnp.where(t > 0, 1.0, 0.0).astype(F32)
        speed = [half_ref[pl.ds(8 * c, 8), :] + again * force[c] for c in range(3)]

        @pl.when(t < ITERS)
        def _():
            half = [speed[c] + force[c] for c in range(3)]
            before = [cur[pl.ds(8 * c, 8), :] for c in range(3)]
            moved = constrain(
                [x + time_step * v for x, v in zip(before, half)],
                [frame[pl.ds(8 * n, 8), :] for n in range(3)],
                [frame[pl.ds(8 * n, 8), :] for n in range(3, 3 + 2 * NORDER + 1)],
                rest_ref[...],
                flag8[...],
            )
            send_coords(moved)
            for c in range(3):
                cur[pl.ds(8 * c, 8), :] = moved[c]
                half_ref[pl.ds(8 * c, 8), :] = (moved[c] - before[c]) / time_step
                speed_ref[pl.ds(8 * c, 8), :] = speed[c]

        @pl.when(t == ITERS)
        def _():
            kinetic(speed, ITERS - 1)
            for c in range(3):
                out_pos[c] = cur[pl.ds(8 * c, 8), :]
                out_vel[c] = speed[c]

        return carry

    lax.fori_loop(0, ITERS + 1, step, 0)
    def distance(offset):
        return sum(min(o, n - o) for o, n in zip(offset, sizes))

    def copy_row(source, target, offset, send, recv):
        pltpu.make_async_remote_copy(
            src_ref=source,
            dst_ref=target,
            send_sem=send,
            recv_sem=recv,
            device_id=at(offset),
            device_id_type=MESH,
        ).start()

    def total_of(slots):
        terms = [slots[n] for n in range(slots.shape[0])]
        while len(terms) > 1:
            terms = [
                terms[n] + terms[n + 1] if n + 1 < len(terms) else terms[n]
                for n in range(0, len(terms), 2)
            ]
        return terms[0]

    offsets = [(0, y, z) for y in range(sizes[1]) for z in range(sizes[2]) if y or z]
    own = me[1] * sizes[2] + me[2]
    for offset in sorted(offsets, key=distance, reverse=True):
        copy_row(row, plane.at[own], offset, p_send.at[0], p_recv.at[0])
    plane[own] = row[...]
    hear()
    tell()
    force_copies()[0].wait_send()
    drain(f_send.at[1], blocks_ref)
    hear()
    drain(p_recv.at[0], rows_ref.at[pl.ds(0, len(offsets))])
    mid[...] = total_of(plane)
    offsets = sorted([(x, 0, 0) for x in range(1, sizes[0])], key=distance)
    lead = me[2] == sizes[2] - 1

    @pl.when(lead)
    def _():
        for x, _, _ in offsets:
            for z in range(sizes[2]):
                copy_row(mid, line.at[me[0]], (x, 0, z), l_send.at[z], l_recv.at[0])

    line[me[0]] = mid[...]
    drain(p_send.at[0], rows_ref.at[pl.ds(0, plane.shape[0] - 1)])
    drain(l_recv.at[0], rows_ref.at[pl.ds(0, len(offsets))])
    out_en[...] = total_of(line)

    @pl.when(lead)
    def _():
        for z in range(sizes[2]):
            drain(l_send.at[z], rows_ref.at[pl.ds(0, len(offsets))])


CL_PAD = 306
KINETIC = 8
VMEM_LIMIT = 12 << 20


def finish(beads, pos_ref, vel_ref, sum_ref, out_pos, out_vel, out_en, energy, stored):
    stores = [
        pltpu.make_async_copy(source, target, stored.at[n])
        for n, (source, target) in enumerate(
            ((pos_ref, out_pos), (vel_ref, out_vel), (energy, out_en))
        )
    ]
    stores[0].start()
    stores[1].start()
    total = sum_ref[...] / F32(beads)
    for n in range(2):
        energy[pl.ds(n, 1), :] = total[:, KINETIC * n : KINETIC * n + ITERS]
    stores[2].start()
    for store in stores:
        store.wait()


def on_device(sizes, positions, velocities, send_list, pair_list, constraint_flags):
    dma = pltpu.SemaphoreType.DMA
    vmem = pltpu.VMEM
    plane = sizes[1] * sizes[2]
    results = pl.pallas_call(
        functools.partial(kernel, sizes),
        out_shape=(
            jax.ShapeDtypeStruct((3, 8, 128), F32),
            jax.ShapeDtypeStruct((3, 8, 128), F32),
            jax.ShapeDtypeStruct((1, 128), F32),
        ),
        in_specs=[pl.BlockSpec(memory_space=pltpu.HBM)] * 5,
        out_specs=[pl.BlockSpec(memory_space=vmem)] * 3,
        scratch_shapes=[
            vmem((24, 128), F32),
            vmem((24, 128), F32),
            vmem((8, 128), F32),
            vmem((48, 128), jnp.int32),
            vmem((8, 128), jnp.int32),
            vmem((8, 128), F32),
            vmem((2 * SLOTS, 384), jnp.bfloat16),
            vmem((128, 128), jnp.bfloat16),
            vmem((256, 384), jnp.bfloat16),
            vmem((16, 128), F32),
            vmem((24 + 8 * (2 * NORDER + 1), 128), F32),
            vmem((114, 8, 128), F32),
            vmem((48 * PITCH, 128), F32),
            vmem((24, 128), F32),
            vmem((2, 8, 128), F32),
            vmem((24, 128), F32),
            vmem((2, 8, 128), F32),
            vmem((24, 128), F32),
            vmem((6, 8, 128), F32),
            vmem((24, 128), F32),
            vmem((6, 8, 128), F32),
            vmem((1, 128), F32),
            vmem((plane, 1, 128), F32),
            vmem((1, 128), F32),
            vmem((sizes[0], 1, 128), F32),
            dma((2,)),
            dma((3,)),
            dma((2,)),
            dma((3,)),
            dma((1,)),
            dma((1,)),
            dma((sizes[2],)),
            dma((1,)),
            pltpu.SemaphoreType.REGULAR((4,)),
            vmem((3, 8, 128), F32),
            vmem((3, 8, 128), F32),
            vmem((1, 178), jnp.int32),
            vmem((2, SLOTS), jnp.int32),
            vmem((7, 128), jnp.int32),
            dma((5,)),
            vmem((6, 8, 128), F32),
            vmem((max(plane, sizes[0]) - 1, 1, 128), F32),
            vmem((24, 128), F32),
            vmem((4, 8, 128), jnp.int32),
            vmem((2, 8, 128), F32),
        ],
        compiler_params=pltpu.CompilerParams(
            collective_id=0, has_side_effects=True, vmem_limit_bytes=VMEM_LIMIT
        ),
        name="membrane",
    )(
        *[
            pltpu.with_memory_space_constraint(x, pltpu.HBM)
            for x in (
                positions,
                velocities,
                send_list.reshape(1, -1),
                pair_list,
                constraint_flags,
            )
        ]
    )
    position, velocity, energies = pl.pallas_call(
        functools.partial(finish, 8 * 128 * sizes[0] * sizes[1] * sizes[2]),
        out_shape=(
            jax.ShapeDtypeStruct((3, 8, 128), F32),
            jax.ShapeDtypeStruct((3, 8, 128), F32),
            jax.ShapeDtypeStruct((2, ITERS), F32),
        ),
        in_specs=[pl.BlockSpec(memory_space=vmem)] * 3,
        out_specs=[pl.BlockSpec(memory_space=pltpu.HBM)] * 3,
        scratch_shapes=[vmem((2, ITERS), F32), dma((3,))],
        compiler_params=pltpu.CompilerParams(vmem_limit_bytes=1 << 20),
        name="finish",
    )(*results)
    return position, velocity, energies.T


def solution(mesh):
    sizes = tuple(mesh.shape[a] for a in AXES)
    spec = ("runs", "gx", "gy", "gz")
    return jax.shard_map(
        functools.partial(on_device, sizes),
        mesh=mesh,
        in_specs=(
            P(None, None, spec),
            P(None, None, spec),
            P(spec),
            P(None, spec),
            P(None, spec),
        ),
        out_specs=(P(None, None, spec), P(None, None, spec), P("runs", None)),
        check_vma=False,
    )
```

```python
import functools

import jax
import jax.numpy as jnp
from jax import lax
from jax.experimental import pallas as pl
from jax.experimental.pallas import tpu as pltpu
from jax.sharding import PartitionSpec as P

CX, CY, CZ = 1, 8, 16
ITERS = 3
NORDER = 4
time_step = 0.02
root_half = 0.7071067811865476
MESH = pl.DeviceIdType.MESH
ZONES = ((1, 0, 0), (0, 1, 0), (0, 0, 1), (1, 1, 0), (1, 0, 1), (0, 1, 1), (1, 1, 1))
AXES = ("gx", "gy", "gz")
FIRST, SECOND = 24, 26
FAR, NEAR = (3, 6, 4, 5), (1, 2)
GROUPS = 14
SLOTS = 1792
PITCH = 24
F32 = jnp.float32


def roll(x, by, axis):
    size = x.shape[axis]
    by = by % size
    return x if by == 0 else pltpu.roll(x, by, axis)


def lanes(rows=8):
    return lax.broadcasted_iota(jnp.int32, (rows, 128), 1)


def side_by_side(parts, first, width):
    lane = lanes()
    return jnp.where(
        lane < first + width,
        parts[0],
        jnp.where(lane < first + 2 * width, roll(parts[1], width, 1), roll(parts[2], 2 * width, 1)),
    )


def merge(zone, received):
    block = received[0]
    for n in range(1, len(received)):
        block = jnp.where(zone >= n, received[n], block)
    return block


PASSES = ((0, 8), (8, 4), (12, 2))


def place(side, g):
    for begin, width in PASSES:
        if g < begin + width:
            return 2 * begin + width * side + g - begin


def pass_of(g):
    return max(n for n, (begin, _) in enumerate(PASSES) if begin <= g)


def where_is(side, p, c, k):
    width = PASSES[p][1]
    return sum(3 * w for _, w in PASSES[:p]) + c * width + k if side == 0 else 42 + 24 * p + 8 * c + k


def rows_of(row, width, k):
    sublane = lax.broadcasted_iota(jnp.int32, (8, 128), 0)
    value = jnp.broadcast_to(row(k), (8, 128))
    for n in range(1, 8 // width):
        value = jnp.where(sublane >= n * width, jnp.broadcast_to(row(k + n * width), (8, 128)), value)
    return value


def halves(value):
    high = value.astype(jnp.bfloat16).astype(F32)
    return jnp.concatenate([high, value - high], axis=0).astype(jnp.bfloat16)


def pick(table, index):
    return jnp.take_along_axis(table, index, axis=1, mode="promise_in_bounds")


def up(x):
    return roll(x, -1, 0)


def down(x):
    return roll(x, 1, 0)


def dot3(a, b):
    return a[0] * b[0] + a[1] * b[1] + a[2] * b[2]


def lag(x, by):
    return roll(x, -by, 0)


def expansion(coupling):
    coupling_down = down(coupling)
    power = {0: None}
    weights = {0: jnp.ones(coupling.shape, F32)}
    for _ in range(NORDER):
        later = {}
        for m, weight in power.items():
            lower = coupling_down if weight is None else coupling_down * down(weight)
            upper = coupling if weight is None else coupling * up(weight)
            for where_to, term in ((m - 1, lower), (m + 1, upper)):
                later[where_to] = later[where_to] + term if where_to in later else term
        power = later
        for m, weight in power.items():
            weights[m] = weights[m] + weight if m in weights else weight
    return [weights[m] for m in range(-NORDER, NORDER + 1)]


def expand(weights, source):
    terms = [w * lag(source, m - NORDER) for m, w in enumerate(weights)]
    while len(terms) > 1:
        terms = [
            terms[n] + terms[n + 1] if n + 1 < len(terms) else terms[n]
            for n in range(0, len(terms), 2)
        ]
    return terms[0]


def link_frame(previous, flags_pair):
    old = [x - up(x) for x in previous]
    length = jnp.maximum(jnp.sqrt(dot3(old, old)), 0.2)
    direction = [x / length for x in old]
    coupling = 0.5 * dot3(direction, [up(x) for x in direction]) * flags_pair
    return direction, expansion(coupling)


def constrain(updated, direction, weights, rest, flags):
    links = [x - up(x) for x in updated]
    solution = expand(weights, flags * root_half * (dot3(direction, links) - rest))
    shifts = [x * (root_half * solution) for x in direction]
    updated = [x - s + down(s) for x, s in zip(updated, shifts)]
    links = [x - (s + s) + (down(s) + up(s)) for x, s in zip(links, shifts)]
    squared = dot3(links, links)
    target = jnp.sqrt(jnp.maximum(2.0 * rest * rest - squared, 0.25 * rest * rest))
    solution = expand(weights, flags * root_half * (rest - target))
    shifts = [x * (root_half * solution) for x in direction]
    return [x - s + down(s) for x, s in zip(updated, shifts)]


def kernel(
    sizes,
    pos_in,
    vel_in,
    send_in,
    pair_in,
    flag_in,
    out_pos,
    out_vel,
    out_en,
    cur,
    half_ref,
    rest_ref,
    ids,
    send_ids,
    flag8,
    table,
    back,
    back2,
    near,
    frame,
    pair_x,
    pair_f,
    coord_x,
    coord_m,
    force_x,
    force_m,
    got_x,
    got_m,
    ret_x,
    ret_m,
    row,
    plane,
    mid,
    line,
    c_send,
    c_recv,
    f_send,
    f_recv,
    p_send,
    p_recv,
    l_send,
    l_recv,
    token,
    pos_ref,
    vel_ref,
    send_ref,
    pair_ref,
    flag_ref,
    loaded,
    blocks_ref,
    rows_ref,
    speed_ref,
    packed,
    shift,
):
    me = tuple(lax.axis_index(a) for a in AXES)

    def at(offset):
        return {
            a: lax.rem(me[i] + (offset[i] % sizes[i]), sizes[i])
            for i, a in enumerate(AXES)
            if offset[i] % sizes[i]
        }

    loads = [
        pltpu.make_async_copy(source, target, loaded.at[n])
        for n, (source, target) in enumerate(
            (
                (send_in, send_ref),
                (pos_in, pos_ref),
                (pair_in, pair_ref),
                (vel_in, vel_ref),
                (flag_in, flag_ref),
            )
        )
    ]
    for load in loads[:2]:
        load.start()
    barrier = pltpu.get_barrier_semaphore()
    for number in FAR + (0,) + NEAR:
        pl.semaphore_signal(
            barrier, inc=1, device_id=at(ZONES[number]), device_id_type=MESH
        )
    for load in loads[2:]:
        load.start()

    lane = lanes()
    row[...] = jnp.zeros(row.shape, F32)
    loads[0].wait()
    loads[1].wait()
    send_ids[...] = jnp.full(send_ids.shape, -1, jnp.int32)
    send_ids[pl.ds(0, 1), :] = send_ref[:, pl.ds(0, 128)]
    send_ids[pl.ds(1, 1), pl.ds(0, FIRST + SECOND)] = send_ref[:, pl.ds(128, FIRST + SECOND)]
    for c in range(3):
        cur[pl.ds(8 * c, 8), :] = pos_ref[c]

    def prepare():
        for load in loads[2:]:
            load.wait()
        for c in range(3):
            half_ref[pl.ds(8 * c, 8), :] = vel_ref[c]
        for side in range(2):
            for p, (begin, width) in enumerate(PASSES):
                for n in range(8):
                    g = begin + n % width
                    ids[pl.ds(24 * side + 8 * p + n, 1), :] = pair_ref[
                        pl.ds(side, 1), pl.ds(128 * g, 128)
                    ]
        flag8[...] = jnp.zeros(flag8.shape, F32)
        flag8[pl.ds(0, 7), :] = flag_ref[...].astype(F32)
        columns = jnp.transpose(ids[...].astype(F32))
        entry = jnp.broadcast_to(send_ids[pl.ds(1, 1), :], (8, 128))
        goals = [entry + 128 * c for c in range(3)]
        for n, (first, width) in enumerate(((0, FIRST), (FIRST, SECOND))):
            goal = side_by_side(goals, first, width)
            goal = jnp.where((lane >= first) & (lane < first + 3 * width), goal, -1)
            send_ids[pl.ds(2 + n, 1), :] = goal[:1]
        send_columns = jnp.transpose(send_ids[...].astype(F32))
        wide = lax.broadcasted_iota(jnp.int32, (128, 384), 1).astype(F32)
        for side in range(2):
            value = 12.0 if side == 0 else -12.0
            for g in range(GROUPS):
                at_row = 24 * side + 8 * pass_of(g) + g - PASSES[pass_of(g)][0]
                column = columns[:, at_row : at_row + 1]
                table[pl.ds(128 * place(side, g), 128), :] = jnp.where(
                    wide == column, value, 0.0
                ).astype(jnp.bfloat16)
        back[...] = jnp.where(wide[:, :128] == send_columns[:, 0:1], 1.0, 0.0).astype(jnp.bfloat16)
        for b in range(2):
            back2[pl.ds(128 * b, 128), :] = jnp.where(
                wide == send_columns[:, 2 + b : 3 + b], 1.0, 0.0
            ).astype(jnp.bfloat16)
        links = [pos_ref[c] - up(pos_ref[c]) for c in range(3)]
        rest_ref[...] = jnp.sqrt(dot3(links, links))

    ring = [tuple(sign if a == axis else 0 for a in range(3)) for axis in (0, 1) for sign in (1, -1)]

    def tell():
        for number, offset in enumerate(ring):
            pl.semaphore_signal(
                token.at[number], inc=1, device_id=at(offset), device_id_type=MESH
            )

    def hear():
        for number in range(len(ring)):
            pl.semaphore_wait(token.at[number], 1)

    def coord_copies():
        copies = []
        for number, zone in enumerate(ZONES):
            source = coord_x if number == 0 else coord_m.at[0 if number < 3 else 1]
            target = got_x if number == 0 else got_m.at[number - 1]
            copies.append(
                pltpu.make_async_remote_copy(
                    src_ref=source,
                    dst_ref=target,
                    send_sem=c_send.at[0 if number == 0 else 1],
                    recv_sem=c_recv.at[0 if number == 0 else 1 if number in NEAR else 2],
                    device_id=at(tuple(-z for z in zone)),
                    device_id_type=MESH,
                )
            )
        return copies

    def force_copies():
        copies = []
        for number, zone in enumerate(ZONES):
            source = force_x if number == 0 else force_m.at[0 if number < 3 else 1]
            target = ret_x if number == 0 else ret_m.at[number - 1]
            copies.append(
                pltpu.make_async_remote_copy(
                    src_ref=source,
                    dst_ref=target,
                    send_sem=f_send.at[0 if number == 0 else 1],
                    recv_sem=f_recv.at[0 if number == 0 else 1 if number in NEAR else 2],
                    device_id=at(zone),
                    device_id_type=MESH,
                )
            )
        return copies

    def drain(sem, ref):
        pltpu.make_async_copy(ref, ref, sem).wait()

    def kinetic(speed, number):
        total = jnp.sum(
            jnp.sum(dot3(speed, speed), axis=0, keepdims=True), axis=1, keepdims=True
        )
        row[...] = jnp.where(lanes(1) == KINETIC + number, 0.5 * total, row[...])

    edges = (0, 16, 24, 40, 48, 49, 50)
    entry = jnp.broadcast_to(send_ids[pl.ds(1, 1), :], (8, 128))
    for n, (first, width) in enumerate(((0, FIRST), (FIRST, SECOND))):
        zone = jnp.zeros((8, 128), jnp.int32)
        offset = [jnp.zeros((8, 128), F32) for _ in range(3)]
        for number in range(1, 7):
            begin = edges[number - 1]
            inside = (lane >= begin) & (lane < edges[number])
            zone = jnp.where(inside, number - 1 if n == 0 else number - 3, zone)
            for c, length in enumerate((CX, CY, CZ)):
                if ZONES[number][c]:
                    offset[c] = jnp.where(inside, F32(length), offset[c])
        packed[n] = side_by_side([zone] * 3, first, width)
        packed[2 + n] = jnp.maximum(side_by_side([entry] * 3, first, width), 0)
        shift[n] = side_by_side(offset, first, width)

    def chosen(n, home):
        first, width = ((0, FIRST), (FIRST, SECOND))[n]
        index = packed[2 + n]
        picked = [pick(x, index) for x in home]
        return shift[n] + jnp.where(
            lane < first + width,
            picked[0],
            jnp.where(lane < first + 2 * width, picked[1], picked[2]),
        )

    def build_x(home):
        send_x = jnp.broadcast_to(send_ids[pl.ds(0, 1), :], (8, 128))
        for c in range(3):
            value = pick(home[c], send_x)
            coord_x[pl.ds(8 * c, 8), :] = value + F32(CX) if c == 0 else value

    def send_coords(home):
        copies = coord_copies()
        coord_m[1] = chosen(1, home)
        for number in FAR:
            copies[number].start()
        coord_m[0] = chosen(0, home)
        for number in NEAR:
            copies[number].start()
        build_x(home)
        copies[0].start()

    start = [pos_ref[c] for c in range(3)]
    coord_m[1] = chosen(1, start)
    coord_m[0] = chosen(0, start)
    build_x(start)
    pl.semaphore_wait(barrier, len(ZONES))
    copies = coord_copies()
    for number in FAR + NEAR + (0,):
        copies[number].start()

    def step(t, carry):
        copies = coord_copies()
        pl.when(t == 0)(prepare)

        @pl.when(t > 0)
        def _():
            pl.when(t > 1)(hear)
            tell()
            force_copies()[0].wait_send()
            drain(f_send.at[1], blocks_ref)
            kinetic([speed_ref[pl.ds(8 * c, 8), :] for c in range(3)], t - 2)

        index = [[ids[pl.ds(24 * side + 8 * p, 8), :] for p in range(3)] for side in range(2)]
        low = [[x & 127 for x in side] for side in index]

        def gather(row, keep, places, which):
            for side, p, k in which:
                width = PASSES[p][1]
                for c in range(3):
                    if side == 0:
                        source = rows_of(lambda n: row(c, n), width, k)
                    else:
                        source = jnp.broadcast_to(row(c, k), (8, 128))
                    slot = where_is(side, p, c, k)
                    value = pick(source, places[side][p][c])
                    if keep is not None:
                        value = jnp.where(keep[side][p], pair_x[slot], value)
                    pair_x[slot] = value

        def blocks_of(passes):
            return [(1, p, k) for k in range(8) for p in passes] + [
                (0, p, k) for p in passes for k in range(PASSES[p][1])
            ]

        everywhere = [[[x] * 3 for x in side] for side in low]
        gather(lambda c, k: cur[pl.ds(8 * c + k, 1), :], None, everywhere, blocks_of(range(3)))

        not_x = [[(x < 128) | (x >= 256) for x in side] for side in index]
        in_x = [[x < 256 for x in side] for side in index]
        in_near = [[x < 256 + FIRST for x in side] for side in index]
        near_place, far_place = [
            [[[(x + width * c) & 127 for c in range(3)] for x in side] for side in low]
            for width in (FIRST, SECOND)
        ]
        drain(c_recv.at[1], blocks_ref.at[pl.ds(0, 2)])
        near[pl.ds(0, 8), :] = merge(packed[0], [got_m[n] for n in range(2)])
        gather(lambda c, k: near[pl.ds(k, 1), :], in_x, near_place, blocks_of(range(3)))

        copies[0].wait_recv()
        gather(lambda c, k: got_x[pl.ds(8 * c + k, 1), :], not_x, everywhere, blocks_of(range(3)))

        drain(c_recv.at[2], blocks_ref.at[pl.ds(0, 4)])
        near[pl.ds(8, 8), :] = merge(packed[1], [got_m[n] for n in range(2, 6)])

        def complete(which):
            gather(lambda c, k: near[pl.ds(8 + k, 1), :], in_near, far_place, which)

        complete(blocks_of(range(1)))

        energy = jnp.zeros((8, 128), F32)
        sublane = lax.broadcasted_iota(jnp.int32, (8, 128), 0)
        lefts = []
        parts = []
        for p, (begin, width) in enumerate(PASSES):
            usable = jnp.where(index[0][p] == CL_PAD, 0.0, 1.0)
            distinct = jnp.where(index[0][p] == index[1][p], 0.0, usable)
            limits = [distinct]
            for n in range(1, 8 // width):
                limits.append(jnp.where(sublane < n * width, usable, distinct))
            limits.append(usable)
            second = [[None] * 3 for _ in range(8)]
            for k in range(width):
                xi = [pair_x[where_is(0, p, c, k)] for c in range(3)]
                first = [None] * 3
                for l in range(8):
                    limit = limits[min(max(-((k - l) // width), 0), 8 // width)]
                    d = [xi[c] - pair_x[where_is(1, p, c, l)] for c in range(3)]
                    u = jnp.maximum(limit - dot3(d, d), 0.0)
                    uu = u * u
                    energy = energy + uu * u
                    for c in range(3):
                        push = uu * d[c]
                        first[c] = push if l == 0 else first[c] + push
                        second[l][c] = push if k == 0 else second[l][c] + push
                for n in range(8 // width):
                    for c in range(3):
                        pair_f[pl.ds((8 * c + k + n * width) * PITCH + begin, width), :] = roll(
                            first[c], -n * width, 0
                        )[:width]
                if p == 0:
                    complete(
                        [(1, 1, k), (1, 2, k)]
                        + ([(0, 1, k)] if k < 4 else [(0, 2, k - 4)] if k < 6 else [])
                    )
            for l in range(8):
                for c in range(3):
                    value = second[l][c]
                    turn = 4
                    while turn >= width:
                        value = value + roll(value, turn, 0)
                        turn //= 2
                    pair_f[pl.ds((24 + 8 * c + l) * PITCH + begin, width), :] = value[:width]
            left = jnp.concatenate(
                [
                    halves(pair_f[pl.ds(24 * PITCH * side + g, 24, stride=PITCH), :])
                    for side in range(2)
                    for g in range(begin, begin + width)
                ],
                axis=1,
            )
            lefts.append(left)
            parts.append(
                jnp.dot(
                    left,
                    table[
                        pl.ds(256 * begin, left.shape[1]),
                        pl.ds(128 if p == 0 else 256, 256 if p == 0 else 128),
                    ],
                    preferred_element_type=F32,
                )
            )

        halo = parts[0][:, 128:] + parts[1] + parts[2]
        halo = halo[:24] + halo[24:]
        returns = force_copies()
        beyond = [halo[8 * c : 8 * c + 8] for c in range(3)]
        force_m[1] = side_by_side(beyond, FIRST, SECOND)
        for number in FAR:
            returns[number].start()
        force_m[0] = side_by_side(beyond, 0, FIRST)
        for number in NEAR:
            returns[number].start()
        rest = jnp.dot(
            jnp.concatenate(lefts[1:], axis=1),
            table[pl.ds(2048, 1536), pl.ds(0, 256)],
            preferred_element_type=F32,
        )
        halo = parts[0][:, :128] + rest[:, 128:]
        force_x[...] = halo[:24] + halo[24:]
        returns[0].start()
        own = rest[:, :128] + jnp.dot(
            lefts[0], table[pl.ds(0, 2048), pl.ds(0, 128)], preferred_element_type=F32
        )
        own = own[:24] + own[24:]
        @pl.when(t > 0)
        def _():
            hear()
            tell()

        total = jnp.sum(jnp.sum(energy, axis=0, keepdims=True), axis=1, keepdims=True)
        row[...] = jnp.where(lanes(1) == t - 1, 2.0 * total, row[...])
        flags = flag8[...]
        direction, weights = link_frame(
            [cur[pl.ds(8 * c, 8), :] for c in range(3)], flags * up(flags)
        )
        for n, value in enumerate(direction + weights):
            frame[pl.ds(8 * n, 8), :] = value

        copies[0].wait_send()
        drain(c_send.at[1], blocks_ref)
        returns[0].wait_recv()
        came = jnp.dot(
            halves(ret_x[...]), back[...], preferred_element_type=F32
        )
        own = own + came[:24] + came[24:]
        drain(f_recv.at[1], blocks_ref.at[pl.ds(0, 2)])
        came = merge(packed[0], [ret_m[n] for n in range(2)])
        came = jnp.dot(halves(came), back2[pl.ds(0, 128), :], preferred_element_type=F32)
        came = came[:8] + came[8:]
        own = [
            own[8 * c : 8 * c + 8] + came[:, 128 * c : 128 * c + 128] for c in range(3)
        ]
        drain(f_recv.at[2], blocks_ref.at[pl.ds(0, 4)])
        came = merge(packed[1], [ret_m[n] for n in range(2, 6)])
        came = jnp.dot(halves(came), back2[pl.ds(128, 128), :], preferred_element_type=F32)
        came = came[:8] + came[8:]
        force = [
            0.5 * time_step * (own[c] + came[:, 128 * c : 128 * c + 128])
            for c in range(3)
        ]

        again = jnp.where(t > 0, 1.0, 0.0).astype(F32)
        speed = [half_ref[pl.ds(8 * c, 8), :] + again * force[c] for c in range(3)]

        @pl.when(t < ITERS)
        def _():
            half = [speed[c] + force[c] for c in range(3)]
            before = [cur[pl.ds(8 * c, 8), :] for c in range(3)]
            moved = constrain(
                [x + time_step * v for x, v in zip(before, half)],
                [frame[pl.ds(8 * n, 8), :] for n in range(3)],
                [frame[pl.ds(8 * n, 8), :] for n in range(3, 3 + 2 * NORDER + 1)],
                rest_ref[...],
                flag8[...],
            )
            send_coords(moved)
            for c in range(3):
                cur[pl.ds(8 * c, 8), :] = moved[c]
                half_ref[pl.ds(8 * c, 8), :] = (moved[c] - before[c]) / time_step
                speed_ref[pl.ds(8 * c, 8), :] = speed[c]

        @pl.when(t == ITERS)
        def _():
            kinetic(speed, ITERS - 1)
            for c in range(3):
                out_pos[c] = cur[pl.ds(8 * c, 8), :]
                out_vel[c] = speed[c]

        return carry

    lax.fori_loop(0, ITERS + 1, step, 0)
    def distance(offset):
        return sum(min(o, n - o) for o, n in zip(offset, sizes))

    def copy_row(source, target, offset, send, recv):
        pltpu.make_async_remote_copy(
            src_ref=source,
            dst_ref=target,
            send_sem=send,
            recv_sem=recv,
            device_id=at(offset),
            device_id_type=MESH,
        ).start()

    def total_of(slots):
        terms = [slots[n] for n in range(slots.shape[0])]
        while len(terms) > 1:
            terms = [
                terms[n] + terms[n + 1] if n + 1 < len(terms) else terms[n]
                for n in range(0, len(terms), 2)
            ]
        return terms[0]

    offsets = [(0, y, z) for y in range(sizes[1]) for z in range(sizes[2]) if y or z]
    own = me[1] * sizes[2] + me[2]
    for offset in sorted(offsets, key=distance, reverse=True):
        copy_row(row, plane.at[own], offset, p_send.at[0], p_recv.at[0])
    plane[own] = row[...]
    hear()
    tell()
    force_copies()[0].wait_send()
    drain(f_send.at[1], blocks_ref)
    hear()
    drain(p_recv.at[0], rows_ref.at[pl.ds(0, len(offsets))])
    mid[...] = total_of(plane)
    offsets = sorted([(x, 0, 0) for x in range(1, sizes[0])], key=distance)
    lead = me[2] == sizes[2] - 1

    @pl.when(lead)
    def _():
        for x, _, _ in offsets:
            for z in range(sizes[2]):
                copy_row(mid, line.at[me[0]], (x, 0, z), l_send.at[z], l_recv.at[0])

    line[me[0]] = mid[...]
    drain(p_send.at[0], rows_ref.at[pl.ds(0, plane.shape[0] - 1)])
    drain(l_recv.at[0], rows_ref.at[pl.ds(0, len(offsets))])
    out_en[...] = total_of(line)

    @pl.when(lead)
    def _():
        for z in range(sizes[2]):
            drain(l_send.at[z], rows_ref.at[pl.ds(0, len(offsets))])


CL_PAD = 306
KINETIC = 8
VMEM_LIMIT = 12 << 20


def finish(beads, pos_ref, vel_ref, sum_ref, out_pos, out_vel, out_en, energy, stored):
    stores = [
        pltpu.make_async_copy(source, target, stored.at[n])
        for n, (source, target) in enumerate(
            ((pos_ref, out_pos), (vel_ref, out_vel), (energy, out_en))
        )
    ]
    stores[0].start()
    stores[1].start()
    total = sum_ref[...] / F32(beads)
    for n in range(2):
        energy[pl.ds(n, 1), :] = total[:, KINETIC * n : KINETIC * n + ITERS]
    stores[2].start()
    for store in stores:
        store.wait()


def on_device(sizes, positions, velocities, send_list, pair_list, constraint_flags):
    dma = pltpu.SemaphoreType.DMA
    vmem = pltpu.VMEM
    plane = sizes[1] * sizes[2]
    results = pl.pallas_call(
        functools.partial(kernel, sizes),
        out_shape=(
            jax.ShapeDtypeStruct((3, 8, 128), F32),
            jax.ShapeDtypeStruct((3, 8, 128), F32),
            jax.ShapeDtypeStruct((1, 128), F32),
        ),
        in_specs=[pl.BlockSpec(memory_space=pltpu.HBM)] * 5,
        out_specs=[pl.BlockSpec(memory_space=vmem)] * 3,
        scratch_shapes=[
            vmem((24, 128), F32),
            vmem((24, 128), F32),
            vmem((8, 128), F32),
            vmem((48, 128), jnp.int32),
            vmem((8, 128), jnp.int32),
            vmem((8, 128), F32),
            vmem((2 * SLOTS, 384), jnp.bfloat16),
            vmem((128, 128), jnp.bfloat16),
            vmem((256, 384), jnp.bfloat16),
            vmem((16, 128), F32),
            vmem((24 + 8 * (2 * NORDER + 1), 128), F32),
            vmem((114, 8, 128), F32),
            vmem((49 * PITCH, 128), F32),
            vmem((24, 128), F32),
            vmem((2, 8, 128), F32),
            vmem((24, 128), F32),
            vmem((2, 8, 128), F32),
            vmem((24, 128), F32),
            vmem((6, 8, 128), F32),
            vmem((24, 128), F32),
            vmem((6, 8, 128), F32),
            vmem((1, 128), F32),
            vmem((plane, 1, 128), F32),
            vmem((1, 128), F32),
            vmem((sizes[0], 1, 128), F32),
            dma((2,)),
            dma((3,)),
            dma((2,)),
            dma((3,)),
            dma((1,)),
            dma((1,)),
            dma((sizes[2],)),
            dma((1,)),
            pltpu.SemaphoreType.REGULAR((4,)),
            vmem((3, 8, 128), F32),
            vmem((3, 8, 128), F32),
            vmem((1, 178), jnp.int32),
            vmem((2, SLOTS), jnp.int32),
            vmem((7, 128), jnp.int32),
            dma((5,)),
            vmem((6, 8, 128), F32),
            vmem((max(plane, sizes[0]) - 1, 1, 128), F32),
            vmem((24, 128), F32),
            vmem((4, 8, 128), jnp.int32),
            vmem((2, 8, 128), F32),
        ],
        compiler_params=pltpu.CompilerParams(
            collective_id=0, has_side_effects=True, vmem_limit_bytes=VMEM_LIMIT
        ),
        name="membrane",
    )(
        *[
            pltpu.with_memory_space_constraint(x, pltpu.HBM)
            for x in (
                positions,
                velocities,
                send_list.reshape(1, -1),
                pair_list,
                constraint_flags,
            )
        ]
    )
    position, velocity, energies = pl.pallas_call(
        functools.partial(finish, 8 * 128 * sizes[0] * sizes[1] * sizes[2]),
        out_shape=(
            jax.ShapeDtypeStruct((3, 8, 128), F32),
            jax.ShapeDtypeStruct((3, 8, 128), F32),
            jax.ShapeDtypeStruct((2, ITERS), F32),
        ),
        in_specs=[pl.BlockSpec(memory_space=vmem)] * 3,
        out_specs=[pl.BlockSpec(memory_space=pltpu.HBM)] * 3,
        scratch_shapes=[vmem((2, ITERS), F32), dma((3,))],
        compiler_params=pltpu.CompilerParams(vmem_limit_bytes=1 << 20),
        name="finish",
    )(*results)
    return position, velocity, energies.T


def solution(mesh):
    sizes = tuple(mesh.shape[a] for a in AXES)
    spec = ("runs", "gx", "gy", "gz")
    return jax.shard_map(
        functools.partial(on_device, sizes),
        mesh=mesh,
        in_specs=(
            P(None, None, spec),
            P(None, None, spec),
            P(spec),
            P(None, spec),
            P(None, spec),
        ),
        out_specs=(P(None, None, spec), P(None, None, spec), P("runs", None)),
        check_vma=False,
    )
```

```python
import functools

import jax
import jax.numpy as jnp
from jax import lax
from jax.experimental import pallas as pl
from jax.experimental.pallas import tpu as pltpu
from jax.sharding import PartitionSpec as P

CX, CY, CZ = 1, 8, 16
ITERS = 3
NORDER = 4
time_step = 0.02
root_half = 0.7071067811865476
MESH = pl.DeviceIdType.MESH
ZONES = ((1, 0, 0), (0, 1, 0), (0, 0, 1), (1, 1, 0), (1, 0, 1), (0, 1, 1), (1, 1, 1))
AXES = ("gx", "gy", "gz")
FIRST, SECOND = 24, 26
FAR, NEAR = (3, 6, 4, 5), (1, 2)
GROUPS = 14
SLOTS = 1792
PITCH = 24
F32 = jnp.float32


def roll(x, by, axis):
    size = x.shape[axis]
    by = by % size
    return x if by == 0 else pltpu.roll(x, by, axis)


def lanes(rows=8):
    return lax.broadcasted_iota(jnp.int32, (rows, 128), 1)


def side_by_side(parts, first, width):
    lane = lanes()
    return jnp.where(
        lane < first + width,
        parts[0],
        jnp.where(lane < first + 2 * width, roll(parts[1], width, 1), roll(parts[2], 2 * width, 1)),
    )


def merge(zone, received):
    block = received[0]
    for n in range(1, len(received)):
        block = jnp.where(zone >= n, received[n], block)
    return block


PASSES = ((0, 8), (8, 4), (12, 2))


def place(side, g):
    for begin, width in PASSES:
        if g < begin + width:
            return 2 * begin + width * side + g - begin


def pass_of(g):
    return max(n for n, (begin, _) in enumerate(PASSES) if begin <= g)


def where_is(side, p, c, k):
    width = PASSES[p][1]
    return sum(3 * w for _, w in PASSES[:p]) + c * width + k if side == 0 else 42 + 24 * p + 8 * c + k


def rows_of(row, width, k):
    sublane = lax.broadcasted_iota(jnp.int32, (8, 128), 0)
    value = jnp.broadcast_to(row(k), (8, 128))
    for n in range(1, 8 // width):
        value = jnp.where(sublane >= n * width, jnp.broadcast_to(row(k + n * width), (8, 128)), value)
    return value


def halves(value):
    high = value.astype(jnp.bfloat16).astype(F32)
    return jnp.concatenate([high, value - high], axis=0).astype(jnp.bfloat16)


def pick(table, index):
    return jnp.take_along_axis(table, index, axis=1, mode="promise_in_bounds")


def up(x):
    return roll(x, -1, 0)


def down(x):
    return roll(x, 1, 0)


def dot3(a, b):
    return a[0] * b[0] + a[1] * b[1] + a[2] * b[2]


def lag(x, by):
    return roll(x, -by, 0)


def expansion(coupling):
    coupling_down = down(coupling)
    power = {0: None}
    weights = {0: jnp.ones(coupling.shape, F32)}
    for _ in range(NORDER):
        later = {}
        for m, weight in power.items():
            lower = coupling_down if weight is None else coupling_down * down(weight)
            upper = coupling if weight is None else coupling * up(weight)
            for where_to, term in ((m - 1, lower), (m + 1, upper)):
                later[where_to] = later[where_to] + term if where_to in later else term
        power = later
        for m, weight in power.items():
            weights[m] = weights[m] + weight if m in weights else weight
    return [weights[m] for m in range(-NORDER, NORDER + 1)]


def expand(weights, source):
    terms = [w * lag(source, m - NORDER) for m, w in enumerate(weights)]
    while len(terms) > 1:
        terms = [
            terms[n] + terms[n + 1] if n + 1 < len(terms) else terms[n]
            for n in range(0, len(terms), 2)
        ]
    return terms[0]


def link_frame(previous, flags_pair):
    old = [x - up(x) for x in previous]
    length = jnp.maximum(jnp.sqrt(dot3(old, old)), 0.2)
    direction = [x / length for x in old]
    coupling = 0.5 * dot3(direction, [up(x) for x in direction]) * flags_pair
    return direction, expansion(coupling)


def constrain(updated, links, source, direction, weights, rest, flags):
    solution = expand(weights, source)
    shifts = [x * (root_half * solution) for x in direction]
    updated = [x - s + down(s) for x, s in zip(updated, shifts)]
    links = [x - (s + s) + (down(s) + up(s)) for x, s in zip(links, shifts)]
    squared = dot3(links, links)
    target = jnp.sqrt(jnp.maximum(2.0 * rest * rest - squared, 0.25 * rest * rest))
    solution = expand(weights, flags * root_half * (rest - target))
    shifts = [x * (root_half * solution) for x in direction]
    return [x - s + down(s) for x, s in zip(updated, shifts)]


def kernel(
    sizes,
    pos_in,
    vel_in,
    send_in,
    pair_in,
    flag_in,
    out_pos,
    out_vel,
    out_en,
    cur,
    half_ref,
    rest_ref,
    ids,
    send_ids,
    flag8,
    table,
    back,
    back2,
    near,
    frame,
    pair_x,
    pair_f,
    coord_x,
    coord_m,
    force_x,
    force_m,
    got_x,
    got_m,
    ret_x,
    ret_m,
    row,
    plane,
    mid,
    line,
    c_send,
    c_recv,
    f_send,
    f_recv,
    p_send,
    p_recv,
    l_send,
    l_recv,
    token,
    pos_ref,
    vel_ref,
    send_ref,
    pair_ref,
    flag_ref,
    loaded,
    blocks_ref,
    rows_ref,
    speed_ref,
    packed,
    shift,
):
    me = tuple(lax.axis_index(a) for a in AXES)

    def at(offset):
        return {
            a: lax.rem(me[i] + (offset[i] % sizes[i]), sizes[i])
            for i, a in enumerate(AXES)
            if offset[i] % sizes[i]
        }

    loads = [
        pltpu.make_async_copy(source, target, loaded.at[n])
        for n, (source, target) in enumerate(
            (
                (send_in, send_ref),
                (pos_in, pos_ref),
                (pair_in, pair_ref),
                (vel_in, vel_ref),
                (flag_in, flag_ref),
            )
        )
    ]
    for load in loads[:2]:
        load.start()
    barrier = pltpu.get_barrier_semaphore()
    for number in FAR + (0,) + NEAR:
        pl.semaphore_signal(
            barrier, inc=1, device_id=at(ZONES[number]), device_id_type=MESH
        )
    for load in loads[2:]:
        load.start()

    lane = lanes()
    row[...] = jnp.zeros(row.shape, F32)
    loads[0].wait()
    loads[1].wait()
    send_ids[...] = jnp.full(send_ids.shape, -1, jnp.int32)
    send_ids[pl.ds(0, 1), :] = send_ref[:, pl.ds(0, 128)]
    send_ids[pl.ds(1, 1), pl.ds(0, FIRST + SECOND)] = send_ref[:, pl.ds(128, FIRST + SECOND)]
    for c in range(3):
        cur[pl.ds(8 * c, 8), :] = pos_ref[c]

    def prepare():
        for load in loads[2:]:
            load.wait()
        for c in range(3):
            half_ref[pl.ds(8 * c, 8), :] = vel_ref[c]
        for side in range(2):
            for p, (begin, width) in enumerate(PASSES):
                for n in range(8):
                    g = begin + n % width
                    ids[pl.ds(24 * side + 8 * p + n, 1), :] = pair_ref[
                        pl.ds(side, 1), pl.ds(128 * g, 128)
                    ]
        flag8[...] = jnp.zeros(flag8.shape, F32)
        flag8[pl.ds(0, 7), :] = flag_ref[...].astype(F32)
        columns = jnp.transpose(ids[...].astype(F32))
        entry = jnp.broadcast_to(send_ids[pl.ds(1, 1), :], (8, 128))
        goals = [entry + 128 * c for c in range(3)]
        for n, (first, width) in enumerate(((0, FIRST), (FIRST, SECOND))):
            goal = side_by_side(goals, first, width)
            goal = jnp.where((lane >= first) & (lane < first + 3 * width), goal, -1)
            send_ids[pl.ds(2 + n, 1), :] = goal[:1]
        send_columns = jnp.transpose(send_ids[...].astype(F32))
        wide = lax.broadcasted_iota(jnp.int32, (128, 384), 1).astype(F32)
        for side in range(2):
            value = 12.0 if side == 0 else -12.0
            for g in range(GROUPS):
                at_row = 24 * side + 8 * pass_of(g) + g - PASSES[pass_of(g)][0]
                column = columns[:, at_row : at_row + 1]
                table[pl.ds(128 * place(side, g), 128), :] = jnp.where(
                    wide == column, value, 0.0
                ).astype(jnp.bfloat16)
        back[...] = jnp.where(wide[:, :128] == send_columns[:, 0:1], 1.0, 0.0).astype(jnp.bfloat16)
        for b in range(2):
            back2[pl.ds(128 * b, 128), :] = jnp.where(
                wide == send_columns[:, 2 + b : 3 + b], 1.0, 0.0
            ).astype(jnp.bfloat16)
        links = [pos_ref[c] - up(pos_ref[c]) for c in range(3)]
        rest_ref[...] = jnp.sqrt(dot3(links, links))

    ring = [tuple(sign if a == axis else 0 for a in range(3)) for axis in (0, 1) for sign in (1, -1)]

    def tell():
        for number, offset in enumerate(ring):
            pl.semaphore_signal(
                token.at[number], inc=1, device_id=at(offset), device_id_type=MESH
            )

    def hear():
        for number in range(len(ring)):
            pl.semaphore_wait(token.at[number], 1)

    def coord_copies():
        copies = []
        for number, zone in enumerate(ZONES):
            source = coord_x if number == 0 else coord_m.at[0 if number < 3 else 1]
            target = got_x if number == 0 else got_m.at[number - 1]
            copies.append(
                pltpu.make_async_remote_copy(
                    src_ref=source,
                    dst_ref=target,
                    send_sem=c_send.at[0 if number == 0 else 1],
                    recv_sem=c_recv.at[0 if number == 0 else 1 if number in NEAR else 2],
                    device_id=at(tuple(-z for z in zone)),
                    device_id_type=MESH,
                )
            )
        return copies

    def force_copies():
        copies = []
        for number, zone in enumerate(ZONES):
            source = force_x if number == 0 else force_m.at[0 if number < 3 else 1]
            target = ret_x if number == 0 else ret_m.at[number - 1]
            copies.append(
                pltpu.make_async_remote_copy(
                    src_ref=source,
                    dst_ref=target,
                    send_sem=f_send.at[0 if number == 0 else 1],
                    recv_sem=f_recv.at[0 if number == 0 else 1 if number in NEAR else 2],
                    device_id=at(zone),
                    device_id_type=MESH,
                )
            )
        return copies

    def drain(sem, ref):
        pltpu.make_async_copy(ref, ref, sem).wait()

    def kinetic(speed, number):
        total = jnp.sum(
            jnp.sum(dot3(speed, speed), axis=0, keepdims=True), axis=1, keepdims=True
        )
        row[...] = jnp.where(lanes(1) == KINETIC + number, 0.5 * total, row[...])

    edges = (0, 16, 24, 40, 48, 49, 50)
    entry = jnp.broadcast_to(send_ids[pl.ds(1, 1), :], (8, 128))
    for n, (first, width) in enumerate(((0, FIRST), (FIRST, SECOND))):
        zone = jnp.zeros((8, 128), jnp.int32)
        offset = [jnp.zeros((8, 128), F32) for _ in range(3)]
        for number in range(1, 7):
            begin = edges[number - 1]
            inside = (lane >= begin) & (lane < edges[number])
            zone = jnp.where(inside, number - 1 if n == 0 else number - 3, zone)
            for c, length in enumerate((CX, CY, CZ)):
                if ZONES[number][c]:
                    offset[c] = jnp.where(inside, F32(length), offset[c])
        packed[n] = side_by_side([zone] * 3, first, width)
        packed[2 + n] = jnp.maximum(side_by_side([entry] * 3, first, width), 0)
        shift[n] = side_by_side(offset, first, width)

    def chosen(n, home):
        first, width = ((0, FIRST), (FIRST, SECOND))[n]
        index = packed[2 + n]
        picked = [pick(x, index) for x in home]
        return shift[n] + jnp.where(
            lane < first + width,
            picked[0],
            jnp.where(lane < first + 2 * width, picked[1], picked[2]),
        )

    def build_x(home):
        send_x = jnp.broadcast_to(send_ids[pl.ds(0, 1), :], (8, 128))
        for c in range(3):
            value = pick(home[c], send_x)
            coord_x[pl.ds(8 * c, 8), :] = value + F32(CX) if c == 0 else value

    def send_coords(home):
        copies = coord_copies()
        coord_m[1] = chosen(1, home)
        for number in FAR:
            copies[number].start()
        coord_m[0] = chosen(0, home)
        for number in NEAR:
            copies[number].start()
        build_x(home)
        copies[0].start()

    start = [pos_ref[c] for c in range(3)]
    coord_m[1] = chosen(1, start)
    coord_m[0] = chosen(0, start)
    build_x(start)
    pl.semaphore_wait(barrier, len(ZONES))
    copies = coord_copies()
    for number in FAR + NEAR + (0,):
        copies[number].start()

    def step(t, carry):
        copies = coord_copies()
        pl.when(t == 0)(prepare)

        @pl.when(t > 0)
        def _():
            pl.when(t > 1)(hear)
            tell()
            force_copies()[0].wait_send()
            drain(f_send.at[1], blocks_ref)
            kinetic([speed_ref[pl.ds(8 * c, 8), :] for c in range(3)], t - 2)

        index = [[ids[pl.ds(24 * side + 8 * p, 8), :] for p in range(3)] for side in range(2)]
        low = [[x & 127 for x in side] for side in index]

        def gather(row, keep, places, which):
            for side, p, k in which:
                width = PASSES[p][1]
                for c in range(3):
                    if side == 0:
                        source = rows_of(lambda n: row(c, n), width, k)
                    else:
                        source = jnp.broadcast_to(row(c, k), (8, 128))
                    slot = where_is(side, p, c, k)
                    value = pick(source, places[side][p][c])
                    if keep is not None:
                        value = jnp.where(keep[side][p], pair_x[slot], value)
                    pair_x[slot] = value

        def blocks_of(passes):
            return [(1, p, k) for k in range(8) for p in passes] + [
                (0, p, k) for p in passes for k in range(PASSES[p][1])
            ]

        everywhere = [[[x] * 3 for x in side] for side in low]
        gather(lambda c, k: cur[pl.ds(8 * c + k, 1), :], None, everywhere, blocks_of(range(3)))

        not_x = [[(x < 128) | (x >= 256) for x in side] for side in index]
        in_x = [[x < 256 for x in side] for side in index]
        in_near = [[x < 256 + FIRST for x in side] for side in index]
        near_place, far_place = [
            [[[(x + width * c) & 127 for c in range(3)] for x in side] for side in low]
            for width in (FIRST, SECOND)
        ]
        drain(c_recv.at[1], blocks_ref.at[pl.ds(0, 2)])
        near[pl.ds(0, 8), :] = merge(packed[0], [got_m[n] for n in range(2)])
        gather(lambda c, k: near[pl.ds(k, 1), :], in_x, near_place, blocks_of(range(3)))

        copies[0].wait_recv()
        gather(lambda c, k: got_x[pl.ds(8 * c + k, 1), :], not_x, everywhere, blocks_of(range(3)))

        drain(c_recv.at[2], blocks_ref.at[pl.ds(0, 4)])
        near[pl.ds(8, 8), :] = merge(packed[1], [got_m[n] for n in range(2, 6)])

        def complete(which):
            gather(lambda c, k: near[pl.ds(8 + k, 1), :], in_near, far_place, which)

        complete(blocks_of(range(1)))

        energy = jnp.zeros((8, 128), F32)
        sublane = lax.broadcasted_iota(jnp.int32, (8, 128), 0)
        lefts = []
        parts = []
        for p, (begin, width) in enumerate(PASSES):
            usable = jnp.where(index[0][p] == CL_PAD, 0.0, 1.0)
            distinct = jnp.where(index[0][p] == index[1][p], 0.0, usable)
            limits = [distinct]
            for n in range(1, 8 // width):
                limits.append(jnp.where(sublane < n * width, usable, distinct))
            limits.append(usable)
            second = [[None] * 3 for _ in range(8)]
            for k in range(width):
                xi = [pair_x[where_is(0, p, c, k)] for c in range(3)]
                first = [None] * 3
                for l in range(8):
                    limit = limits[min(max(-((k - l) // width), 0), 8 // width)]
                    d = [xi[c] - pair_x[where_is(1, p, c, l)] for c in range(3)]
                    u = jnp.maximum(limit - dot3(d, d), 0.0)
                    uu = u * u
                    energy = energy + uu * u
                    for c in range(3):
                        push = uu * d[c]
                        first[c] = push if l == 0 else first[c] + push
                        second[l][c] = push if k == 0 else second[l][c] + push
                for n in range(8 // width):
                    for c in range(3):
                        pair_f[pl.ds((8 * c + k + n * width) * PITCH + begin, width), :] = roll(
                            first[c], -n * width, 0
                        )[:width]
                if p == 0:
                    complete(
                        [(1, 1, k), (1, 2, k)]
                        + ([(0, 1, k)] if k < 4 else [(0, 2, k - 4)] if k < 6 else [])
                    )
            for l in range(8):
                for c in range(3):
                    value = second[l][c]
                    turn = 4
                    while turn >= width:
                        value = value + roll(value, turn, 0)
                        turn //= 2
                    pair_f[pl.ds((24 + 8 * c + l) * PITCH + begin, width), :] = value[:width]
            left = jnp.concatenate(
                [
                    halves(pair_f[pl.ds(24 * PITCH * side + g, 24, stride=PITCH), :])
                    for side in range(2)
                    for g in range(begin, begin + width)
                ],
                axis=1,
            )
            lefts.append(left)
            parts.append(
                jnp.dot(
                    left,
                    table[
                        pl.ds(256 * begin, left.shape[1]),
                        pl.ds(128 if p == 0 else 256, 256 if p == 0 else 128),
                    ],
                    preferred_element_type=F32,
                )
            )

        halo = parts[0][:, 128:] + parts[1] + parts[2]
        halo = halo[:24] + halo[24:]
        returns = force_copies()
        beyond = [halo[8 * c : 8 * c + 8] for c in range(3)]
        force_m[1] = side_by_side(beyond, FIRST, SECOND)
        for number in FAR:
            returns[number].start()
        force_m[0] = side_by_side(beyond, 0, FIRST)
        for number in NEAR:
            returns[number].start()
        rest = jnp.dot(
            jnp.concatenate(lefts[1:], axis=1),
            table[pl.ds(2048, 1536), pl.ds(0, 256)],
            preferred_element_type=F32,
        )
        halo = parts[0][:, :128] + rest[:, 128:]
        force_x[...] = halo[:24] + halo[24:]
        returns[0].start()
        own = rest[:, :128] + jnp.dot(
            lefts[0], table[pl.ds(0, 2048), pl.ds(0, 128)], preferred_element_type=F32
        )
        own = own[:24] + own[24:]
        @pl.when(t > 0)
        def _():
            hear()
            tell()

        total = jnp.sum(jnp.sum(energy, axis=0, keepdims=True), axis=1, keepdims=True)
        row[...] = jnp.where(lanes(1) == t - 1, 2.0 * total, row[...])
        flags = flag8[...]
        direction, weights = link_frame(
            [cur[pl.ds(8 * c, 8), :] for c in range(3)], flags * up(flags)
        )
        for n, value in enumerate(direction + weights):
            frame[pl.ds(8 * n, 8), :] = value

        copies[0].wait_send()
        drain(c_send.at[1], blocks_ref)
        returns[0].wait_recv()
        came = jnp.dot(
            halves(ret_x[...]), back[...], preferred_element_type=F32
        )
        own = own + came[:24] + came[24:]
        drain(f_recv.at[1], blocks_ref.at[pl.ds(0, 2)])
        came = merge(packed[0], [ret_m[n] for n in range(2)])
        came = jnp.dot(halves(came), back2[pl.ds(0, 128), :], preferred_element_type=F32)
        came = came[:8] + came[8:]
        own = [
            own[8 * c : 8 * c + 8] + came[:, 128 * c : 128 * c + 128] for c in range(3)
        ]
        again = jnp.where(t > 0, 1.0, 0.0).astype(F32)
        share = F32(0.5 * time_step)
        gain = share * F32(time_step) * (1.0 + again)
        calm = [half_ref[pl.ds(8 * c, 8), :] + again * (share * own[c]) for c in range(3)]
        base = [
            cur[pl.ds(8 * c, 8), :] + time_step * (calm[c] + share * own[c]) for c in range(3)
        ]
        base_links = [x - up(x) for x in base]
        held = flag8[...] * root_half
        source = held * (dot3(direction, base_links) - rest_ref[...])
        pull = [held * gain * d for d in direction]
        drain(f_recv.at[2], blocks_ref.at[pl.ds(0, 4)])
        came = merge(packed[1], [ret_m[n] for n in range(2, 6)])
        came = jnp.dot(halves(came), back2[pl.ds(128, 128), :], preferred_element_type=F32)
        came = came[:8] + came[8:]
        came = [came[:, 128 * c : 128 * c + 128] for c in range(3)]
        speed = [calm[c] + (again * share) * came[c] for c in range(3)]

        @pl.when(t < ITERS)
        def _():
            before = [cur[pl.ds(8 * c, 8), :] for c in range(3)]
            bends = [x - up(x) for x in came]
            moved = constrain(
                [x + gain * f for x, f in zip(base, came)],
                [x + gain * b for x, b in zip(base_links, bends)],
                source + dot3(pull, bends),
                [frame[pl.ds(8 * n, 8), :] for n in range(3)],
                [frame[pl.ds(8 * n, 8), :] for n in range(3, 3 + 2 * NORDER + 1)],
                rest_ref[...],
                flag8[...],
            )
            send_coords(moved)
            for c in range(3):
                cur[pl.ds(8 * c, 8), :] = moved[c]
                half_ref[pl.ds(8 * c, 8), :] = (moved[c] - before[c]) / time_step
                speed_ref[pl.ds(8 * c, 8), :] = speed[c]

        @pl.when(t == ITERS)
        def _():
            kinetic(speed, ITERS - 1)
            for c in range(3):
                out_pos[c] = cur[pl.ds(8 * c, 8), :]
                out_vel[c] = speed[c]

        return carry

    lax.fori_loop(0, ITERS + 1, step, 0)
    def distance(offset):
        return sum(min(o, n - o) for o, n in zip(offset, sizes))

    def copy_row(source, target, offset, send, recv):
        pltpu.make_async_remote_copy(
            src_ref=source,
            dst_ref=target,
            send_sem=send,
            recv_sem=recv,
            device_id=at(offset),
            device_id_type=MESH,
        ).start()

    def total_of(slots):
        terms = [slots[n] for n in range(slots.shape[0])]
        while len(terms) > 1:
            terms = [
                terms[n] + terms[n + 1] if n + 1 < len(terms) else terms[n]
                for n in range(0, len(terms), 2)
            ]
        return terms[0]

    offsets = [(0, y, z) for y in range(sizes[1]) for z in range(sizes[2]) if y or z]
    own = me[1] * sizes[2] + me[2]
    for offset in sorted(offsets, key=distance, reverse=True):
        copy_row(row, plane.at[own], offset, p_send.at[0], p_recv.at[0])
    plane[own] = row[...]
    hear()
    tell()
    force_copies()[0].wait_send()
    drain(f_send.at[1], blocks_ref)
    hear()
    drain(p_recv.at[0], rows_ref.at[pl.ds(0, len(offsets))])
    mid[...] = total_of(plane)
    offsets = sorted([(x, 0, 0) for x in range(1, sizes[0])], key=distance)
    lead = me[2] == sizes[2] - 1

    @pl.when(lead)
    def _():
        for x, _, _ in offsets:
            for z in range(sizes[2]):
                copy_row(mid, line.at[me[0]], (x, 0, z), l_send.at[z], l_recv.at[0])

    line[me[0]] = mid[...]
    drain(p_send.at[0], rows_ref.at[pl.ds(0, plane.shape[0] - 1)])
    drain(l_recv.at[0], rows_ref.at[pl.ds(0, len(offsets))])
    out_en[...] = total_of(line)

    @pl.when(lead)
    def _():
        for z in range(sizes[2]):
            drain(l_send.at[z], rows_ref.at[pl.ds(0, len(offsets))])


CL_PAD = 306
KINETIC = 8
VMEM_LIMIT = 12 << 20


def finish(beads, pos_ref, vel_ref, sum_ref, out_pos, out_vel, out_en, energy, stored):
    stores = [
        pltpu.make_async_copy(source, target, stored.at[n])
        for n, (source, target) in enumerate(
            ((pos_ref, out_pos), (vel_ref, out_vel), (energy, out_en))
        )
    ]
    stores[0].start()
    stores[1].start()
    total = sum_ref[...] / F32(beads)
    for n in range(2):
        energy[pl.ds(n, 1), :] = total[:, KINETIC * n : KINETIC * n + ITERS]
    stores[2].start()
    for store in stores:
        store.wait()


def on_device(sizes, positions, velocities, send_list, pair_list, constraint_flags):
    dma = pltpu.SemaphoreType.DMA
    vmem = pltpu.VMEM
    plane = sizes[1] * sizes[2]
    results = pl.pallas_call(
        functools.partial(kernel, sizes),
        out_shape=(
            jax.ShapeDtypeStruct((3, 8, 128), F32),
            jax.ShapeDtypeStruct((3, 8, 128), F32),
            jax.ShapeDtypeStruct((1, 128), F32),
        ),
        in_specs=[pl.BlockSpec(memory_space=pltpu.HBM)] * 5,
        out_specs=[pl.BlockSpec(memory_space=vmem)] * 3,
        scratch_shapes=[
            vmem((24, 128), F32),
            vmem((24, 128), F32),
            vmem((8, 128), F32),
            vmem((48, 128), jnp.int32),
            vmem((8, 128), jnp.int32),
            vmem((8, 128), F32),
            vmem((2 * SLOTS, 384), jnp.bfloat16),
            vmem((128, 128), jnp.bfloat16),
            vmem((256, 384), jnp.bfloat16),
            vmem((16, 128), F32),
            vmem((24 + 8 * (2 * NORDER + 1), 128), F32),
            vmem((114, 8, 128), F32),
            vmem((49 * PITCH, 128), F32),
            vmem((24, 128), F32),
            vmem((2, 8, 128), F32),
            vmem((24, 128), F32),
            vmem((2, 8, 128), F32),
            vmem((24, 128), F32),
            vmem((6, 8, 128), F32),
            vmem((24, 128), F32),
            vmem((6, 8, 128), F32),
            vmem((1, 128), F32),
            vmem((plane, 1, 128), F32),
            vmem((1, 128), F32),
            vmem((sizes[0], 1, 128), F32),
            dma((2,)),
            dma((3,)),
            dma((2,)),
            dma((3,)),
            dma((1,)),
            dma((1,)),
            dma((sizes[2],)),
            dma((1,)),
            pltpu.SemaphoreType.REGULAR((4,)),
            vmem((3, 8, 128), F32),
            vmem((3, 8, 128), F32),
            vmem((1, 178), jnp.int32),
            vmem((2, SLOTS), jnp.int32),
            vmem((7, 128), jnp.int32),
            dma((5,)),
            vmem((6, 8, 128), F32),
            vmem((max(plane, sizes[0]) - 1, 1, 128), F32),
            vmem((24, 128), F32),
            vmem((4, 8, 128), jnp.int32),
            vmem((2, 8, 128), F32),
        ],
        compiler_params=pltpu.CompilerParams(
            collective_id=0, has_side_effects=True, vmem_limit_bytes=VMEM_LIMIT
        ),
        name="membrane",
    )(
        *[
            pltpu.with_memory_space_constraint(x, pltpu.HBM)
            for x in (
                positions,
                velocities,
                send_list.reshape(1, -1),
                pair_list,
                constraint_flags,
            )
        ]
    )
    position, velocity, energies = pl.pallas_call(
        functools.partial(finish, 8 * 128 * sizes[0] * sizes[1] * sizes[2]),
        out_shape=(
            jax.ShapeDtypeStruct((3, 8, 128), F32),
            jax.ShapeDtypeStruct((3, 8, 128), F32),
            jax.ShapeDtypeStruct((2, ITERS), F32),
        ),
        in_specs=[pl.BlockSpec(memory_space=vmem)] * 3,
        out_specs=[pl.BlockSpec(memory_space=pltpu.HBM)] * 3,
        scratch_shapes=[vmem((2, ITERS), F32), dma((3,))],
        compiler_params=pltpu.CompilerParams(vmem_limit_bytes=1 << 20),
        name="finish",
    )(*results)
    return position, velocity, energies.T


def solution(mesh):
    sizes = tuple(mesh.shape[a] for a in AXES)
    spec = ("runs", "gx", "gy", "gz")
    return jax.shard_map(
        functools.partial(on_device, sizes),
        mesh=mesh,
        in_specs=(
            P(None, None, spec),
            P(None, None, spec),
            P(spec),
            P(None, spec),
            P(None, spec),
        ),
        out_specs=(P(None, None, spec), P(None, None, spec), P("runs", None)),
        check_vma=False,
    )
```

```python
import functools

import jax
import jax.numpy as jnp
from jax import lax
from jax.experimental import pallas as pl
from jax.experimental.pallas import tpu as pltpu
from jax.sharding import PartitionSpec as P

CX, CY, CZ = 1, 8, 16
ITERS = 3
NORDER = 4
time_step = 0.02
root_half = 0.7071067811865476
MESH = pl.DeviceIdType.MESH
ZONES = ((1, 0, 0), (0, 1, 0), (0, 0, 1), (1, 1, 0), (1, 0, 1), (0, 1, 1), (1, 1, 1))
AXES = ("gx", "gy", "gz")
FIRST, SECOND = 24, 26
FAR, NEAR = (3, 6, 4, 5), (1, 2)
GROUPS = 14
SLOTS = 1792
PITCH = 24
F32 = jnp.float32


def roll(x, by, axis):
    size = x.shape[axis]
    by = by % size
    return x if by == 0 else pltpu.roll(x, by, axis)


def lanes(rows=8):
    return lax.broadcasted_iota(jnp.int32, (rows, 128), 1)


def side_by_side(parts, first, width):
    lane = lanes()
    return jnp.where(
        lane < first + width,
        parts[0],
        jnp.where(lane < first + 2 * width, roll(parts[1], width, 1), roll(parts[2], 2 * width, 1)),
    )


def merge(zone, received):
    block = received[0]
    for n in range(1, len(received)):
        block = jnp.where(zone >= n, received[n], block)
    return block


PASSES = ((0, 8), (8, 4), (12, 2))


def place(side, g):
    for begin, width in PASSES:
        if g < begin + width:
            return 2 * begin + width * side + g - begin


def pass_of(g):
    return max(n for n, (begin, _) in enumerate(PASSES) if begin <= g)


def where_is(side, p, c, k):
    width = PASSES[p][1]
    return sum(3 * w for _, w in PASSES[:p]) + c * width + k if side == 0 else 42 + 24 * p + 8 * c + k


def rows_of(row, width, k):
    sublane = lax.broadcasted_iota(jnp.int32, (8, 128), 0)
    value = jnp.broadcast_to(row(k), (8, 128))
    for n in range(1, 8 // width):
        value = jnp.where(sublane >= n * width, jnp.broadcast_to(row(k + n * width), (8, 128)), value)
    return value


def halves(value):
    high = value.astype(jnp.bfloat16).astype(F32)
    return jnp.concatenate([high, value - high], axis=0).astype(jnp.bfloat16)


def pick(table, index):
    return jnp.take_along_axis(table, index, axis=1, mode="promise_in_bounds")


def up(x):
    return roll(x, -1, 0)


def down(x):
    return roll(x, 1, 0)


def dot3(a, b):
    return a[0] * b[0] + a[1] * b[1] + a[2] * b[2]


def lag(x, by):
    return roll(x, -by, 0)


def expansion(coupling):
    coupling_down = down(coupling)
    power = {0: None}
    weights = {0: jnp.ones(coupling.shape, F32)}
    for _ in range(NORDER):
        later = {}
        for m, weight in power.items():
            lower = coupling_down if weight is None else coupling_down * down(weight)
            upper = coupling if weight is None else coupling * up(weight)
            for where_to, term in ((m - 1, lower), (m + 1, upper)):
                later[where_to] = later[where_to] + term if where_to in later else term
        power = later
        for m, weight in power.items():
            weights[m] = weights[m] + weight if m in weights else weight
    return [weights[m] for m in range(-NORDER, NORDER + 1)]


def expand(weights, source):
    terms = [w * lag(source, m - NORDER) for m, w in enumerate(weights)]
    while len(terms) > 1:
        terms = [
            terms[n] + terms[n + 1] if n + 1 < len(terms) else terms[n]
            for n in range(0, len(terms), 2)
        ]
    return terms[0]


def link_frame(previous, flags_pair):
    old = [x - up(x) for x in previous]
    length = jnp.maximum(jnp.sqrt(dot3(old, old)), 0.2)
    direction = [x / length for x in old]
    coupling = 0.5 * dot3(direction, [up(x) for x in direction]) * flags_pair
    return direction, expansion(coupling)


def constrain(updated, direction, weights, rest, flags):
    links = [x - up(x) for x in updated]
    solution = expand(weights, flags * root_half * (dot3(direction, links) - rest))
    shifts = [x * (root_half * solution) for x in direction]
    updated = [x - s + down(s) for x, s in zip(updated, shifts)]
    links = [x - (s + s) + (down(s) + up(s)) for x, s in zip(links, shifts)]
    squared = dot3(links, links)
    target = jnp.sqrt(jnp.maximum(2.0 * rest * rest - squared, 0.25 * rest * rest))
    solution = expand(weights, flags * root_half * (rest - target))
    shifts = [x * (root_half * solution) for x in direction]
    return [x - s + down(s) for x, s in zip(updated, shifts)]


def kernel(
    sizes,
    pos_in,
    vel_in,
    send_in,
    pair_in,
    flag_in,
    out_pos,
    out_vel,
    out_en,
    cur,
    half_ref,
    rest_ref,
    ids,
    send_ids,
    flag8,
    table,
    back,
    back2,
    near,
    frame,
    pair_x,
    pair_f,
    coord_x,
    coord_m,
    force_x,
    force_m,
    got_x,
    got_m,
    ret_x,
    ret_m,
    row,
    plane,
    mid,
    line,
    c_send,
    c_recv,
    f_send,
    f_recv,
    p_send,
    p_recv,
    l_send,
    l_recv,
    token,
    pos_ref,
    vel_ref,
    send_ref,
    pair_ref,
    flag_ref,
    loaded,
    blocks_ref,
    rows_ref,
    speed_ref,
    packed,
    shift,
):
    me = tuple(lax.axis_index(a) for a in AXES)

    def at(offset):
        return {
            a: lax.rem(me[i] + (offset[i] % sizes[i]), sizes[i])
            for i, a in enumerate(AXES)
            if offset[i] % sizes[i]
        }

    loads = [
        pltpu.make_async_copy(source, target, loaded.at[n])
        for n, (source, target) in enumerate(
            (
                (send_in, send_ref),
                (pos_in, pos_ref),
                (pair_in, pair_ref),
                (vel_in, vel_ref),
                (flag_in, flag_ref),
            )
        )
    ]
    for load in loads[:2]:
        load.start()
    barrier = pltpu.get_barrier_semaphore()
    for number in FAR + (0,) + NEAR:
        pl.semaphore_signal(
            barrier, inc=1, device_id=at(ZONES[number]), device_id_type=MESH
        )
    for load in loads[2:]:
        load.start()

    lane = lanes()
    row[...] = jnp.zeros(row.shape, F32)
    loads[0].wait()
    loads[1].wait()
    send_ids[...] = jnp.full(send_ids.shape, -1, jnp.int32)
    send_ids[pl.ds(0, 1), :] = send_ref[:, pl.ds(0, 128)]
    send_ids[pl.ds(1, 1), pl.ds(0, FIRST + SECOND)] = send_ref[:, pl.ds(128, FIRST + SECOND)]
    for c in range(3):
        cur[pl.ds(8 * c, 8), :] = pos_ref[c]

    def prepare():
        for load in loads[2:]:
            load.wait()
        for c in range(3):
            half_ref[pl.ds(8 * c, 8), :] = vel_ref[c]
        for side in range(2):
            for p, (begin, width) in enumerate(PASSES):
                for n in range(8):
                    g = begin + n % width
                    ids[pl.ds(24 * side + 8 * p + n, 1), :] = pair_ref[
                        pl.ds(side, 1), pl.ds(128 * g, 128)
                    ]
        flag8[...] = jnp.zeros(flag8.shape, F32)
        flag8[pl.ds(0, 7), :] = flag_ref[...].astype(F32)
        columns = jnp.transpose(ids[...].astype(F32))
        entry = jnp.broadcast_to(send_ids[pl.ds(1, 1), :], (8, 128))
        goals = [entry + 128 * c for c in range(3)]
        for n, (first, width) in enumerate(((0, FIRST), (FIRST, SECOND))):
            goal = side_by_side(goals, first, width)
            goal = jnp.where((lane >= first) & (lane < first + 3 * width), goal, -1)
            send_ids[pl.ds(2 + n, 1), :] = goal[:1]
        send_columns = jnp.transpose(send_ids[...].astype(F32))
        wide = lax.broadcasted_iota(jnp.int32, (128, 384), 1).astype(F32)
        for side in range(2):
            value = 12.0 if side == 0 else -12.0
            for g in range(GROUPS):
                at_row = 24 * side + 8 * pass_of(g) + g - PASSES[pass_of(g)][0]
                column = columns[:, at_row : at_row + 1]
                table[pl.ds(128 * place(side, g), 128), :] = jnp.where(
                    wide == column, value, 0.0
                ).astype(jnp.bfloat16)
        back[...] = jnp.where(wide[:, :128] == send_columns[:, 0:1], 1.0, 0.0).astype(jnp.bfloat16)
        for b in range(2):
            back2[pl.ds(128 * b, 128), :] = jnp.where(
                wide == send_columns[:, 2 + b : 3 + b], 1.0, 0.0
            ).astype(jnp.bfloat16)
        links = [pos_ref[c] - up(pos_ref[c]) for c in range(3)]
        rest_ref[...] = jnp.sqrt(dot3(links, links))

    ring = [tuple(sign if a == axis else 0 for a in range(3)) for axis in (0, 1) for sign in (1, -1)]

    def tell():
        for number, offset in enumerate(ring):
            pl.semaphore_signal(
                token.at[number], inc=1, device_id=at(offset), device_id_type=MESH
            )

    def hear():
        for number in range(len(ring)):
            pl.semaphore_wait(token.at[number], 1)

    def coord_copies():
        copies = []
        for number, zone in enumerate(ZONES):
            source = coord_x if number == 0 else coord_m.at[0 if number < 3 else 1]
            target = got_x if number == 0 else got_m.at[number - 1]
            copies.append(
                pltpu.make_async_remote_copy(
                    src_ref=source,
                    dst_ref=target,
                    send_sem=c_send.at[0],
                    recv_sem=c_recv.at[0 if number == 0 else 1 if number in NEAR else 2],
                    device_id=at(tuple(-z for z in zone)),
                    device_id_type=MESH,
                )
            )
        return copies

    def force_copies():
        copies = []
        for number, zone in enumerate(ZONES):
            source = force_x if number == 0 else force_m.at[0 if number < 3 else 1]
            target = ret_x if number == 0 else ret_m.at[number - 1]
            copies.append(
                pltpu.make_async_remote_copy(
                    src_ref=source,
                    dst_ref=target,
                    send_sem=f_send.at[0],
                    recv_sem=f_recv.at[0 if number == 0 else 1 if number in NEAR else 2],
                    device_id=at(zone),
                    device_id_type=MESH,
                )
            )
        return copies

    def drain(sem, ref):
        pltpu.make_async_copy(ref, ref, sem).wait()

    def kinetic(speed, number):
        total = jnp.sum(
            jnp.sum(dot3(speed, speed), axis=0, keepdims=True), axis=1, keepdims=True
        )
        row[...] = jnp.where(lanes(1) == KINETIC + number, 0.5 * total, row[...])

    edges = (0, 16, 24, 40, 48, 49, 50)
    entry = jnp.broadcast_to(send_ids[pl.ds(1, 1), :], (8, 128))
    for n, (first, width) in enumerate(((0, FIRST), (FIRST, SECOND))):
        zone = jnp.zeros((8, 128), jnp.int32)
        offset = [jnp.zeros((8, 128), F32) for _ in range(3)]
        for number in range(1, 7):
            begin = edges[number - 1]
            inside = (lane >= begin) & (lane < edges[number])
            zone = jnp.where(inside, number - 1 if n == 0 else number - 3, zone)
            for c, length in enumerate((CX, CY, CZ)):
                if ZONES[number][c]:
                    offset[c] = jnp.where(inside, F32(length), offset[c])
        packed[n] = side_by_side([zone] * 3, first, width)
        packed[2 + n] = jnp.maximum(side_by_side([entry] * 3, first, width), 0)
        shift[n] = side_by_side(offset, first, width)

    def chosen(n, home):
        first, width = ((0, FIRST), (FIRST, SECOND))[n]
        index = packed[2 + n]
        picked = [pick(x, index) for x in home]
        return shift[n] + jnp.where(
            lane < first + width,
            picked[0],
            jnp.where(lane < first + 2 * width, picked[1], picked[2]),
        )

    def build_x(home):
        send_x = jnp.broadcast_to(send_ids[pl.ds(0, 1), :], (8, 128))
        for c in range(3):
            value = pick(home[c], send_x)
            coord_x[pl.ds(8 * c, 8), :] = value + F32(CX) if c == 0 else value

    def send_coords(home):
        copies = coord_copies()
        coord_m[1] = chosen(1, home)
        for number in FAR:
            copies[number].start()
        coord_m[0] = chosen(0, home)
        for number in NEAR:
            copies[number].start()
        build_x(home)
        copies[0].start()

    start = [pos_ref[c] for c in range(3)]
    coord_m[1] = chosen(1, start)
    coord_m[0] = chosen(0, start)
    build_x(start)
    pl.semaphore_wait(barrier, len(ZONES))
    copies = coord_copies()
    for number in FAR + NEAR + (0,):
        copies[number].start()

    def step(t, carry):
        copies = coord_copies()
        pl.when(t == 0)(prepare)

        @pl.when(t > 0)
        def _():
            pl.when(t > 1)(hear)
            tell()
            drain(f_send.at[0], blocks_ref)
            kinetic([speed_ref[pl.ds(8 * c, 8), :] for c in range(3)], t - 2)

        index = [[ids[pl.ds(24 * side + 8 * p, 8), :] for p in range(3)] for side in range(2)]
        low = [[x & 127 for x in side] for side in index]

        def gather(row, keep, places, which):
            for side, p, k in which:
                width = PASSES[p][1]
                for c in range(3):
                    if side == 0:
                        source = rows_of(lambda n: row(c, n), width, k)
                    else:
                        source = jnp.broadcast_to(row(c, k), (8, 128))
                    slot = where_is(side, p, c, k)
                    value = pick(source, places[side][p][c])
                    if keep is not None:
                        value = jnp.where(keep[side][p], pair_x[slot], value)
                    pair_x[slot] = value

        def blocks_of(passes):
            return [(1, p, k) for k in range(8) for p in passes] + [
                (0, p, k) for p in passes for k in range(PASSES[p][1])
            ]

        everywhere = [[[x] * 3 for x in side] for side in low]
        gather(lambda c, k: cur[pl.ds(8 * c + k, 1), :], None, everywhere, blocks_of(range(3)))

        not_x = [[(x < 128) | (x >= 256) for x in side] for side in index]
        in_x = [[x < 256 for x in side] for side in index]
        in_near = [[x < 256 + FIRST for x in side] for side in index]
        near_place, far_place = [
            [[[(x + width * c) & 127 for c in range(3)] for x in side] for side in low]
            for width in (FIRST, SECOND)
        ]
        drain(c_recv.at[1], blocks_ref.at[pl.ds(0, 2)])
        near[pl.ds(0, 8), :] = merge(packed[0], [got_m[n] for n in range(2)])
        gather(lambda c, k: near[pl.ds(k, 1), :], in_x, near_place, blocks_of(range(3)))

        copies[0].wait_recv()
        gather(lambda c, k: got_x[pl.ds(8 * c + k, 1), :], not_x, everywhere, blocks_of(range(3)))

        drain(c_recv.at[2], blocks_ref.at[pl.ds(0, 4)])
        near[pl.ds(8, 8), :] = merge(packed[1], [got_m[n] for n in range(2, 6)])

        def complete(which):
            gather(lambda c, k: near[pl.ds(8 + k, 1), :], in_near, far_place, which)

        complete(blocks_of(range(1)))

        energy = jnp.zeros((8, 128), F32)
        sublane = lax.broadcasted_iota(jnp.int32, (8, 128), 0)
        lefts = []
        parts = []
        for p, (begin, width) in enumerate(PASSES):
            usable = jnp.where(index[0][p] == CL_PAD, 0.0, 1.0)
            distinct = jnp.where(index[0][p] == index[1][p], 0.0, usable)
            limits = [distinct]
            for n in range(1, 8 // width):
                limits.append(jnp.where(sublane < n * width, usable, distinct))
            limits.append(usable)
            second = [[None] * 3 for _ in range(8)]
            for k in range(width):
                xi = [pair_x[where_is(0, p, c, k)] for c in range(3)]
                first = [None] * 3
                for l in range(8):
                    limit = limits[min(max(-((k - l) // width), 0), 8 // width)]
                    d = [xi[c] - pair_x[where_is(1, p, c, l)] for c in range(3)]
                    u = jnp.maximum(limit - dot3(d, d), 0.0)
                    uu = u * u
                    energy = energy + uu * u
                    for c in range(3):
                        push = uu * d[c]
                        first[c] = push if l == 0 else first[c] + push
                        second[l][c] = push if k == 0 else second[l][c] + push
                for n in range(8 // width):
                    for c in range(3):
                        pair_f[pl.ds((8 * c + k + n * width) * PITCH + begin, width), :] = roll(
                            first[c], -n * width, 0
                        )[:width]
                if p == 0:
                    complete(
                        [(1, 1, k), (1, 2, k)]
                        + ([(0, 1, k)] if k < 4 else [(0, 2, k - 4)] if k < 6 else [])
                    )
            for l in range(8):
                for c in range(3):
                    value = second[l][c]
                    turn = 4
                    while turn >= width:
                        value = value + roll(value, turn, 0)
                        turn //= 2
                    pair_f[pl.ds((24 + 8 * c + l) * PITCH + begin, width), :] = value[:width]
            left = jnp.concatenate(
                [
                    halves(pair_f[pl.ds(24 * PITCH * side + g, 24, stride=PITCH), :])
                    for side in range(2)
                    for g in range(begin, begin + width)
                ],
                axis=1,
            )
            lefts.append(left)
            parts.append(
                jnp.dot(
                    left,
                    table[
                        pl.ds(256 * begin, left.shape[1]),
                        pl.ds(128 if p == 0 else 256, 256 if p == 0 else 128),
                    ],
                    preferred_element_type=F32,
                )
            )

        halo = parts[0][:, 128:] + parts[1] + parts[2]
        halo = halo[:24] + halo[24:]
        returns = force_copies()
        beyond = [halo[8 * c : 8 * c + 8] for c in range(3)]
        force_m[1] = side_by_side(beyond, FIRST, SECOND)
        for number in FAR:
            returns[number].start()
        force_m[0] = side_by_side(beyond, 0, FIRST)
        for number in NEAR:
            returns[number].start()
        rest = jnp.dot(
            jnp.concatenate(lefts[1:], axis=1),
            table[pl.ds(2048, 1536), pl.ds(0, 256)],
            preferred_element_type=F32,
        )
        halo = parts[0][:, :128] + rest[:, 128:]
        force_x[...] = halo[:24] + halo[24:]
        returns[0].start()
        own = rest[:, :128] + jnp.dot(
            lefts[0], table[pl.ds(0, 2048), pl.ds(0, 128)], preferred_element_type=F32
        )
        own = own[:24] + own[24:]
        @pl.when(t > 0)
        def _():
            hear()
            tell()

        total = jnp.sum(jnp.sum(energy, axis=0, keepdims=True), axis=1, keepdims=True)
        row[...] = jnp.where(lanes(1) == t - 1, 2.0 * total, row[...])
        flags = flag8[...]
        direction, weights = link_frame(
            [cur[pl.ds(8 * c, 8), :] for c in range(3)], flags * up(flags)
        )
        for n, value in enumerate(direction + weights):
            frame[pl.ds(8 * n, 8), :] = value

        drain(c_send.at[0], blocks_ref)
        returns[0].wait_recv()
        came = jnp.dot(
            halves(ret_x[...]), back[...], preferred_element_type=F32
        )
        own = own + came[:24] + came[24:]
        drain(f_recv.at[1], blocks_ref.at[pl.ds(0, 2)])
        came = merge(packed[0], [ret_m[n] for n in range(2)])
        came = jnp.dot(halves(came), back2[pl.ds(0, 128), :], preferred_element_type=F32)
        came = came[:8] + came[8:]
        own = [
            own[8 * c : 8 * c + 8] + came[:, 128 * c : 128 * c + 128] for c in range(3)
        ]
        drain(f_recv.at[2], blocks_ref.at[pl.ds(0, 4)])
        came = merge(packed[1], [ret_m[n] for n in range(2, 6)])
        came = jnp.dot(halves(came), back2[pl.ds(128, 128), :], preferred_element_type=F32)
        came = came[:8] + came[8:]
        force = [
            0.5 * time_step * (own[c] + came[:, 128 * c : 128 * c + 128])
            for c in range(3)
        ]

        again = jnp.where(t > 0, 1.0, 0.0).astype(F32)
        speed = [half_ref[pl.ds(8 * c, 8), :] + again * force[c] for c in range(3)]

        @pl.when(t < ITERS)
        def _():
            half = [speed[c] + force[c] for c in range(3)]
            before = [cur[pl.ds(8 * c, 8), :] for c in range(3)]
            moved = constrain(
                [x + time_step * v for x, v in zip(before, half)],
                [frame[pl.ds(8 * n, 8), :] for n in range(3)],
                [frame[pl.ds(8 * n, 8), :] for n in range(3, 3 + 2 * NORDER + 1)],
                rest_ref[...],
                flag8[...],
            )
            send_coords(moved)
            for c in range(3):
                cur[pl.ds(8 * c, 8), :] = moved[c]
                half_ref[pl.ds(8 * c, 8), :] = (moved[c] - before[c]) / time_step
                speed_ref[pl.ds(8 * c, 8), :] = speed[c]

        @pl.when(t == ITERS)
        def _():
            kinetic(speed, ITERS - 1)
            for c in range(3):
                out_pos[c] = cur[pl.ds(8 * c, 8), :]
                out_vel[c] = speed[c]

        return carry

    lax.fori_loop(0, ITERS + 1, step, 0)
    def distance(offset):
        return sum(min(o, n - o) for o, n in zip(offset, sizes))

    def copy_row(source, target, offset, send, recv):
        pltpu.make_async_remote_copy(
            src_ref=source,
            dst_ref=target,
            send_sem=send,
            recv_sem=recv,
            device_id=at(offset),
            device_id_type=MESH,
        ).start()

    def total_of(slots):
        terms = [slots[n] for n in range(slots.shape[0])]
        while len(terms) > 1:
            terms = [
                terms[n] + terms[n + 1] if n + 1 < len(terms) else terms[n]
                for n in range(0, len(terms), 2)
            ]
        return terms[0]

    offsets = [(0, y, z) for y in range(sizes[1]) for z in range(sizes[2]) if y or z]
    own = me[1] * sizes[2] + me[2]
    for offset in sorted(offsets, key=distance, reverse=True):
        copy_row(row, plane.at[own], offset, p_send.at[0], p_recv.at[0])
    plane[own] = row[...]
    hear()
    tell()
    drain(f_send.at[0], blocks_ref)
    hear()
    drain(p_recv.at[0], rows_ref.at[pl.ds(0, len(offsets))])
    mid[...] = total_of(plane)
    offsets = sorted([(x, 0, 0) for x in range(1, sizes[0])], key=distance)
    lead = me[2] == sizes[2] - 1

    @pl.when(lead)
    def _():
        for x, _, _ in offsets:
            for z in range(sizes[2]):
                copy_row(mid, line.at[me[0]], (x, 0, z), l_send.at[0], l_recv.at[0])

    line[me[0]] = mid[...]
    drain(p_send.at[0], rows_ref.at[pl.ds(0, plane.shape[0] - 1)])
    drain(l_recv.at[0], rows_ref.at[pl.ds(0, len(offsets))])
    out_en[...] = total_of(line)

    @pl.when(lead)
    def _():
        drain(l_send.at[0], rows_ref.at[pl.ds(0, sizes[2] * len(offsets))])


CL_PAD = 306
KINETIC = 8
VMEM_LIMIT = 12 << 20


def finish(beads, pos_ref, vel_ref, sum_ref, out_pos, out_vel, out_en, energy, stored):
    stores = [
        pltpu.make_async_copy(source, target, stored.at[n])
        for n, (source, target) in enumerate(
            ((pos_ref, out_pos), (vel_ref, out_vel), (energy, out_en))
        )
    ]
    stores[0].start()
    stores[1].start()
    total = sum_ref[...] / F32(beads)
    for n in range(2):
        energy[pl.ds(n, 1), :] = total[:, KINETIC * n : KINETIC * n + ITERS]
    stores[2].start()
    for store in stores:
        store.wait()


def on_device(sizes, positions, velocities, send_list, pair_list, constraint_flags):
    dma = pltpu.SemaphoreType.DMA
    vmem = pltpu.VMEM
    plane = sizes[1] * sizes[2]
    results = pl.pallas_call(
        functools.partial(kernel, sizes),
        out_shape=(
            jax.ShapeDtypeStruct((3, 8, 128), F32),
            jax.ShapeDtypeStruct((3, 8, 128), F32),
            jax.ShapeDtypeStruct((1, 128), F32),
        ),
        in_specs=[pl.BlockSpec(memory_space=pltpu.HBM)] * 5,
        out_specs=[pl.BlockSpec(memory_space=vmem)] * 3,
        scratch_shapes=[
            vmem((24, 128), F32),
            vmem((24, 128), F32),
            vmem((8, 128), F32),
            vmem((48, 128), jnp.int32),
            vmem((8, 128), jnp.int32),
            vmem((8, 128), F32),
            vmem((2 * SLOTS, 384), jnp.bfloat16),
            vmem((128, 128), jnp.bfloat16),
            vmem((256, 384), jnp.bfloat16),
            vmem((16, 128), F32),
            vmem((24 + 8 * (2 * NORDER + 1), 128), F32),
            vmem((114, 8, 128), F32),
            vmem((49 * PITCH, 128), F32),
            vmem((24, 128), F32),
            vmem((2, 8, 128), F32),
            vmem((24, 128), F32),
            vmem((2, 8, 128), F32),
            vmem((24, 128), F32),
            vmem((6, 8, 128), F32),
            vmem((24, 128), F32),
            vmem((6, 8, 128), F32),
            vmem((1, 128), F32),
            vmem((plane, 1, 128), F32),
            vmem((1, 128), F32),
            vmem((sizes[0], 1, 128), F32),
            dma((1,)),
            dma((3,)),
            dma((1,)),
            dma((3,)),
            dma((1,)),
            dma((1,)),
            dma((1,)),
            dma((1,)),
            pltpu.SemaphoreType.REGULAR((4,)),
            vmem((3, 8, 128), F32),
            vmem((3, 8, 128), F32),
            vmem((1, 178), jnp.int32),
            vmem((2, SLOTS), jnp.int32),
            vmem((7, 128), jnp.int32),
            dma((5,)),
            vmem((9, 8, 128), F32),
            vmem((max(plane - 1, sizes[2] * (sizes[0] - 1)), 1, 128), F32),
            vmem((24, 128), F32),
            vmem((4, 8, 128), jnp.int32),
            vmem((2, 8, 128), F32),
        ],
        compiler_params=pltpu.CompilerParams(
            collective_id=0, has_side_effects=True, vmem_limit_bytes=VMEM_LIMIT
        ),
        name="membrane",
    )(
        *[
            pltpu.with_memory_space_constraint(x, pltpu.HBM)
            for x in (
                positions,
                velocities,
                send_list.reshape(1, -1),
                pair_list,
                constraint_flags,
            )
        ]
    )
    position, velocity, energies = pl.pallas_call(
        functools.partial(finish, 8 * 128 * sizes[0] * sizes[1] * sizes[2]),
        out_shape=(
            jax.ShapeDtypeStruct((3, 8, 128), F32),
            jax.ShapeDtypeStruct((3, 8, 128), F32),
            jax.ShapeDtypeStruct((2, ITERS), F32),
        ),
        in_specs=[pl.BlockSpec(memory_space=vmem)] * 3,
        out_specs=[pl.BlockSpec(memory_space=pltpu.HBM)] * 3,
        scratch_shapes=[vmem((2, ITERS), F32), dma((3,))],
        compiler_params=pltpu.CompilerParams(vmem_limit_bytes=1 << 20),
        name="finish",
    )(*results)
    return position, velocity, energies.T


def solution(mesh):
    sizes = tuple(mesh.shape[a] for a in AXES)
    spec = ("runs", "gx", "gy", "gz")
    return jax.shard_map(
        functools.partial(on_device, sizes),
        mesh=mesh,
        in_specs=(
            P(None, None, spec),
            P(None, None, spec),
            P(spec),
            P(None, spec),
            P(None, spec),
        ),
        out_specs=(P(None, None, spec), P(None, None, spec), P("runs", None)),
        check_vma=False,
    )
```
